32 devices in a mesh: dp: 8 (over z, x), tensor: 4 (over y, core).
Axes of the slice: x: 2, y: 2, z: 4, core: 2. Of those that a mesh axis runs over, the one named last changes fastest.
Arguments:
- tokens: bfloat16 [4096, 2560], P('dp'), may hold values from -6 to 6
- doc_start: int32 [4096], P('dp'), may hold values from 0 to 4095, as said below
- norm1_gain: float32 [2560], replicated, may hold values from 0.5 to 1.5
- proj_x: bfloat16 [2560, 2560], P(None, 'tensor'), may hold values from -0.125 to 0.125
- proj_y: bfloat16 [2560, 2560], P(None, 'tensor'), may hold values from -0.125 to 0.125
- conv_weight: float32 [4, 2560], P(None, 'tensor'), may hold values from -3 to 3
- conv_bias: float32 [2560], P('tensor'), may hold values from -2 to 2
- gate_x_weight: bfloat16 [256, 2560], P(None, 'tensor'), may hold values from -0.375 to 0.375
- gate_x_bias: float32 [2560], P('tensor'), may hold values from -4 to 4
- gate_a_weight: bfloat16 [256, 2560], P(None, 'tensor'), may hold values from -0.375 to 0.375
- gate_a_bias: float32 [2560], P('tensor'), may hold values from -4 to 4
- decay_param: float32 [2560], P('tensor'), as said below
- proj_out: bfloat16 [2560, 2560], P('tensor'), may hold values from -0.5 to 0.5
- norm2_gain: float32 [2560], replicated, may hold values from 0.5 to 1.5
- mlp_gate: bfloat16 [2560, 7680], P('dp', 'tensor'), may hold values from -0.125 to 0.125
- mlp_up: bfloat16 [2560, 7680], P('dp', 'tensor'), may hold values from -0.125 to 0.125
- mlp_down: bfloat16 [2560, 7680], P('dp', 'tensor'), may hold values from -0.125 to 0.125
- cotangent: bfloat16 [4096, 2560], P('dp'), may hold values from -6 to 6
Outputs:
- block_out: float32 [4096, 2560], P(('dp', 'tensor'))
- grad_tokens: float32 [4096, 2560], P(('dp', 'tensor'))
- grad_norm1_gain: float32 [2560], replicated
- grad_proj_x: float32 [2560, 2560], P('dp', 'tensor')
- grad_proj_y: float32 [2560, 2560], P('dp', 'tensor')
- grad_conv_weight: float32 [4, 2560], P(None, 'tensor')
- grad_conv_bias: float32 [2560], P('tensor')
- grad_gate_x_weight: float32 [256, 2560], P(None, 'tensor')
- grad_gate_x_bias: float32 [2560], P('tensor')
- grad_gate_a_weight: float32 [256, 2560], P(None, 'tensor')
- grad_gate_a_bias: float32 [2560], P('tensor')
- grad_decay_param: float32 [2560], P('tensor')
- grad_proj_out: float32 [2560, 2560], P('tensor', 'dp')
- grad_norm2_gain: float32 [2560], replicated
- grad_mlp_gate: float32 [2560, 7680], P('dp', 'tensor')
- grad_mlp_up: float32 [2560, 7680], P('dp', 'tensor')
- grad_mlp_down: float32 [2560, 7680], P('dp', 'tensor')
The draws below stay inside these ranges and needn't reach their ends.
Inputs may be any that keep to these rules, and one draw needn't show every extreme that they name: `doc_start`: each token's entry is the stream position at which its document begins. Sequences of 2048 tokens begin at the positions 1792 + k * 2048, so the stream begins and ends with part of one; each begins a document. In each sequence the first document runs 3 * 512 to 2047 tokens and later ones 2048 // 10 to 2047 tokens, the last one cut at the sequence's end. `decay_param`: softplus of each entry lies between 0.02 / 2048 and 0.008.
All inputs are finite; a program needn't handle non-finite values.
Results may differ from the reference program's by a relative error of at most 0.025.
Values may be sent and summed in bfloat16 or wider, within the bound.
A program may use at most 448 MiB of HBM per device.

```python
import math
import jax
import jax.numpy as jnp
from jax import lax

D = 2560
BW = 256
HEADS = 10
R = 2560
FF = 7680
CONV = 4
SEQ = 2048
TOKENS = 4096


def draw_doc_start(key, part):
    lead_count = SEQ // 8
    seq_count = TOKENS // SEQ + 1
    shortest = max(SEQ // 10, 1)
    pieces = SEQ // shortest + 1
    first_key = jax.random.fold_in(key, 11)
    rest_key = jax.random.fold_in(key, 23)
    first_len = jax.random.randint(first_key, (seq_count, 1), 3 * SEQ // 4, SEQ).astype(jnp.int32)
    rest_len = jax.random.randint(rest_key, (seq_count, pieces), shortest, SEQ).astype(jnp.int32)
    lengths = jnp.concatenate([first_len, rest_len], axis=1)
    bounds = jnp.cumsum(lengths, axis=1) - lengths
    offsets = jnp.arange(SEQ, dtype=jnp.int32)
    covered = bounds[:, None, :] <= offsets[None, :, None]
    within = jnp.max(jnp.where(covered, bounds[:, None, :], 0), axis=2)
    base_pos = jnp.arange(seq_count, dtype=jnp.int32) * SEQ - lead_count
    starts = (within + base_pos[:, None]).reshape(seq_count * SEQ)
    result = starts[lead_count:lead_count + TOKENS]
    return jnp.maximum(result, 0).astype(jnp.int32)


def draw_decay_param(key, part):
    uniform_val = jax.random.uniform(key, (R,), jnp.float32)
    lower_log = math.log(0.02 / SEQ)
    upper_log = math.log(0.008)
    softplus_val = jnp.exp(lower_log + uniform_val * (upper_log - lower_log))
    return (softplus_val + jnp.log(-jnp.expm1(-softplus_val))).astype(jnp.float32)


def shard_levels(rng, shape, shards, least, largest):
    loudness = 1.0
    for position, parts in shards:
        heights = jax.random.uniform(jax.random.fold_in(jax.random.fold_in(rng, 6), position), (parts,), jnp.float32, least / len(shards), largest / len(shards))
        loudness = loudness * jnp.repeat(jnp.exp(heights), shape[position] // parts).reshape((-1,) + (1,) * (len(shape) - 1 - position))
    return loudness


def gaussian(stream_key, extent, deviation, reach, split=(), kind=jnp.bfloat16):
    values = deviation * jax.random.normal(stream_key, extent, jnp.float32)
    if split:
        values = values * shard_levels(stream_key, extent, split, -0.22, 0.18)
    return jnp.clip(values, -reach, reach).astype(kind)


def setup_inputs(seed: int = 0) -> dict:
    splits = jax.random.split(jax.random.key(seed), 19)
    return {
        "tokens": gaussian(splits[0], (TOKENS, D), 1.0, 6.0, ((0, 8),)),
        "doc_start": draw_doc_start(jax.random.fold_in(splits[18], 71), 0),
        "norm1_gain": jnp.clip(1.0 + 0.1 * jax.random.normal(splits[2], (D,), jnp.float32), 0.5, 1.5),
        "proj_x": gaussian(splits[3], (D, R), D ** -0.5, 0.125, ((1, 4),)),
        "proj_y": gaussian(splits[4], (D, R), D ** -0.5, 0.125, ((1, 4),)),
        "conv_weight": gaussian(splits[5], (CONV, R), 0.5, 3.0, ((1, 4),), jnp.float32),
        "conv_bias": gaussian(splits[6], (R,), 0.3, 2.0, ((0, 4),), jnp.float32),
        "gate_x_weight": gaussian(splits[7], (BW, R), BW ** -0.5, 0.375, ((1, 4),)),
        "gate_x_bias": gaussian(splits[8], (R,), 1.0, 4.0, ((0, 4),), jnp.float32),
        "gate_a_weight": gaussian(splits[9], (BW, R), BW ** -0.5, 0.375, ((1, 4),)),
        "gate_a_bias": gaussian(splits[10], (R,), 1.0, 4.0, ((0, 4),), jnp.float32),
        "decay_param": draw_decay_param(jax.random.fold_in(splits[18], 71), 0),
        "proj_out": gaussian(splits[12], (R, D), (R // 16) ** -0.5, 0.5, ((0, 4),)),
        "norm2_gain": jnp.clip(1.0 + 0.1 * jax.random.normal(splits[13], (D,), jnp.float32), 0.5, 1.5),
        "mlp_gate": gaussian(splits[14], (D, FF), D ** -0.5, 0.125, ((0, 8), (1, 4))),
        "mlp_up": gaussian(splits[15], (D, FF), D ** -0.5, 0.125, ((0, 8), (1, 4))),
        "mlp_down": gaussian(splits[16], (D, FF), (FF // 4) ** -0.5, 0.125, ((0, 8), (1, 4))),
        "cotangent": gaussian(splits[17], (TOKENS, D), 1.0, 6.0, ((0, 8),)),
    }


@jax.custom_vjp
def low(v):
    return lax.optimization_barrier(v.astype(jnp.bfloat16)).astype(jnp.float32)

@jax.custom_vjp
def low_back(v):
    return v

def low_keep(v):
    return (low(v), None)

def low_pass(kept, grad):
    return (grad,)

def back_keep(v):
    return (v, None)

def back_low(kept, grad):
    return (low(grad),)
low.defvjp(low_keep, low_pass)
low_back.defvjp(back_keep, back_low)
epsilon = 1e-06
highest = lax.Precision.HIGHEST

def rms_norm(values, gain_vec):
    inv_rms = lax.rsqrt(lax.optimization_barrier(jnp.mean(values * values, axis=-1, keepdims=True)) + epsilon)
    return values * inv_rms * gain_vec

def gelu_tanh(values):
    return jax.nn.gelu(values, approximate=True)

def linear_step(earlier, latter):
    return (earlier[0] * latter[0], latter[0] * earlier[1] + latter[1])

def matmul(left_rows, right_rows):
    return jnp.dot(left_rows, right_rows, precision=highest)

def forward(tokens, norm1_gain, proj_x, proj_y, conv_weight, conv_bias, gate_x_weight, gate_x_bias, gate_a_weight, gate_a_bias, decay_param, proj_out, norm2_gain, mlp_gate, mlp_up, mlp_down, doc_start):
    stream_len = tokens.shape[0]
    positions = jnp.arange(stream_len, dtype=jnp.int32)
    normed = low(rms_norm(tokens, norm1_gain))
    branch_y = low_back(matmul(normed, proj_y))
    branch_x = low(low_back(matmul(normed, proj_x)))
    conv_out = conv_bias + conv_weight[0] * branch_x
    for offset in range(1, CONV):
        shifted = jnp.concatenate([jnp.zeros((offset, branch_x.shape[1]), jnp.float32), branch_x[:stream_len - offset]], axis=0)
        inside = (positions - offset >= doc_start).astype(jnp.float32)[:, None]
        conv_out = conv_out + conv_weight[offset] * shifted * inside
    conv_out = low(conv_out)
    blocks = conv_out.reshape(stream_len, HEADS, BW)

    def gate_pre(weight, bias_vec):
        mixed_blocks = jnp.einsum('nhi,ihj->nhj', blocks, weight.reshape(BW, HEADS, BW), precision=highest)
        return low_back(mixed_blocks.reshape(stream_len, R)) + bias_vec
    pre_input = gate_pre(gate_x_weight, gate_x_bias)
    pre_recur = gate_pre(gate_a_weight, gate_a_bias)
    starting = (doc_start == positions)[:, None]
    log_decay = -8.0 * jax.nn.sigmoid(pre_recur) * jax.nn.softplus(decay_param)
    decay = jnp.where(starting, 0.0, jnp.exp(log_decay))
    multiplier = jnp.where(starting, 1.0, jnp.sqrt(-jnp.expm1(2.0 * log_decay)))
    drive = multiplier * jax.nn.sigmoid(pre_input) * conv_out
    states = lax.associative_scan(linear_step, (decay, drive), axis=0)[1]
    lru_out = low_back(matmul(low(states * gelu_tanh(branch_y)), proj_out))
    resid = tokens + lru_out
    normed2 = low(rms_norm(resid, norm2_gain))
    gate_act = low_back(matmul(normed2, mlp_gate))
    up_act = low_back(matmul(normed2, mlp_up))
    hidden = low(gelu_tanh(gate_act) * up_act)
    return resid + matmul(hidden, mlp_down.T)

def reference(tokens, doc_start, norm1_gain, proj_x, proj_y, conv_weight, conv_bias, gate_x_weight, gate_x_bias, gate_a_weight, gate_a_bias, decay_param, proj_out, norm2_gain, mlp_gate, mlp_up, mlp_down, cotangent):
    floats = [array_in.astype(jnp.float32) for array_in in (tokens, norm1_gain, proj_x, proj_y, conv_weight, conv_bias, gate_x_weight, gate_x_bias, gate_a_weight, gate_a_bias, decay_param, proj_out, norm2_gain, mlp_gate, mlp_up, mlp_down)]

    def wrapped(*arrays):
        return forward(*arrays, doc_start)
    block_out, pullback = jax.vjp(wrapped, *floats)
    grads = pullback(cotangent.astype(jnp.float32))
    return (block_out, grads[0], grads[1], grads[2], grads[3], grads[4], grads[5], grads[6], grads[7], grads[8], grads[9], grads[10], grads[11], grads[12], grads[13], grads[14], grads[15])
```

```python
import functools

import jax
import jax.numpy as jnp
from jax import lax
from jax.experimental import pallas as pl
from jax.experimental.pallas import tpu as pltpu
from jax.sharding import PartitionSpec as P

epsilon = 1e-06
MESH = pl.DeviceIdType.MESH
GROUP = 4
LINKS = (("dp", 1), ("dp", 0), ("tensor", 1))
CORE = ("tensor", 0)
ORDERS = ((1, 2, 0), (2, 0, 1), (0, 1, 2))


def gelu_tanh(values):
    return jax.nn.gelu(values, approximate=True)


def gated_product(gate_vals, up_vals):
    return gelu_tanh(gate_vals) * up_vals


def contract_last(left_rows, right_rows):
    return lax.dot_general(
        left_rows, right_rows, (((1,), (1,)), ((), ())), preferred_element_type=jnp.float32
    )


def contract_first(left_rows, right_rows):
    return lax.dot_general(
        left_rows, right_rows, (((0,), (0,)), ((), ())), preferred_element_type=jnp.float32
    )


def matmul(left_rows, right_rows):
    return jnp.dot(left_rows, right_rows, preferred_element_type=jnp.float32)


def shifted(block, axis, distance):
    devices = range(lax.axis_size(axis))
    route = [(i - distance, i) for i in devices if i - distance in devices]
    return lax.ppermute(block, axis, route)


def flipped(array, axis, mask):
    return lax.ppermute(array, axis, [(i, i ^ mask) for i in range(lax.axis_size(axis))])


def bit_of(axis, bit):
    return (lax.axis_index(axis) // (1 << bit)) % 2


def across(axis, bit):
    index = lax.axis_index(axis)
    return {axis: index + (1 - 2 * ((index // (1 << bit)) % 2)) * (1 << bit)}


def thirds(width):
    tiles = width // 128
    spans, start = [], 0
    for k in range(3):
        count = (tiles + 2 - k) // 3
        spans.append((start * 128, count * 128))
        start += count
    return spans


def send(src, dst, send_sem, recv_sem, device):
    copy = pltpu.make_async_remote_copy(
        src_ref=src,
        dst_ref=dst,
        send_sem=send_sem,
        recv_sem=recv_sem,
        device_id=device,
        device_id_type=MESH,
    )
    copy.start()
    return copy


def greet(devices):
    barrier = pltpu.get_barrier_semaphore()
    for device in devices:
        pl.semaphore_signal(barrier, inc=1, device_id=device, device_id_type=MESH)
    pl.semaphore_wait(barrier, len(devices))


def gather_block(x_ref, out_ref, send_sem, recv_sem, core_send, core_recv, own_sem):
    me = [bit_of(*link) for link in LINKS]
    core = bit_of(*CORE)
    peers = [across(*link) for link in LINKS]
    core_peer = across(*CORE)
    spans = thirds(x_ref.shape[1])
    own = pltpu.make_async_copy(x_ref, out_ref.at[me[0], me[1], me[2], core], own_sem)
    own.start()

    def region(idx, k):
        return out_ref.at[idx[0], idx[1], idx[2], core, :, pl.ds(*spans[k])]

    moving = [
        send(
            x_ref.at[:, pl.ds(*spans[k])],
            region(me, k),
            send_sem.at[k, 0],
            recv_sem.at[k, 0],
            peers[ORDERS[k][0]],
        )
        for k in range(3)
    ]
    to_core = [
        send(
            x_ref,
            out_ref.at[me[0], me[1], me[2], core],
            core_send.at[9],
            core_recv.at[9],
            core_peer,
        )
    ]
    sent = []
    own.wait()
    for step in range(3):
        for k in range(3):
            order = ORDERS[k]
            moving[k].wait_recv()
            sent.append(moving[k])
            if step < 2:
                held = [slice(None) if d in order[: step + 1] else me[d] for d in range(3)]
                moving[k] = send(
                    region(held, k),
                    region(held, k),
                    send_sem.at[k, step + 1],
                    recv_sem.at[k, step + 1],
                    peers[order[step + 1]],
                )
            fresh = [
                slice(None) if d in order[:step] else (1 - me[d] if d == order[step] else me[d])
                for d in range(3)
            ]
            to_core.append(
                send(
                    region(fresh, k),
                    region(fresh, k),
                    core_send.at[3 * step + k],
                    core_recv.at[3 * step + k],
                    core_peer,
                )
            )
    for copy in sent:
        copy.wait_send()
    for copy in to_core:
        copy.wait()


GATHER_SEMS = [
    pltpu.SemaphoreType.DMA((3, 3)),
    pltpu.SemaphoreType.DMA((3, 3)),
    pltpu.SemaphoreType.DMA((10,)),
    pltpu.SemaphoreType.DMA((10,)),
    pltpu.SemaphoreType.DMA,
]


def sum_tensor(part_ref, q, core_buf, link_buf, sems_s, sems_r, own_sem):
    high, core = bit_of(*LINKS[2]), bit_of(*CORE)
    link_peer, core_peer = across(*LINKS[2]), across(*CORE)
    own = pltpu.make_async_copy(part_ref.at[:, core], q, own_sem)
    own.start()
    far = send(
        part_ref.at[1 - high, 1 - core], core_buf.at[1 - high], sems_s.at[0], sems_r.at[0], core_peer
    )
    near = send(part_ref.at[high, 1 - core], core_buf.at[high], sems_s.at[1], sems_r.at[1], core_peer)
    own.wait()
    far.wait_recv()
    q[1 - high] = q[1 - high] + core_buf[1 - high]
    along = send(q.at[1 - high], link_buf, sems_s.at[2], sems_r.at[2], link_peer)
    near.wait_recv()
    along.wait_recv()
    return high, (far, near, along)


SUM_SEMS = [
    pltpu.SemaphoreType.DMA((3,)),
    pltpu.SemaphoreType.DMA((3,)),
    pltpu.SemaphoreType.DMA,
]
STRIP = 16


def middle_kernel(
    part_ref, tok_ref, gain_ref, resid_ref, all_ref,
    q, core_buf, link_buf, low, sum_s, sum_r, sum_own, *gather_sems
):
    greet([across(*link) for link in LINKS] + [across(*CORE)])
    high, copies = sum_tensor(part_ref, q, core_buf, link_buf, sum_s, sum_r, sum_own)

    def strip(i, carry):
        rows = pl.ds(pl.multiple_of(i * STRIP, STRIP), STRIP)
        total = (
            q[high, rows].astype(jnp.float32)
            + core_buf[high, rows].astype(jnp.float32)
            + link_buf[rows].astype(jnp.float32)
        )
        resid = tok_ref[rows].astype(jnp.float32) + total
        resid_ref[rows] = resid
        inv = lax.rsqrt(jnp.mean(resid * resid, axis=-1, keepdims=True) + epsilon)
        low[rows] = (resid * inv * gain_ref[...]).astype(low.dtype)
        return carry

    lax.fori_loop(0, tok_ref.shape[0] // STRIP, strip, 0)
    for copy in copies:
        copy.wait_send()
    gather_block(low, all_ref, *gather_sems)


def middle(part, tok, gain):
    rows, width = tok.shape
    return pl.pallas_call(
        middle_kernel,
        name="middle",
        out_shape=(
            jax.ShapeDtypeStruct((rows, width), jnp.float32),
            jax.ShapeDtypeStruct((2, 2, 2, 2, rows, width), jnp.bfloat16),
        ),
        in_specs=[
            pl.BlockSpec(memory_space=pl.ANY),
            pl.BlockSpec(memory_space=pltpu.VMEM),
            pl.BlockSpec(memory_space=pltpu.VMEM),
        ],
        out_specs=(pl.BlockSpec(memory_space=pltpu.VMEM), pl.BlockSpec(memory_space=pl.ANY)),
        scratch_shapes=[
            pltpu.VMEM((2, rows, width), jnp.bfloat16),
            pltpu.VMEM((2, rows, width), jnp.bfloat16),
            pltpu.VMEM((rows, width), jnp.bfloat16),
            pltpu.VMEM((rows, width), jnp.bfloat16),
            *SUM_SEMS,
            *GATHER_SEMS,
        ],
        compiler_params=pltpu.CompilerParams(
            collective_id=1, has_side_effects=True, vmem_limit_bytes=32 * 2**20
        ),
    )(part.reshape(2, 2, rows, width), tok, gain.reshape(1, width))


def norm_back(rows, back, base_ref, gain_ref, keep_ref, gain_acc):
    base = base_ref[rows].astype(jnp.float32)
    inv = lax.rsqrt(jnp.mean(base * base, axis=-1, keepdims=True) + epsilon)
    unit = base * inv
    scaled = gain_ref[...] * back
    grad = inv * (scaled - unit * jnp.mean(unit * scaled, axis=-1, keepdims=True))
    terms = back * unit
    gain_acc[...] += terms[:8] + terms[8:]
    return keep_ref[rows].astype(jnp.float32) + grad


def back_kernel(
    p_ref, resid_ref, cot_ref, gain_ref, grad_ref, all_ref, gain_out,
    q, cb, r0, r1, r2, low, gain_acc, ssem, rsem, fs, fr, own_sem, gs, gr, gather_own
):
    me = [bit_of(*link) for link in LINKS]
    core = bit_of(*CORE)
    peers = [across(*link) for link in LINKS]
    core_peer = across(*CORE)
    spans = thirds(q.shape[-1])
    own = pltpu.make_async_copy(p_ref.at[:, :, :, core], q, own_sem)
    own.start()
    greet(peers + [core_peer])

    def half(k, near):
        first = ORDERS[k][0]
        return [(me[d] if near else 1 - me[d]) if d == first else slice(None) for d in range(3)]

    to_core = []
    for near in (False, True):
        for k in range(3):
            i = half(k, near)
            to_core.append(
                send(
                    p_ref.at[i[0], i[1], i[2], 1 - core, :, pl.ds(*spans[k])],
                    cb.at[i[0], i[1], i[2], :, pl.ds(*spans[k])],
                    fs.at[len(to_core)],
                    fr.at[len(to_core)],
                    core_peer,
                )
            )
    own.wait()

    def add(i, k, other):
        s, n = spans[k]
        q[i[0], i[1], i[2], :, s : s + n] = q[i[0], i[1], i[2], :, s : s + n] + other

    moving, sent = [], []
    for near in (False, True):
        for k in range(3):
            to_core[3 * near + k].wait_recv()
            i = half(k, near)
            s, n = spans[k]
            add(i, k, cb[i[0], i[1], i[2], :, s : s + n])
            if not near:
                moving.append(
                    send(
                        q.at[i[0], i[1], i[2], :, pl.ds(s, n)],
                        r0.at[:, :, :, pl.ds(s, n)],
                        ssem.at[k, 0],
                        rsem.at[k, 0],
                        peers[ORDERS[k][0]],
                    )
                )
    for step in (1, 2):
        for k in range(3):
            s, n = spans[k]
            order = ORDERS[k]
            moving[k].wait_recv()
            sent.append(moving[k])
            kept = [me[d] if d in order[:step] else slice(None) for d in range(3)]
            add(kept, k, r0[:, :, :, s : s + n] if step == 1 else r1[:, :, s : s + n])
            away = [
                me[d] if d in order[:step] else (1 - me[d] if d == order[step] else slice(None))
                for d in range(3)
            ]
            moving[k] = send(
                q.at[away[0], away[1], away[2], :, pl.ds(s, n)],
                r1.at[:, :, pl.ds(s, n)] if step == 1 else r2.at[:, pl.ds(s, n)],
                ssem.at[k, step],
                rsem.at[k, step],
                peers[order[step]],
            )
    for k in range(3):
        moving[k].wait_recv()
        sent.append(moving[k])
    gain_acc[...] = jnp.zeros_like(gain_acc)

    def strip(i, carry):
        rows = pl.ds(pl.multiple_of(i * STRIP, STRIP), STRIP)
        back = q[me[0], me[1], me[2], rows].astype(jnp.float32) + r2[rows].astype(jnp.float32)
        grad = norm_back(rows, back, resid_ref, gain_ref, cot_ref, gain_acc)
        grad_ref[rows] = grad
        low[rows] = grad.astype(low.dtype)
        return carry

    lax.fori_loop(0, low.shape[0] // STRIP, strip, 0)
    for copy in sent + to_core:
        copy.wait_send()
    gain_out[...] = jnp.sum(gain_acc[...], axis=0, keepdims=True)
    mine = all_ref.at[me[2], core]
    local = pltpu.make_async_copy(low, mine, gather_own)
    local.start()
    along = send(low, mine, gs.at[0], gr.at[0], peers[2])
    beside = send(low, mine, gs.at[1], gr.at[1], core_peer)
    along.wait_recv()
    theirs = all_ref.at[1 - me[2], core]
    onward = send(theirs, theirs, gs.at[2], gr.at[2], core_peer)
    local.wait()
    beside.wait()
    onward.wait()
    along.wait_send()


def back_pass(part, resid, cot, gain):
    rows, width = resid.shape
    wide = lambda *lead: pltpu.VMEM((*lead, rows, width), jnp.bfloat16)
    vmem = pl.BlockSpec(memory_space=pltpu.VMEM)
    return pl.pallas_call(
        back_kernel,
        name="back",
        out_shape=(
            jax.ShapeDtypeStruct((rows, width), jnp.float32),
            jax.ShapeDtypeStruct((2, 2, rows, width), jnp.bfloat16),
            jax.ShapeDtypeStruct((1, width), jnp.float32),
        ),
        in_specs=[pl.BlockSpec(memory_space=pl.ANY), vmem, vmem, vmem],
        out_specs=(vmem, pl.BlockSpec(memory_space=pl.ANY), vmem),
        scratch_shapes=[
            wide(2, 2, 2),
            wide(2, 2, 2),
            wide(2, 2),
            wide(2),
            wide(),
            wide(),
            pltpu.VMEM((8, width), jnp.float32),
            pltpu.SemaphoreType.DMA((3, 3)),
            pltpu.SemaphoreType.DMA((3, 3)),
            pltpu.SemaphoreType.DMA((6,)),
            pltpu.SemaphoreType.DMA((6,)),
            pltpu.SemaphoreType.DMA,
            pltpu.SemaphoreType.DMA((3,)),
            pltpu.SemaphoreType.DMA((3,)),
            pltpu.SemaphoreType.DMA,
        ],
        compiler_params=pltpu.CompilerParams(
            collective_id=2, has_side_effects=True, vmem_limit_bytes=40 * 2**20
        ),
    )(part.reshape(2, 2, 2, 2, rows, width), resid, cot, gain.reshape(1, width))


def last_kernel(
    part_ref, tok_ref, keep_ref, gain_ref, grad_ref, gain_out,
    q, core_buf, link_buf, gain_acc, sum_s, sum_r, sum_own
):
    greet([across(*LINKS[2]), across(*CORE)])
    high, copies = sum_tensor(part_ref, q, core_buf, link_buf, sum_s, sum_r, sum_own)
    gain_acc[...] = jnp.zeros_like(gain_acc)

    def strip(i, carry):
        rows = pl.ds(pl.multiple_of(i * STRIP, STRIP), STRIP)
        back = (
            q[high, rows].astype(jnp.float32)
            + core_buf[high, rows].astype(jnp.float32)
            + link_buf[rows].astype(jnp.float32)
        )
        grad_ref[rows] = norm_back(rows, back, tok_ref, gain_ref, keep_ref, gain_acc)
        return carry

    lax.fori_loop(0, tok_ref.shape[0] // STRIP, strip, 0)
    gain_out[...] = jnp.sum(gain_acc[...], axis=0, keepdims=True)
    for copy in copies:
        copy.wait_send()


def last_pass(part, tok, keep, gain):
    rows, width = tok.shape
    vmem = pl.BlockSpec(memory_space=pltpu.VMEM)
    return pl.pallas_call(
        last_kernel,
        name="last",
        out_shape=(
            jax.ShapeDtypeStruct((rows, width), jnp.float32),
            jax.ShapeDtypeStruct((1, width), jnp.float32),
        ),
        in_specs=[pl.BlockSpec(memory_space=pl.ANY), vmem, vmem, vmem],
        out_specs=(vmem, vmem),
        scratch_shapes=[
            pltpu.VMEM((2, rows, width), jnp.bfloat16),
            pltpu.VMEM((2, rows, width), jnp.bfloat16),
            pltpu.VMEM((rows, width), jnp.bfloat16),
            pltpu.VMEM((8, width), jnp.float32),
            *SUM_SEMS,
        ],
        compiler_params=pltpu.CompilerParams(
            collective_id=3, has_side_effects=True, vmem_limit_bytes=32 * 2**20
        ),
    )(part.reshape(2, 2, rows, width), tok, keep, gain.reshape(1, width))


def scan_kernel(n, reverse, a_ref, b_ref, out_ref, edge_ref, fa, fb, mine, others, ssem, rsem):
    place = lax.axis_index("dp")
    sign = -1 if reverse else 1
    barrier = pltpu.get_barrier_semaphore()
    peers = [{"dp": (place + sign * hop + n) % n} for hop in range(1, n)]
    for peer in peers:
        pl.semaphore_signal(barrier, inc=1, device_id=peer, device_id_type=MESH)
    rows, width = a_ref.shape
    length = rows // 8
    lanes = range(width // 128)
    for k in lanes:
        fa[k * rows : (k + 1) * rows] = a_ref[:, k * 128 : (k + 1) * 128]
        fb[k * rows : (k + 1) * rows] = b_ref[:, k * 128 : (k + 1) * 128]

    def at(k, r):
        return pl.ds(k * rows + (length - 1 - r if reverse else r), 8, stride=length)

    def local(r, carry):
        result = []
        for k in lanes:
            prod, state = carry[k]
            decay = fa[at(k, r), :]
            term = fb[at(k, r), :]
            if reverse:
                fa[at(k, r), :] = prod
                total = term + state
                fb[at(k, r), :] = total
                result.append((prod * decay, decay * total))
            else:
                prod = prod * decay
                state = decay * state + term
                fa[at(k, r), :] = prod
                fb[at(k, r), :] = state
                result.append((prod, state))
        return result

    start = [(jnp.ones((8, 128), jnp.float32), jnp.zeros((8, 128), jnp.float32)) for k in lanes]
    ends = lax.fori_loop(0, length, local, start, unroll=2)
    prod = jnp.concatenate([end[0] for end in ends], axis=1)
    state = jnp.concatenate([end[1] for end in ends], axis=1)
    order = range(7, -1, -1) if reverse else range(8)
    run_a, run_b = jnp.ones((1, width), jnp.float32), jnp.zeros((1, width), jnp.float32)
    before = [None] * 8
    for s in order:
        before[s] = (run_a, run_b)
        pa, pb = prod[s : s + 1], state[s : s + 1]
        run_a, run_b = pa * run_a, pa * run_b + pb
    mine[0:1] = run_a
    mine[1:2] = run_b
    pl.semaphore_wait(barrier, n - 1)
    copies = [
        send(mine, others.at[hop - 1], ssem.at[hop - 1], rsem.at[hop - 1], peers[hop - 1])
        for hop in range(1, n)
    ]
    carry = jnp.zeros((1, width), jnp.float32)
    ahead = n - 1 - place if reverse else place
    for copy in copies:
        copy.wait_recv()
    for hop in range(n - 1, 0, -1):
        step = others[hop - 1, 0:1] * carry + others[hop - 1, 1:2]
        carry = jnp.where(hop <= ahead, step, carry)
    edge_ref[...] = carry
    entering = jnp.concatenate([pa * carry + pb for pa, pb in before], axis=0)

    def fix(r, c):
        for k in lanes:
            fb[at(k, r), :] = fb[at(k, r), :] + fa[at(k, r), :] * entering[:, k * 128 : (k + 1) * 128]
        return c

    lax.fori_loop(0, length, fix, 0, unroll=2)
    for k in lanes:
        out_ref[:, k * 128 : (k + 1) * 128] = fb[k * rows : (k + 1) * rows]
    for copy in copies:
        copy.wait_send()


def scan_stream(decay, term, reverse):
    n = lax.axis_size("dp")
    rows, width = decay.shape
    vmem = pl.BlockSpec(memory_space=pltpu.VMEM)
    return pl.pallas_call(
        functools.partial(scan_kernel, n, reverse),
        name="scan_back" if reverse else "scan",
        out_shape=(
            jax.ShapeDtypeStruct((rows, width), jnp.float32),
            jax.ShapeDtypeStruct((1, width), jnp.float32),
        ),
        in_specs=[vmem, vmem],
        out_specs=(vmem, vmem),
        scratch_shapes=[
            pltpu.VMEM((rows * width // 128, 128), jnp.float32),
            pltpu.VMEM((rows * width // 128, 128), jnp.float32),
            pltpu.VMEM((2, width), jnp.float32),
            pltpu.VMEM((n - 1, 2, width), jnp.float32),
            pltpu.SemaphoreType.DMA((n - 1,)),
            pltpu.SemaphoreType.DMA((n - 1,)),
        ],
        compiler_params=pltpu.CompilerParams(
            collective_id=5 if reverse else 4, has_side_effects=True, vmem_limit_bytes=32 * 2**20
        ),
    )(decay, term)


def in_order(bit, mine, theirs, axis=0):
    return jnp.where(
        bit == 0, jnp.concatenate([mine, theirs], axis), jnp.concatenate([theirs, mine], axis)
    )


def four_in_order(place, pieces):
    low, high = place % 2, (place // 2) % 2
    same = in_order(low, pieces[0], pieces[1])
    other = in_order(low, pieces[2], pieces[3])
    return in_order(high, same, other)


def weight_columns(weight):
    place = lax.axis_index("dp")
    held = weight[None]
    for step in range((lax.axis_size("dp") // GROUP).bit_length() - 1):
        held = in_order((place // (GROUP << step)) % 2, held, flipped(held, "dp", GROUP << step))
    blocks, rows, width = held.shape
    share = width // GROUP
    cut = held.reshape(blocks * rows, GROUP, share).transpose(1, 0, 2)
    spot = place % GROUP
    pieces = [
        flipped(lax.dynamic_index_in_dim(cut, spot ^ m, 0), "dp", m)
        if m
        else lax.dynamic_index_in_dim(cut, spot, 0)
        for m in range(GROUP)
    ]
    full = four_in_order(spot, pieces).reshape(GROUP, blocks, rows, share)
    return full.transpose(1, 0, 2, 3).reshape(blocks * GROUP * rows, share)


def weight_rows(grad):
    place = lax.axis_index("dp")
    blocks = lax.axis_size("dp") // GROUP
    held = grad.astype(jnp.bfloat16)
    for step in reversed(range(blocks.bit_length() - 1)):
        bit = (place // (GROUP << step)) % 2
        halves = held.reshape(2, held.shape[0] // 2, held.shape[1])
        keep = lax.dynamic_index_in_dim(halves, bit, 0, False)
        away = lax.dynamic_index_in_dim(halves, 1 - bit, 0, False)
        came = flipped(away, "dp", GROUP << step)
        held = (keep.astype(jnp.float32) + came.astype(jnp.float32)).astype(jnp.bfloat16)
    rows = held.shape[0] // GROUP
    cut = held.reshape(GROUP, rows, held.shape[1])
    spot = place % GROUP
    pieces = [
        flipped(lax.dynamic_index_in_dim(cut, spot ^ m, 0), "dp", m)
        if m
        else lax.dynamic_index_in_dim(cut, spot, 0)
        for m in range(GROUP)
    ]
    full = four_in_order(spot, pieces)
    return full.transpose(1, 0, 2).reshape(rows, GROUP * held.shape[1]).astype(jnp.float32)


def local(
    tokens,
    doc_start,
    norm1_gain,
    proj_x,
    proj_y,
    conv_weight,
    conv_bias,
    gate_x_weight,
    gate_x_bias,
    gate_a_weight,
    gate_a_bias,
    decay_param,
    proj_out,
    norm2_gain,
    mlp_gate,
    mlp_up,
    mlp_down,
    cotangent,
):
    tok_rows = tokens.shape[0]
    chan_width = proj_x.shape[1]
    block_width = gate_x_weight.shape[0]
    half_width = block_width // 2
    tap_count = conv_weight.shape[0]
    parity = lax.axis_index("tensor") % 2
    full_start = parity * half_width
    shared_start = (1 - parity) * 2 * block_width
    tensor_size = lax.axis_size("tensor")
    share_rows = tok_rows // tensor_size
    own_start = lax.axis_index("tensor") * share_rows
    positions = lax.axis_index("dp") * tok_rows + lax.iota(jnp.int32, tok_rows)
    starting = (doc_start == positions)[:, None]
    groups = [
        [(g * GROUP + i) * tensor_size + t for i in range(GROUP) for t in range(tensor_size)]
        for g in range(lax.axis_size("dp") // GROUP)
    ]
    everyone = ("dp", "tensor")

    gate_cols = weight_columns(mlp_gate)
    up_cols = weight_columns(mlp_up)
    down_cols = weight_columns(mlp_down)
    tok_own = lax.dynamic_slice_in_dim(tokens, own_start, share_rows, 0)
    cot_own = lax.dynamic_slice_in_dim(cotangent, own_start, share_rows, 0)
    cot_all = lax.all_gather(cot_own, everyone, axis_index_groups=groups, tiled=True)

    def normalize(values):
        values = values.astype(jnp.float32)
        inv_rms = lax.rsqrt(jnp.mean(values * values, axis=-1, keepdims=True) + epsilon)
        return (values * inv_rms * norm1_gain).astype(jnp.bfloat16)

    halo = 16
    normed_low = normalize(tokens)
    normed_prev = normalize(shifted(tokens[tok_rows - halo :], "dp", 1))
    branch_y = matmul(normed_low, proj_y)
    branch_x = matmul(normed_low, proj_x).astype(jnp.bfloat16)
    prev_x = matmul(normed_prev, proj_x).astype(jnp.bfloat16)
    extended = jnp.concatenate([prev_x[halo - tap_count + 1 :], branch_x], axis=0).astype(
        jnp.float32
    )

    def conv_apply(ext_rows, weight, bias_vec):
        conv_out = bias_vec + weight[0] * ext_rows[tap_count - 1 :]
        for offset in range(1, tap_count):
            inside = (positions - offset >= doc_start).astype(jnp.float32)[:, None]
            lagged = ext_rows[tap_count - 1 - offset : tap_count - 1 - offset + tok_rows]
            conv_out = conv_out + weight[offset] * lagged * inside
        return conv_out

    conv_out, conv_pull = jax.vjp(conv_apply, extended, conv_weight, conv_bias)
    mixed_low = conv_out.astype(jnp.bfloat16)
    own_half = lax.dynamic_slice_in_dim(mixed_low, shared_start, half_width, 1)
    other_half = flipped(own_half, "tensor", 1)
    shared_in = in_order(parity, own_half, other_half, 1)
    full_in = lax.dynamic_slice_in_dim(mixed_low, full_start, 2 * block_width, 1).reshape(
        tok_rows, 2, block_width
    )

    def place(full_part, shared_part):
        return in_order(parity, full_part, shared_part, 1)

    def full_weight(weight):
        return lax.dynamic_slice_in_dim(weight, full_start, 2 * block_width, 1).reshape(
            block_width, 2, block_width
        )

    def shared_weight(weight):
        return lax.dynamic_slice_in_dim(weight, shared_start, half_width, 1)

    def gate_pre(weight, bias_vec):
        full_out = jnp.einsum(
            "nhi,ihj->nhj", full_in, full_weight(weight), preferred_element_type=jnp.float32
        ).reshape(tok_rows, 2 * block_width)
        shared_out = matmul(shared_in, shared_weight(weight))
        return place(full_out, shared_out) + bias_vec

    def recurrence_in(conv_vals, pre_input, pre_recur, param_vec):
        log_decay = -8.0 * jax.nn.sigmoid(pre_recur) * jax.nn.softplus(param_vec)
        decay = jnp.where(starting, 0.0, jnp.exp(log_decay))
        multiplier = jnp.where(starting, 1.0, jnp.sqrt(-jnp.expm1(2.0 * log_decay)))
        return (decay, multiplier * jax.nn.sigmoid(pre_input) * conv_vals)

    pre_input = gate_pre(gate_x_weight, gate_x_bias)
    pre_recur = gate_pre(gate_a_weight, gate_a_bias)
    (decay, drive), recur_pull = jax.vjp(
        recurrence_in, mixed_low.astype(jnp.float32), pre_input, pre_recur, decay_param
    )
    states, entering = scan_stream(decay, drive, False)
    previous = jnp.concatenate([entering, states[:-1]], axis=0)
    gelu_y, gelu_pull = jax.vjp(gelu_tanh, branch_y)
    product_low = (states * gelu_y).astype(jnp.bfloat16)
    resid, normed2_all = middle(
        matmul(product_low, proj_out).astype(jnp.bfloat16), tok_own, norm2_gain
    )
    normed2_all = normed2_all.reshape(GROUP * tok_rows, -1)
    gate_act = matmul(normed2_all, gate_cols)
    up_act = matmul(normed2_all, up_cols)
    hidden, act_pull = jax.vjp(gated_product, gate_act, up_act)
    hidden_low = hidden.astype(jnp.bfloat16)
    grad_hidden = matmul(cot_all, down_cols)
    grad_gate, grad_up = act_pull(grad_hidden)
    grad_gate_low = grad_gate.astype(jnp.bfloat16)
    grad_up_low = grad_up.astype(jnp.bfloat16)
    grad_resid, grad_lru_low, grad_gain2 = back_pass(
        (contract_last(grad_gate_low, gate_cols) + contract_last(grad_up_low, up_cols)).astype(
            jnp.bfloat16
        ),
        resid,
        cot_own,
        norm2_gain,
    )
    grad_lru_low = grad_lru_low.reshape(tok_rows, -1)
    block_out = resid + lax.psum_scatter(
        contract_last(hidden_low, down_cols).astype(jnp.bfloat16),
        everyone,
        axis_index_groups=groups,
        scatter_dimension=0,
        tiled=True,
    ).astype(jnp.float32)
    grad_mlp_down = weight_rows(contract_first(cot_all, hidden_low))
    grad_mlp_gate = weight_rows(contract_first(normed2_all, grad_gate_low))
    grad_mlp_up = weight_rows(contract_first(normed2_all, grad_up_low))

    def scatter_grads(operand_pairs):
        pieces = [contract_first(left_rows, right_rows) for left_rows, right_rows in operand_pairs]
        return lax.psum_scatter(
            jnp.concatenate(pieces, axis=1).astype(jnp.bfloat16),
            "dp",
            scatter_dimension=0,
            tiled=True,
        ).astype(jnp.float32)

    grad_product = contract_last(grad_lru_low, proj_out)
    grad_states = grad_product * gelu_y
    grad_y_low = gelu_pull(grad_product * states)[0].astype(jnp.bfloat16)
    early = scatter_grads([(normed_low, grad_y_low), (grad_lru_low, product_low)])
    grad_proj_y = early[:, :chan_width]
    grad_proj_out = early[:, chan_width:].T
    total_grad, _ = scan_stream(decay, grad_states, True)
    conv_direct, grad_pre_input, grad_pre_recur, grad_param = recur_pull(
        (total_grad * previous, total_grad)
    )

    def gate_back(weight, grad_pre):
        grad_pre_low = grad_pre.astype(jnp.bfloat16)
        grad_full = lax.dynamic_slice_in_dim(grad_pre_low, full_start, 2 * block_width, 1).reshape(
            tok_rows, 2, block_width
        )
        grad_share = lax.dynamic_slice_in_dim(grad_pre_low, shared_start, half_width, 1)
        into_full = jnp.einsum(
            "nhj,ihj->nhi", grad_full, full_weight(weight), preferred_element_type=jnp.float32
        ).reshape(tok_rows, 2 * block_width)
        into_share = contract_last(grad_share, shared_weight(weight))
        weight_full = jnp.einsum(
            "nhi,nhj->ihj", full_in, grad_full, preferred_element_type=jnp.float32
        ).reshape(block_width, 2 * block_width)
        weight_share = contract_first(shared_in, grad_share)
        return (into_full, into_share, place(weight_full, weight_share))

    input_full, input_share, grad_gx_weight = gate_back(gate_x_weight, grad_pre_input)
    recur_full, recur_share, grad_ga_weight = gate_back(gate_a_weight, grad_pre_recur)
    full_sum = input_full + recur_full
    share_sum = input_share + recur_share
    own_grad = jnp.where(parity == 0, share_sum[:, :half_width], share_sum[:, half_width:])
    other_grad = jnp.where(parity == 0, share_sum[:, half_width:], share_sum[:, :half_width])
    returned = flipped(other_grad.astype(jnp.bfloat16), "tensor", 1).astype(other_grad.dtype)
    grad_conv = conv_direct + place(full_sum, own_grad + returned)
    grad_extended, grad_conv_weight, grad_conv_bias = conv_pull(grad_conv)
    rim_grad = shifted(grad_extended[: tap_count - 1], "dp", -1)
    grad_branch_x = grad_extended[tap_count - 1 :] + jnp.concatenate(
        [jnp.zeros((tok_rows - tap_count + 1, chan_width), jnp.float32), rim_grad], axis=0
    )
    grad_x_low = grad_branch_x.astype(jnp.bfloat16)
    grad_tokens, grad_gain1 = last_pass(
        (contract_last(grad_x_low, proj_x) + contract_last(grad_y_low, proj_y)).astype(
            jnp.bfloat16
        ),
        tok_own,
        grad_resid,
        norm1_gain,
    )
    grad_proj_x = scatter_grads([(normed_low, grad_x_low)])

    gains = lax.psum(
        jnp.concatenate([grad_gain1, grad_gain2], axis=0).astype(jnp.bfloat16), everyone
    ).astype(jnp.float32)
    small = lax.psum(
        jnp.concatenate(
            [
                grad_conv_weight,
                grad_conv_bias[None],
                jnp.sum(grad_pre_input, axis=0)[None],
                jnp.sum(grad_pre_recur, axis=0)[None],
                grad_param[None],
            ],
            axis=0,
        ).astype(jnp.bfloat16),
        "dp",
    ).astype(jnp.float32)
    wide = lax.psum(
        jnp.concatenate([grad_gx_weight, grad_ga_weight], axis=0).astype(jnp.bfloat16), "dp"
    ).astype(jnp.float32)
    return (
        block_out,
        grad_tokens,
        gains[0],
        grad_proj_x,
        grad_proj_y,
        small[:tap_count],
        small[tap_count],
        wide[:block_width],
        small[tap_count + 1],
        wide[block_width:],
        small[tap_count + 2],
        small[tap_count + 3],
        grad_proj_out,
        gains[1],
        grad_mlp_gate,
        grad_mlp_up,
        grad_mlp_down,
    )


def solution(mesh):
    placed = (
        P("dp", None),
        P("dp"),
        P(),
        P(None, "tensor"),
        P(None, "tensor"),
        P(None, "tensor"),
        P("tensor"),
        P(None, "tensor"),
        P("tensor"),
        P(None, "tensor"),
        P("tensor"),
        P("tensor"),
        P("tensor", None),
        P(),
        P("dp", "tensor"),
        P("dp", "tensor"),
        P("dp", "tensor"),
        P("dp", None),
    )
    return jax.shard_map(
        local,
        mesh=mesh,
        in_specs=placed,
        out_specs=(
            P(("dp", "tensor"), None),
            P(("dp", "tensor"), None),
            P(),
            P("dp", "tensor"),
            P("dp", "tensor"),
            P(None, "tensor"),
            P("tensor"),
            P(None, "tensor"),
            P("tensor"),
            P(None, "tensor"),
            P("tensor"),
            P("tensor"),
            P("tensor", "dp"),
            P(),
            P("dp", "tensor"),
            P("dp", "tensor"),
            P("dp", "tensor"),
        ),
        check_vma=False,
    )
```

```python
import functools

import jax
import jax.numpy as jnp
from jax import lax
from jax.experimental import pallas as pl
from jax.experimental.pallas import tpu as pltpu
from jax.sharding import PartitionSpec as P

epsilon = 1e-06
MESH = pl.DeviceIdType.MESH
GROUP = 4
LINKS = (("dp", 1), ("dp", 0), ("tensor", 1))
CORE = ("tensor", 0)
ORDERS = ((1, 2, 0), (2, 0, 1), (0, 1, 2))


def gelu_tanh(values):
    return jax.nn.gelu(values, approximate=True)


def gated_product(gate_vals, up_vals):
    return gelu_tanh(gate_vals) * up_vals


def contract_last(left_rows, right_rows):
    return lax.dot_general(
        left_rows, right_rows, (((1,), (1,)), ((), ())), preferred_element_type=jnp.float32
    )


def contract_first(left_rows, right_rows):
    return lax.dot_general(
        left_rows, right_rows, (((0,), (0,)), ((), ())), preferred_element_type=jnp.float32
    )


def matmul(left_rows, right_rows):
    return jnp.dot(left_rows, right_rows, preferred_element_type=jnp.float32)


def shifted(block, axis, distance):
    devices = range(lax.axis_size(axis))
    route = [(i - distance, i) for i in devices if i - distance in devices]
    return lax.ppermute(block, axis, route)


def flipped(array, axis, mask):
    return lax.ppermute(array, axis, [(i, i ^ mask) for i in range(lax.axis_size(axis))])


def bit_of(axis, bit):
    return (lax.axis_index(axis) // (1 << bit)) % 2


def across(axis, bit):
    index = lax.axis_index(axis)
    return {axis: index + (1 - 2 * ((index // (1 << bit)) % 2)) * (1 << bit)}


def thirds(width):
    tiles = width // 128
    spans, start = [], 0
    for k in range(3):
        count = (tiles + 2 - k) // 3
        spans.append((start * 128, count * 128))
        start += count
    return spans


def send(src, dst, send_sem, recv_sem, device):
    copy = pltpu.make_async_remote_copy(
        src_ref=src,
        dst_ref=dst,
        send_sem=send_sem,
        recv_sem=recv_sem,
        device_id=device,
        device_id_type=MESH,
    )
    copy.start()
    return copy


def greet(devices):
    barrier = pltpu.get_barrier_semaphore()
    for device in devices:
        pl.semaphore_signal(barrier, inc=1, device_id=device, device_id_type=MESH)
    pl.semaphore_wait(barrier, len(devices))


class Gather:
    def __init__(self, x_ref, out_ref, send_sem, recv_sem, core_send, core_recv, own_sem):
        self.sems = send_sem, recv_sem, core_send, core_recv
        self.out = out_ref
        self.me = [bit_of(*link) for link in LINKS]
        self.core = bit_of(*CORE)
        self.peers = [across(*link) for link in LINKS]
        self.core_peer = across(*CORE)
        self.spans = thirds(x_ref.shape[1])
        me, place = self.me, out_ref.at[self.me[0], self.me[1], self.me[2], self.core]
        self.own = pltpu.make_async_copy(x_ref, place, own_sem)
        self.own.start()
        self.moving = [
            send(
                x_ref.at[:, pl.ds(*self.spans[k])],
                self.region(me, k),
                send_sem.at[k, 0],
                recv_sem.at[k, 0],
                self.peers[ORDERS[k][0]],
            )
            for k in range(3)
        ]
        self.to_core = [send(x_ref, place, core_send.at[9], core_recv.at[9], self.core_peer)]
        self.sent = []

    def region(self, idx, k):
        return self.out.at[idx[0], idx[1], idx[2], self.core, :, pl.ds(*self.spans[k])]

    def step(self, step):
        send_sem, recv_sem, core_send, core_recv = self.sems
        me = self.me
        if step == 0:
            self.own.wait()
        for k in range(3):
            order = ORDERS[k]
            self.moving[k].wait_recv()
            self.sent.append(self.moving[k])
            if step < 2:
                held = [slice(None) if d in order[: step + 1] else me[d] for d in range(3)]
                self.moving[k] = send(
                    self.region(held, k),
                    self.region(held, k),
                    send_sem.at[k, step + 1],
                    recv_sem.at[k, step + 1],
                    self.peers[order[step + 1]],
                )
            fresh = [
                slice(None) if d in order[:step] else (1 - me[d] if d == order[step] else me[d])
                for d in range(3)
            ]
            self.to_core.append(
                send(
                    self.region(fresh, k),
                    self.region(fresh, k),
                    core_send.at[3 * step + k],
                    core_recv.at[3 * step + k],
                    self.core_peer,
                )
            )

    def finish(self):
        for copy in self.sent:
            copy.wait_send()
        for copy in self.to_core:
            copy.wait()


def group_peers():
    index = lax.axis_index("dp")
    spot = index % GROUP
    base = index - spot
    spots = (spot + 1 - 2 * (spot % 2), spot + 2 - 4 * (spot // 2), GROUP - 1 - spot)
    return spot, spots, [{"dp": base + other} for other in spots]


def share_width(width):
    return -(-width // (128 * GROUP)) * 128


def overlap_of(width):
    return GROUP * share_width(width) - width


class Spread:
    def __init__(self, weight_ref, out_ref, stage, send_sem, recv_sem, own_sem):
        spot, spots, peers = group_peers()
        width = weight_ref.shape[1]
        share, over = share_width(width), overlap_of(width)

        def columns(place):
            start = share * place - over * (place // (GROUP - 1))
            return weight_ref.at[:, pl.ds(pl.multiple_of(start, 128), share)]

        self.copies = [
            send(columns(spots[m]), out_ref.at[spot], send_sem.at[m], recv_sem.at[m], peers[m])
            for m in range(GROUP - 1)
        ]
        self.own_in = pltpu.make_async_copy(columns(spot), stage, own_sem.at[0])
        self.own_out = pltpu.make_async_copy(stage, out_ref.at[spot], own_sem.at[1])
        self.own_in.start()

    def finish(self):
        self.own_in.wait()
        self.own_out.start()
        for copy in self.copies:
            copy.wait()
        self.own_out.wait()


def spread_scratch(rows, share):
    return [
        pltpu.VMEM((rows, share), jnp.bfloat16),
        pltpu.SemaphoreType.DMA((GROUP - 1,)),
        pltpu.SemaphoreType.DMA((GROUP - 1,)),
        pltpu.SemaphoreType.DMA((2,)),
    ]


def spread_shape(weight):
    return jax.ShapeDtypeStruct((GROUP, weight.shape[0], share_width(weight.shape[1])), jnp.bfloat16)


def spread_kernel(weight_ref, out_ref, *scratch):
    greet(group_peers()[2])
    Spread(weight_ref, out_ref, *scratch).finish()


def spread(weight):
    return pl.pallas_call(
        spread_kernel,
        name="spread",
        out_shape=spread_shape(weight),
        in_specs=[pl.BlockSpec(memory_space=pl.ANY)],
        out_specs=pl.BlockSpec(memory_space=pl.ANY),
        scratch_shapes=spread_scratch(weight.shape[0], share_width(weight.shape[1])),
        compiler_params=pltpu.CompilerParams(collective_id=6, has_side_effects=True),
    )(weight)


def collect_kernel(part_ref, out_ref, slots, send_sem, recv_sem, own_sem):
    spot, spots, peers = group_peers()
    greet(peers)
    copies = [
        send(part_ref.at[spots[m]], slots.at[spot], send_sem.at[m], recv_sem.at[m], peers[m])
        for m in range(GROUP - 1)
    ]
    own = pltpu.make_async_copy(part_ref.at[spot], slots.at[spot], own_sem)
    own.start()
    own.wait()
    for copy in copies:
        copy.wait()
    width = out_ref.shape[1]
    share, over = share_width(width), overlap_of(width)
    for place in range(GROUP):
        skip = over * (place // (GROUP - 1))
        out_ref[:, share * place : min(share * (place + 1), width)] = slots[
            place, :, skip:share
        ].astype(jnp.float32)


def collect(part, width):
    rows, share = part.shape[0] // GROUP, part.shape[1]
    return pl.pallas_call(
        collect_kernel,
        name="collect",
        out_shape=jax.ShapeDtypeStruct((rows, width), jnp.float32),
        in_specs=[pl.BlockSpec(memory_space=pl.ANY)],
        out_specs=pl.BlockSpec(memory_space=pltpu.VMEM),
        scratch_shapes=[
            pltpu.VMEM((GROUP, rows, share), jnp.bfloat16),
            pltpu.SemaphoreType.DMA((GROUP - 1,)),
            pltpu.SemaphoreType.DMA((GROUP - 1,)),
            pltpu.SemaphoreType.DMA,
        ],
        compiler_params=pltpu.CompilerParams(
            collective_id=7, has_side_effects=True, vmem_limit_bytes=24 * 2**20
        ),
    )(part.reshape(GROUP, rows, share))


def final_kernel(n, bits, small_ref, gain1_ref, gain2_ref, all_ref, gains_ref, came, ssem, rsem, gs, gr):
    place = lax.axis_index("dp")
    peers = [{"dp": (place + hop) % n} for hop in range(1, n)]
    greet(peers + [across("tensor", bit) for axis, bit in bits if axis == "tensor"])
    copies = [
        send(small_ref, all_ref.at[place], ssem.at[hop], rsem.at[hop], peers[hop])
        for hop in range(n - 1)
    ]
    all_ref[place] = small_ref[...]
    gains_ref[0:1] = gain1_ref[...]
    gains_ref[1:2] = gain2_ref[...]
    for step, (axis, bit) in enumerate(bits):
        copy = send(gains_ref, came.at[step], gs.at[step], gr.at[step], across(axis, bit))
        copy.wait()
        gains_ref[...] = gains_ref[...] + came[step]
    for copy in copies:
        copy.wait()


def final_pass(small, gain1, gain2):
    n = lax.axis_size("dp")
    bits = [
        (axis, bit)
        for axis in ("tensor", "dp")
        for bit in range(lax.axis_size(axis).bit_length() - 1)
    ]
    rows, width = small.shape
    vmem = pl.BlockSpec(memory_space=pltpu.VMEM)
    gains = (2, gain1.shape[1])
    return pl.pallas_call(
        functools.partial(final_kernel, n, bits),
        name="final",
        out_shape=(
            jax.ShapeDtypeStruct((n, rows, width), small.dtype),
            jax.ShapeDtypeStruct(gains, jnp.float32),
        ),
        in_specs=[vmem] * 3,
        out_specs=(vmem, vmem),
        scratch_shapes=[
            pltpu.VMEM((len(bits), *gains), jnp.float32),
            pltpu.SemaphoreType.DMA((n - 1,)),
            pltpu.SemaphoreType.DMA((n - 1,)),
            pltpu.SemaphoreType.DMA((len(bits),)),
            pltpu.SemaphoreType.DMA((len(bits),)),
        ],
        compiler_params=pltpu.CompilerParams(
            collective_id=8, has_side_effects=True, vmem_limit_bytes=16 * 2**20
        ),
    )(small, gain1, gain2)


GATHER_SEMS = [
    pltpu.SemaphoreType.DMA((3, 3)),
    pltpu.SemaphoreType.DMA((3, 3)),
    pltpu.SemaphoreType.DMA((10,)),
    pltpu.SemaphoreType.DMA((10,)),
    pltpu.SemaphoreType.DMA,
]


class SumTensor:
    def __init__(self, part_ref, q, core_buf, link_buf, sems_s, sems_r, own_sem):
        high, core = bit_of(*LINKS[2]), bit_of(*CORE)
        core_peer = across(*CORE)
        self.args = high, q, core_buf, link_buf, sems_s, sems_r
        self.own = pltpu.make_async_copy(part_ref.at[:, core], q, own_sem)
        self.own.start()
        self.copies = [
            send(
                part_ref.at[block, 1 - core],
                core_buf.at[block],
                sems_s.at[i],
                sems_r.at[i],
                core_peer,
            )
            for i, block in enumerate((1 - high, high))
        ]

    def pass_on(self):
        high, q, core_buf, link_buf, sems_s, sems_r = self.args
        self.own.wait()
        self.copies[0].wait_recv()
        q[1 - high] = q[1 - high] + core_buf[1 - high]
        self.copies.append(
            send(q.at[1 - high], link_buf, sems_s.at[2], sems_r.at[2], across(*LINKS[2]))
        )

    def arrive(self):
        self.copies[1].wait_recv()
        self.copies[2].wait_recv()

    def rows(self, rows):
        high, q, core_buf, link_buf, _, _ = self.args
        return (
            q[high, rows].astype(jnp.float32)
            + core_buf[high, rows].astype(jnp.float32)
            + link_buf[rows].astype(jnp.float32)
        )

    def finish(self):
        for copy in self.copies:
            copy.wait_send()


SUM_SEMS = [
    pltpu.SemaphoreType.DMA((3,)),
    pltpu.SemaphoreType.DMA((3,)),
    pltpu.SemaphoreType.DMA,
]
STRIP = 16


def middle_kernel(
    part_ref, tok_ref, cot_ref, gain_ref, weight_ref, resid_ref, all_ref, cot_all_ref, share_ref,
    q, core_buf, link_buf, low, *sems
):
    sum_sems, gather_sems, cot_sems, spread_sems = sems[:3], sems[3:8], sems[8:13], sems[13:]
    _, _, four = group_peers()
    greet([across(*link) for link in LINKS] + [across(*CORE), four[2]])
    total = SumTensor(part_ref, q, core_buf, link_buf, *sum_sems)
    cots = Gather(cot_ref, cot_all_ref, *cot_sems)
    total.pass_on()
    shares = Spread(weight_ref, share_ref, *spread_sems)
    cots.step(0)
    total.arrive()

    def strip(i, carry):
        rows = pl.ds(pl.multiple_of(i * STRIP, STRIP), STRIP)
        resid = tok_ref[rows].astype(jnp.float32) + total.rows(rows)
        resid_ref[rows] = resid
        inv = lax.rsqrt(jnp.mean(resid * resid, axis=-1, keepdims=True) + epsilon)
        low[rows] = (resid * inv * gain_ref[...]).astype(low.dtype)
        return carry

    lax.fori_loop(0, tok_ref.shape[0] // STRIP, strip, 0)
    total.finish()
    blocks = Gather(low, all_ref, *gather_sems)
    cots.step(1)
    blocks.step(0)
    cots.step(2)
    blocks.step(1)
    blocks.step(2)
    shares.finish()
    cots.finish()
    blocks.finish()


def middle(part, tok, cot, gain, weight):
    rows, width = tok.shape
    vmem, anywhere = pl.BlockSpec(memory_space=pltpu.VMEM), pl.BlockSpec(memory_space=pl.ANY)
    every = jax.ShapeDtypeStruct((2, 2, 2, 2, rows, width), jnp.bfloat16)
    return pl.pallas_call(
        middle_kernel,
        name="middle",
        out_shape=(
            jax.ShapeDtypeStruct((rows, width), jnp.float32),
            every,
            every,
            spread_shape(weight),
        ),
        in_specs=[anywhere, vmem, vmem, vmem, anywhere],
        out_specs=(vmem, anywhere, anywhere, anywhere),
        scratch_shapes=[
            pltpu.VMEM((2, rows, width), jnp.bfloat16),
            pltpu.VMEM((2, rows, width), jnp.bfloat16),
            pltpu.VMEM((rows, width), jnp.bfloat16),
            pltpu.VMEM((rows, width), jnp.bfloat16),
            *SUM_SEMS,
            *GATHER_SEMS,
            *GATHER_SEMS,
            *spread_scratch(weight.shape[0], share_width(weight.shape[1])),
        ],
        compiler_params=pltpu.CompilerParams(
            collective_id=1, has_side_effects=True, vmem_limit_bytes=32 * 2**20
        ),
    )(part.reshape(2, 2, rows, width), tok, cot, gain.reshape(1, width), weight)


def norm_back(rows, back, base_ref, gain_ref, keep_ref, gain_acc):
    base = base_ref[rows].astype(jnp.float32)
    inv = lax.rsqrt(jnp.mean(base * base, axis=-1, keepdims=True) + epsilon)
    unit = base * inv
    scaled = gain_ref[...] * back
    grad = inv * (scaled - unit * jnp.mean(unit * scaled, axis=-1, keepdims=True))
    terms = back * unit
    gain_acc[...] += terms[:8] + terms[8:]
    return keep_ref[rows].astype(jnp.float32) + grad


def back_kernel(
    p_ref, resid_ref, cot_ref, gain_ref, grad_ref, all_ref, gain_out,
    q, cb, r0, r1, r2, low, gain_acc, ssem, rsem, fs, fr, own_sem, gs, gr, gather_own
):
    me = [bit_of(*link) for link in LINKS]
    core = bit_of(*CORE)
    peers = [across(*link) for link in LINKS]
    core_peer = across(*CORE)
    spans = thirds(q.shape[-1])
    own = pltpu.make_async_copy(p_ref.at[:, :, :, core], q, own_sem)
    own.start()
    greet(peers + [core_peer])

    def half(k, near):
        first = ORDERS[k][0]
        return [(me[d] if near else 1 - me[d]) if d == first else slice(None) for d in range(3)]

    to_core = []
    for near in (False, True):
        for k in range(3):
            i = half(k, near)
            to_core.append(
                send(
                    p_ref.at[i[0], i[1], i[2], 1 - core, :, pl.ds(*spans[k])],
                    cb.at[i[0], i[1], i[2], :, pl.ds(*spans[k])],
                    fs.at[len(to_core)],
                    fr.at[len(to_core)],
                    core_peer,
                )
            )
    own.wait()

    def add(i, k, other):
        s, n = spans[k]
        q[i[0], i[1], i[2], :, s : s + n] = q[i[0], i[1], i[2], :, s : s + n] + other

    moving, sent = [], []
    for near in (False, True):
        for k in range(3):
            to_core[3 * near + k].wait_recv()
            i = half(k, near)
            s, n = spans[k]
            add(i, k, cb[i[0], i[1], i[2], :, s : s + n])
            if not near:
                moving.append(
                    send(
                        q.at[i[0], i[1], i[2], :, pl.ds(s, n)],
                        r0.at[:, :, :, pl.ds(s, n)],
                        ssem.at[k, 0],
                        rsem.at[k, 0],
                        peers[ORDERS[k][0]],
                    )
                )
    for step in (1, 2):
        for k in range(3):
            s, n = spans[k]
            order = ORDERS[k]
            moving[k].wait_recv()
            sent.append(moving[k])
            kept = [me[d] if d in order[:step] else slice(None) for d in range(3)]
            add(kept, k, r0[:, :, :, s : s + n] if step == 1 else r1[:, :, s : s + n])
            away = [
                me[d] if d in order[:step] else (1 - me[d] if d == order[step] else slice(None))
                for d in range(3)
            ]
            moving[k] = send(
                q.at[away[0], away[1], away[2], :, pl.ds(s, n)],
                r1.at[:, :, pl.ds(s, n)] if step == 1 else r2.at[:, pl.ds(s, n)],
                ssem.at[k, step],
                rsem.at[k, step],
                peers[order[step]],
            )
    for k in range(3):
        moving[k].wait_recv()
        sent.append(moving[k])
    gain_acc[...] = jnp.zeros_like(gain_acc)

    def strip(i, carry):
        rows = pl.ds(pl.multiple_of(i * STRIP, STRIP), STRIP)
        back = q[me[0], me[1], me[2], rows].astype(jnp.float32) + r2[rows].astype(jnp.float32)
        grad = norm_back(rows, back, resid_ref, gain_ref, cot_ref, gain_acc)
        grad_ref[rows] = grad
        low[rows] = grad.astype(low.dtype)
        return carry

    lax.fori_loop(0, low.shape[0] // STRIP, strip, 0)
    for copy in sent + to_core:
        copy.wait_send()
    gain_out[...] = jnp.sum(gain_acc[...], axis=0, keepdims=True)
    mine = all_ref.at[me[2], core]
    local = pltpu.make_async_copy(low, mine, gather_own)
    local.start()
    along = send(low, mine, gs.at[0], gr.at[0], peers[2])
    beside = send(low, mine, gs.at[1], gr.at[1], core_peer)
    along.wait_recv()
    theirs = all_ref.at[1 - me[2], core]
    onward = send(theirs, theirs, gs.at[2], gr.at[2], core_peer)
    local.wait()
    beside.wait()
    onward.wait()
    along.wait_send()


def back_pass(part, resid, cot, gain):
    rows, width = resid.shape
    wide = lambda *lead: pltpu.VMEM((*lead, rows, width), jnp.bfloat16)
    vmem = pl.BlockSpec(memory_space=pltpu.VMEM)
    return pl.pallas_call(
        back_kernel,
        name="back",
        out_shape=(
            jax.ShapeDtypeStruct((rows, width), jnp.float32),
            jax.ShapeDtypeStruct((2, 2, rows, width), jnp.bfloat16),
            jax.ShapeDtypeStruct((1, width), jnp.float32),
        ),
        in_specs=[pl.BlockSpec(memory_space=pl.ANY), vmem, vmem, vmem],
        out_specs=(vmem, pl.BlockSpec(memory_space=pl.ANY), vmem),
        scratch_shapes=[
            wide(2, 2, 2),
            wide(2, 2, 2),
            wide(2, 2),
            wide(2),
            wide(),
            wide(),
            pltpu.VMEM((8, width), jnp.float32),
            pltpu.SemaphoreType.DMA((3, 3)),
            pltpu.SemaphoreType.DMA((3, 3)),
            pltpu.SemaphoreType.DMA((6,)),
            pltpu.SemaphoreType.DMA((6,)),
            pltpu.SemaphoreType.DMA,
            pltpu.SemaphoreType.DMA((3,)),
            pltpu.SemaphoreType.DMA((3,)),
            pltpu.SemaphoreType.DMA,
        ],
        compiler_params=pltpu.CompilerParams(
            collective_id=2, has_side_effects=True, vmem_limit_bytes=40 * 2**20
        ),
    )(part.reshape(2, 2, 2, 2, rows, width), resid, cot, gain.reshape(1, width))


def last_kernel(
    part_ref, tok_ref, keep_ref, gain_ref, grad_ref, gain_out,
    q, core_buf, link_buf, gain_acc, sum_s, sum_r, sum_own
):
    greet([across(*LINKS[2]), across(*CORE)])
    total = SumTensor(part_ref, q, core_buf, link_buf, sum_s, sum_r, sum_own)
    total.pass_on()
    total.arrive()
    gain_acc[...] = jnp.zeros_like(gain_acc)

    def strip(i, carry):
        rows = pl.ds(pl.multiple_of(i * STRIP, STRIP), STRIP)
        back = total.rows(rows)
        grad_ref[rows] = norm_back(rows, back, tok_ref, gain_ref, keep_ref, gain_acc)
        return carry

    lax.fori_loop(0, tok_ref.shape[0] // STRIP, strip, 0)
    gain_out[...] = jnp.sum(gain_acc[...], axis=0, keepdims=True)
    total.finish()


def last_pass(part, tok, keep, gain):
    rows, width = tok.shape
    vmem = pl.BlockSpec(memory_space=pltpu.VMEM)
    return pl.pallas_call(
        last_kernel,
        name="last",
        out_shape=(
            jax.ShapeDtypeStruct((rows, width), jnp.float32),
            jax.ShapeDtypeStruct((1, width), jnp.float32),
        ),
        in_specs=[pl.BlockSpec(memory_space=pl.ANY), vmem, vmem, vmem],
        out_specs=(vmem, vmem),
        scratch_shapes=[
            pltpu.VMEM((2, rows, width), jnp.bfloat16),
            pltpu.VMEM((2, rows, width), jnp.bfloat16),
            pltpu.VMEM((rows, width), jnp.bfloat16),
            pltpu.VMEM((8, width), jnp.float32),
            *SUM_SEMS,
        ],
        compiler_params=pltpu.CompilerParams(
            collective_id=3, has_side_effects=True, vmem_limit_bytes=32 * 2**20
        ),
    )(part.reshape(2, 2, rows, width), tok, keep, gain.reshape(1, width))


def scan_kernel(n, reverse, *refs):
    if reverse:
        a_ref, b_ref, out_ref, edge_ref, fa, fb, mine, others, ssem, rsem = refs
    else:
        a_ref, b_ref, weight_ref, out_ref, edge_ref, share_ref, *refs = refs
        fa, fb, mine, others, ssem, rsem, *spread_sems = refs
    place = lax.axis_index("dp")
    sign = -1 if reverse else 1
    barrier = pltpu.get_barrier_semaphore()
    peers = [{"dp": (place + sign * hop + n) % n} for hop in range(1, n)]
    for peer in peers:
        pl.semaphore_signal(barrier, inc=1, device_id=peer, device_id_type=MESH)
    rows, width = a_ref.shape
    length = rows // 8
    lanes = range(width // 128)
    for k in lanes:
        fa[k * rows : (k + 1) * rows] = a_ref[:, k * 128 : (k + 1) * 128]
        fb[k * rows : (k + 1) * rows] = b_ref[:, k * 128 : (k + 1) * 128]

    def at(k, r):
        return pl.ds(k * rows + (length - 1 - r if reverse else r), 8, stride=length)

    def local(r, carry):
        result = []
        for k in lanes:
            prod, state = carry[k]
            decay = fa[at(k, r), :]
            term = fb[at(k, r), :]
            if reverse:
                fa[at(k, r), :] = prod
                total = term + state
                fb[at(k, r), :] = total
                result.append((prod * decay, decay * total))
            else:
                prod = prod * decay
                state = decay * state + term
                fa[at(k, r), :] = prod
                fb[at(k, r), :] = state
                result.append((prod, state))
        return result

    start = [(jnp.ones((8, 128), jnp.float32), jnp.zeros((8, 128), jnp.float32)) for k in lanes]
    ends = lax.fori_loop(0, length, local, start, unroll=2)
    prod = jnp.concatenate([end[0] for end in ends], axis=1)
    state = jnp.concatenate([end[1] for end in ends], axis=1)
    order = range(7, -1, -1) if reverse else range(8)
    run_a, run_b = jnp.ones((1, width), jnp.float32), jnp.zeros((1, width), jnp.float32)
    before = [None] * 8
    for s in order:
        before[s] = (run_a, run_b)
        pa, pb = prod[s : s + 1], state[s : s + 1]
        run_a, run_b = pa * run_a, pa * run_b + pb
    mine[0:1] = run_a
    mine[1:2] = run_b
    pl.semaphore_wait(barrier, n - 1)
    copies = [
        send(mine, others.at[hop - 1], ssem.at[hop - 1], rsem.at[hop - 1], peers[hop - 1])
        for hop in range(1, n)
    ]
    if not reverse:
        shares = Spread(weight_ref, share_ref, *spread_sems)
    carry = jnp.zeros((1, width), jnp.float32)
    ahead = n - 1 - place if reverse else place
    for copy in copies:
        copy.wait_recv()
    for hop in range(n - 1, 0, -1):
        step = others[hop - 1, 0:1] * carry + others[hop - 1, 1:2]
        carry = jnp.where(hop <= ahead, step, carry)
    edge_ref[...] = carry
    entering = jnp.concatenate([pa * carry + pb for pa, pb in before], axis=0)

    def fix(r, c):
        for k in lanes:
            fb[at(k, r), :] = fb[at(k, r), :] + fa[at(k, r), :] * entering[:, k * 128 : (k + 1) * 128]
        return c

    lax.fori_loop(0, length, fix, 0, unroll=2)
    for k in lanes:
        out_ref[:, k * 128 : (k + 1) * 128] = fb[k * rows : (k + 1) * rows]
    for copy in copies:
        copy.wait_send()
    if not reverse:
        shares.finish()


def scan_stream(decay, term, weight=None):
    n = lax.axis_size("dp")
    rows, width = decay.shape
    reverse = weight is None
    vmem, anywhere = pl.BlockSpec(memory_space=pltpu.VMEM), pl.BlockSpec(memory_space=pl.ANY)
    out_shape = [
        jax.ShapeDtypeStruct((rows, width), jnp.float32),
        jax.ShapeDtypeStruct((1, width), jnp.float32),
    ]
    scratch = [
        pltpu.VMEM((rows * width // 128, 128), jnp.float32),
        pltpu.VMEM((rows * width // 128, 128), jnp.float32),
        pltpu.VMEM((2, width), jnp.float32),
        pltpu.VMEM((n - 1, 2, width), jnp.float32),
        pltpu.SemaphoreType.DMA((n - 1,)),
        pltpu.SemaphoreType.DMA((n - 1,)),
    ]
    args = [decay, term]
    in_specs, out_specs = [vmem, vmem], [vmem, vmem]
    if not reverse:
        args.append(weight)
        in_specs.append(anywhere)
        out_specs.append(anywhere)
        out_shape.append(spread_shape(weight))
        scratch += spread_scratch(weight.shape[0], share_width(weight.shape[1]))
    return pl.pallas_call(
        functools.partial(scan_kernel, n, reverse),
        name="scan_back" if reverse else "scan",
        out_shape=out_shape,
        in_specs=in_specs,
        out_specs=out_specs,
        scratch_shapes=scratch,
        compiler_params=pltpu.CompilerParams(
            collective_id=5 if reverse else 4, has_side_effects=True, vmem_limit_bytes=32 * 2**20
        ),
    )(*args)


def in_order(bit, mine, theirs, axis=0):
    return jnp.where(
        bit == 0, jnp.concatenate([mine, theirs], axis), jnp.concatenate([theirs, mine], axis)
    )


def halve(blocks, order):
    place = lax.axis_index("dp")
    left = sorted(order, reverse=True)
    assert blocks.shape[0] == 1 << len(left)
    held = blocks.reshape(*[2 for _ in left], *blocks.shape[1:])
    for bit in order:
        axis = left.index(bit)
        mine = (place // (1 << bit)) % 2
        keep = lax.dynamic_index_in_dim(held, mine, axis, False)
        away = lax.dynamic_index_in_dim(held, 1 - mine, axis, False)
        came = flipped(away, "dp", 1 << bit)
        held = (keep.astype(jnp.float32) + came.astype(jnp.float32)).astype(jnp.bfloat16)
        left.remove(bit)
    return held


def local(
    tokens,
    doc_start,
    norm1_gain,
    proj_x,
    proj_y,
    conv_weight,
    conv_bias,
    gate_x_weight,
    gate_x_bias,
    gate_a_weight,
    gate_a_bias,
    decay_param,
    proj_out,
    norm2_gain,
    mlp_gate,
    mlp_up,
    mlp_down,
    cotangent,
):
    tok_rows = tokens.shape[0]
    chan_width = proj_x.shape[1]
    block_width = gate_x_weight.shape[0]
    half_width = block_width // 2
    tap_count = conv_weight.shape[0]
    parity = lax.axis_index("tensor") % 2
    full_start = parity * half_width
    shared_start = (1 - parity) * 2 * block_width
    tensor_size = lax.axis_size("tensor")
    share_rows = tok_rows // tensor_size
    own_start = lax.axis_index("tensor") * share_rows
    positions = lax.axis_index("dp") * tok_rows + lax.iota(jnp.int32, tok_rows)
    starting = (doc_start == positions)[:, None]
    groups = [
        [(g * GROUP + i) * tensor_size + t for i in range(GROUP) for t in range(tensor_size)]
        for g in range(lax.axis_size("dp") // GROUP)
    ]
    everyone = ("dp", "tensor")

    dp_size = lax.axis_size("dp")
    dp_bits = range(dp_size.bit_length() - 1)
    spot = lax.axis_index("dp") % GROUP
    across_blocks = [[i + GROUP * g for g in range(dp_size // GROUP)] for i in range(GROUP)]
    hidden_width = mlp_gate.shape[1]
    share = share_width(hidden_width)

    def all_rows(part):
        flat = part.reshape(-1, share)
        return lax.all_gather(flat, "dp", axis_index_groups=across_blocks, tiled=True)

    gate_cols = all_rows(spread(mlp_gate))
    tok_own = lax.dynamic_slice_in_dim(tokens, own_start, share_rows, 0)
    cot_own = lax.dynamic_slice_in_dim(cotangent, own_start, share_rows, 0)

    def normalize(values):
        values = values.astype(jnp.float32)
        inv_rms = lax.rsqrt(jnp.mean(values * values, axis=-1, keepdims=True) + epsilon)
        return (values * inv_rms * norm1_gain).astype(jnp.bfloat16)

    halo = 16
    normed_low = normalize(tokens)
    normed_prev = normalize(shifted(tokens[tok_rows - halo :], "dp", 1))
    branch_y = matmul(normed_low, proj_y)
    branch_x = matmul(normed_low, proj_x).astype(jnp.bfloat16)
    prev_x = matmul(normed_prev, proj_x).astype(jnp.bfloat16)
    extended = jnp.concatenate([prev_x[halo - tap_count + 1 :], branch_x], axis=0).astype(
        jnp.float32
    )

    def conv_apply(ext_rows, weight, bias_vec):
        conv_out = bias_vec + weight[0] * ext_rows[tap_count - 1 :]
        for offset in range(1, tap_count):
            inside = (positions - offset >= doc_start).astype(jnp.float32)[:, None]
            lagged = ext_rows[tap_count - 1 - offset : tap_count - 1 - offset + tok_rows]
            conv_out = conv_out + weight[offset] * lagged * inside
        return conv_out

    conv_out, conv_pull = jax.vjp(conv_apply, extended, conv_weight, conv_bias)
    mixed_low = conv_out.astype(jnp.bfloat16)
    own_half = lax.dynamic_slice_in_dim(mixed_low, shared_start, half_width, 1)
    other_half = flipped(own_half, "tensor", 1)
    shared_in = in_order(parity, own_half, other_half, 1)
    full_in = lax.dynamic_slice_in_dim(mixed_low, full_start, 2 * block_width, 1).reshape(
        tok_rows, 2, block_width
    )

    def place(full_part, shared_part):
        return in_order(parity, full_part, shared_part, 1)

    def full_weight(weight):
        return lax.dynamic_slice_in_dim(weight, full_start, 2 * block_width, 1).reshape(
            block_width, 2, block_width
        )

    def shared_weight(weight):
        return lax.dynamic_slice_in_dim(weight, shared_start, half_width, 1)

    def gate_pre(weight, bias_vec):
        full_out = jnp.einsum(
            "nhi,ihj->nhj", full_in, full_weight(weight), preferred_element_type=jnp.float32
        ).reshape(tok_rows, 2 * block_width)
        shared_out = matmul(shared_in, shared_weight(weight))
        return place(full_out, shared_out) + bias_vec

    def recurrence_in(conv_vals, pre_input, pre_recur, param_vec):
        log_decay = -8.0 * jax.nn.sigmoid(pre_recur) * jax.nn.softplus(param_vec)
        decay = jnp.where(starting, 0.0, jnp.exp(log_decay))
        multiplier = jnp.where(starting, 1.0, jnp.sqrt(-jnp.expm1(2.0 * log_decay)))
        return (decay, multiplier * jax.nn.sigmoid(pre_input) * conv_vals)

    pre_input = gate_pre(gate_x_weight, gate_x_bias)
    pre_recur = gate_pre(gate_a_weight, gate_a_bias)
    (decay, drive), recur_pull = jax.vjp(
        recurrence_in, mixed_low.astype(jnp.float32), pre_input, pre_recur, decay_param
    )
    states, entering, up_part = scan_stream(decay, drive, mlp_up)
    up_cols = all_rows(up_part)
    previous = jnp.concatenate([entering, states[:-1]], axis=0)
    gelu_y, gelu_pull = jax.vjp(gelu_tanh, branch_y)
    product_low = (states * gelu_y).astype(jnp.bfloat16)
    resid, normed2_all, cot_all, down_part = middle(
        matmul(product_low, proj_out).astype(jnp.bfloat16), tok_own, cot_own, norm2_gain, mlp_down
    )
    down_cols = all_rows(down_part)
    normed2_all = normed2_all.reshape(GROUP * tok_rows, -1)
    cot_all = cot_all.reshape(GROUP * tok_rows, -1)
    counted = lax.iota(jnp.int32, share) >= overlap_of(hidden_width) * (spot // (GROUP - 1))

    def once(values):
        return jnp.where(counted, values, 0.0).astype(jnp.bfloat16)

    gate_act = matmul(normed2_all, gate_cols)
    up_act = matmul(normed2_all, up_cols)
    hidden, act_pull = jax.vjp(gated_product, gate_act, up_act)
    hidden_low = once(hidden)
    grad_hidden = matmul(cot_all, down_cols)
    grad_gate, grad_up = act_pull(grad_hidden)
    grad_gate_low = once(grad_gate)
    grad_up_low = once(grad_up)

    def own_rows(grad):
        return lax.psum_scatter(
            grad.astype(jnp.bfloat16),
            "dp",
            axis_index_groups=across_blocks,
            scatter_dimension=0,
            tiled=True,
        )

    back_part = (
        contract_last(grad_gate_low, gate_cols) + contract_last(grad_up_low, up_cols)
    ).astype(jnp.bfloat16)
    down_grad = contract_first(cot_all, hidden_low).astype(jnp.bfloat16)
    back_part, down_grad = lax.optimization_barrier((back_part, down_grad))
    grad_mlp_down = collect(own_rows(down_grad), hidden_width)
    grad_resid, grad_lru_low, grad_gain2 = back_pass(back_part, resid, cot_own, norm2_gain)
    grad_lru_low = grad_lru_low.reshape(tok_rows, -1)
    grad_mlp_gate = collect(own_rows(contract_first(normed2_all, grad_gate_low)), hidden_width)
    block_out = resid + lax.psum_scatter(
        contract_last(hidden_low, down_cols).astype(jnp.bfloat16),
        everyone,
        axis_index_groups=groups,
        scatter_dimension=0,
        tiled=True,
    ).astype(jnp.float32)

    grad_product = contract_last(grad_lru_low, proj_out)
    grad_states = grad_product * gelu_y
    grad_y_low = gelu_pull(grad_product * states)[0].astype(jnp.bfloat16)
    total_grad, _ = scan_stream(decay, grad_states)
    total_grad, late_y, late_lru, late_up = lax.optimization_barrier(
        (total_grad, grad_y_low, grad_lru_low, grad_up_low)
    )

    def token_sum(left_rows, right_rows):
        return contract_first(left_rows, right_rows).astype(jnp.bfloat16)

    def per_device(rows):
        return rows.reshape(dp_size, rows.shape[0] // dp_size, rows.shape[1])

    up_grad = token_sum(normed2_all, late_up)
    up_rows = halve(up_grad.reshape(dp_size // GROUP, -1, share), list(dp_bits)[:1:-1])
    grad_mlp_up = collect(up_rows, hidden_width)
    low_first, high_first = list(dp_bits), [1, 0, *dp_bits[2:]]
    grad_proj_y = halve(per_device(token_sum(normed_low, late_y)), low_first).astype(jnp.float32)
    grad_proj_out = (
        halve(per_device(token_sum(late_lru, product_low)), high_first).astype(jnp.float32).T
    )
    conv_direct, grad_pre_input, grad_pre_recur, grad_param = recur_pull(
        (total_grad * previous, total_grad)
    )

    def gate_back(weight, grad_pre):
        grad_pre_low = grad_pre.astype(jnp.bfloat16)
        grad_full = lax.dynamic_slice_in_dim(grad_pre_low, full_start, 2 * block_width, 1).reshape(
            tok_rows, 2, block_width
        )
        grad_share = lax.dynamic_slice_in_dim(grad_pre_low, shared_start, half_width, 1)
        into_full = jnp.einsum(
            "nhj,ihj->nhi", grad_full, full_weight(weight), preferred_element_type=jnp.float32
        ).reshape(tok_rows, 2 * block_width)
        into_share = contract_last(grad_share, shared_weight(weight))
        weight_full = jnp.einsum(
            "nhi,nhj->ihj", full_in, grad_full, preferred_element_type=jnp.float32
        ).reshape(block_width, 2 * block_width)
        weight_share = contract_first(shared_in, grad_share)
        return (into_full, into_share, place(weight_full, weight_share))

    input_full, input_share, grad_gx_weight = gate_back(gate_x_weight, grad_pre_input)
    recur_full, recur_share, grad_ga_weight = gate_back(gate_a_weight, grad_pre_recur)
    full_sum = input_full + recur_full
    share_sum = input_share + recur_share
    own_grad = jnp.where(parity == 0, share_sum[:, :half_width], share_sum[:, half_width:])
    other_grad = jnp.where(parity == 0, share_sum[:, half_width:], share_sum[:, :half_width])
    returned = flipped(other_grad.astype(jnp.bfloat16), "tensor", 1).astype(other_grad.dtype)
    grad_conv = conv_direct + place(full_sum, own_grad + returned)
    grad_extended, grad_conv_weight, grad_conv_bias = conv_pull(grad_conv)
    rim_grad = shifted(grad_extended[: tap_count - 1], "dp", -1)
    grad_branch_x = grad_extended[tap_count - 1 :] + jnp.concatenate(
        [jnp.zeros((tok_rows - tap_count + 1, chan_width), jnp.float32), rim_grad], axis=0
    )
    grad_x_low = grad_branch_x.astype(jnp.bfloat16)
    grad_tokens, grad_gain1 = last_pass(
        (contract_last(grad_x_low, proj_x) + contract_last(grad_y_low, proj_y)).astype(
            jnp.bfloat16
        ),
        tok_own,
        grad_resid,
        norm1_gain,
    )
    wide = jnp.concatenate([grad_gx_weight, grad_ga_weight], axis=0)
    sums = jnp.concatenate(
        [
            grad_conv_weight,
            grad_conv_bias[None],
            jnp.sum(grad_pre_input, axis=0)[None],
            jnp.sum(grad_pre_recur, axis=0)[None],
            grad_param[None],
        ],
        axis=0,
    )
    spare = dp_size * 16 - sums.shape[0]
    sums = jnp.concatenate([sums, jnp.zeros((spare, chan_width), jnp.float32)], axis=0)
    blocks = jnp.concatenate(
        [
            per_device(token_sum(normed_low, grad_x_low)),
            per_device(wide.astype(jnp.bfloat16)),
            per_device(sums.astype(jnp.bfloat16)),
        ],
        axis=1,
    )
    split = chan_width // 256 * 128
    reduced = jnp.concatenate(
        [halve(blocks[:, :, :split], low_first), halve(blocks[:, :, split:], high_first)], axis=1
    )
    model_rows = tokens.shape[1] // dp_size
    grad_proj_x = reduced[:model_rows].astype(jnp.float32)
    shared, gains = final_pass(reduced[model_rows:], grad_gain1, grad_gain2)
    wide_rows = 2 * block_width // dp_size
    wide = shared[:, :wide_rows].reshape(2 * block_width, chan_width).astype(jnp.float32)
    small = shared[:, wide_rows:].reshape(dp_size * 16, chan_width).astype(jnp.float32)
    return (
        block_out,
        grad_tokens,
        gains[0],
        grad_proj_x,
        grad_proj_y,
        small[:tap_count],
        small[tap_count],
        wide[:block_width],
        small[tap_count + 1],
        wide[block_width:],
        small[tap_count + 2],
        small[tap_count + 3],
        grad_proj_out,
        gains[1],
        grad_mlp_gate,
        grad_mlp_up,
        grad_mlp_down,
    )


def solution(mesh):
    placed = (
        P("dp", None),
        P("dp"),
        P(),
        P(None, "tensor"),
        P(None, "tensor"),
        P(None, "tensor"),
        P("tensor"),
        P(None, "tensor"),
        P("tensor"),
        P(None, "tensor"),
        P("tensor"),
        P("tensor"),
        P("tensor", None),
        P(),
        P("dp", "tensor"),
        P("dp", "tensor"),
        P("dp", "tensor"),
        P("dp", None),
    )
    return jax.shard_map(
        local,
        mesh=mesh,
        in_specs=placed,
        out_specs=(
            P(("dp", "tensor"), None),
            P(("dp", "tensor"), None),
            P(),
            P("dp", "tensor"),
            P("dp", "tensor"),
            P(None, "tensor"),
            P("tensor"),
            P(None, "tensor"),
            P("tensor"),
            P(None, "tensor"),
            P("tensor"),
            P("tensor"),
            P("tensor", "dp"),
            P(),
            P("dp", "tensor"),
            P("dp", "tensor"),
            P("dp", "tensor"),
        ),
        check_vma=False,
    )
```

```python
import functools

import jax
import jax.numpy as jnp
from jax import lax
from jax.experimental import pallas as pl
from jax.experimental.pallas import tpu as pltpu
from jax.sharding import PartitionSpec as P

epsilon = 1e-06
MESH = pl.DeviceIdType.MESH
GROUP = 4
STRIP = 16
LINKS = (("dp", 1), ("dp", 0), ("tensor", 1))
CORE = ("tensor", 0)
ORDERS = ((1, 2, 0), (2, 0, 1), (0, 1, 2))


def gelu_tanh(values):
    return jax.nn.gelu(values, approximate=True)


def gated_product(gate_vals, up_vals):
    return gelu_tanh(gate_vals) * up_vals


def contract_last(left_rows, right_rows):
    return lax.dot_general(
        left_rows, right_rows, (((1,), (1,)), ((), ())), preferred_element_type=jnp.float32
    )


def contract_first(left_rows, right_rows):
    return lax.dot_general(
        left_rows, right_rows, (((0,), (0,)), ((), ())), preferred_element_type=jnp.float32
    )


def matmul(left_rows, right_rows):
    return jnp.dot(left_rows, right_rows, preferred_element_type=jnp.float32)


def shifted(block, axis, distance):
    devices = range(lax.axis_size(axis))
    route = [(i - distance, i) for i in devices if i - distance in devices]
    return lax.ppermute(block, axis, route)


def flipped(array, axis, mask):
    return lax.ppermute(array, axis, [(i, i ^ mask) for i in range(lax.axis_size(axis))])


def bit_of(axis, bit):
    return (lax.axis_index(axis) // (1 << bit)) % 2


def across(axis, bit):
    index = lax.axis_index(axis)
    return {axis: index + (1 - 2 * ((index // (1 << bit)) % 2)) * (1 << bit)}


def thirds(width):
    tiles = width // 128
    spans, start = [], 0
    for k in range(3):
        count = (tiles + 2 - k) // 3
        spans.append((start * 128, count * 128))
        start += count
    return spans


def send(src, dst, send_sem, recv_sem, device):
    copy = pltpu.make_async_remote_copy(
        src_ref=src,
        dst_ref=dst,
        send_sem=send_sem,
        recv_sem=recv_sem,
        device_id=device,
        device_id_type=MESH,
    )
    copy.start()
    return copy


def greet(devices):
    barrier = pltpu.get_barrier_semaphore()
    for device in devices:
        pl.semaphore_signal(barrier, inc=1, device_id=device, device_id_type=MESH)
    pl.semaphore_wait(barrier, len(devices))


class Gather:
    def __init__(self, x_ref, out_ref, send_sem, recv_sem, core_send, core_recv, own_sem):
        self.sems = send_sem, recv_sem, core_send, core_recv
        self.out = out_ref
        self.me = [bit_of(*link) for link in LINKS]
        self.core = bit_of(*CORE)
        self.peers = [across(*link) for link in LINKS]
        self.core_peer = across(*CORE)
        self.spans = thirds(x_ref.shape[1])
        me, place = self.me, out_ref.at[self.me[0], self.me[1], self.me[2], self.core]
        self.own = pltpu.make_async_copy(x_ref, place, own_sem)
        self.own.start()
        self.moving = [
            send(
                x_ref.at[:, pl.ds(*self.spans[k])],
                self.region(me, k),
                send_sem.at[k, 0],
                recv_sem.at[k, 0],
                self.peers[ORDERS[k][0]],
            )
            for k in range(3)
        ]
        self.to_core = [send(x_ref, place, core_send.at[9], core_recv.at[9], self.core_peer)]
        self.sent = []

    def region(self, idx, k):
        return self.out.at[idx[0], idx[1], idx[2], self.core, :, pl.ds(*self.spans[k])]

    def step(self, step):
        send_sem, recv_sem, core_send, core_recv = self.sems
        me = self.me
        if step == 0:
            self.own.wait()
        for k in range(3):
            order = ORDERS[k]
            self.moving[k].wait_recv()
            self.sent.append(self.moving[k])
            if step < 2:
                held = [slice(None) if d in order[: step + 1] else me[d] for d in range(3)]
                self.moving[k] = send(
                    self.region(held, k),
                    self.region(held, k),
                    send_sem.at[k, step + 1],
                    recv_sem.at[k, step + 1],
                    self.peers[order[step + 1]],
                )
            fresh = [
                slice(None) if d in order[:step] else (1 - me[d] if d == order[step] else me[d])
                for d in range(3)
            ]
            self.to_core.append(
                send(
                    self.region(fresh, k),
                    self.region(fresh, k),
                    core_send.at[3 * step + k],
                    core_recv.at[3 * step + k],
                    self.core_peer,
                )
            )

    def finish(self):
        for copy in self.sent:
            copy.wait_send()
        for copy in self.to_core:
            copy.wait()


def group_peers():
    index = lax.axis_index("dp")
    spot = index % GROUP
    base = index - spot
    spots = (spot + 1 - 2 * (spot % 2), spot + 2 - 4 * (spot // 2), GROUP - 1 - spot)
    return spot, spots, [{"dp": base + other} for other in spots]


def share_width(width):
    return -(-width // (128 * GROUP)) * 128


def overlap_of(width):
    return GROUP * share_width(width) - width


class Spread:
    def __init__(self, weight_ref, out_ref, stage, send_sem, recv_sem, own_sem):
        spot, spots, peers = group_peers()
        width = weight_ref.shape[1]
        share, over = share_width(width), overlap_of(width)

        def columns(place):
            start = share * place - over * (place // (GROUP - 1))
            return weight_ref.at[:, pl.ds(pl.multiple_of(start, 128), share)]

        self.copies = [
            send(columns(spots[m]), out_ref.at[spot], send_sem.at[m], recv_sem.at[m], peers[m])
            for m in range(GROUP - 1)
        ]
        self.own_in = pltpu.make_async_copy(columns(spot), stage, own_sem.at[0])
        self.own_out = pltpu.make_async_copy(stage, out_ref.at[spot], own_sem.at[1])
        self.own_in.start()

    def finish(self):
        self.own_in.wait()
        self.own_out.start()
        for copy in self.copies:
            copy.wait()
        self.own_out.wait()


def spread_scratch(rows, share):
    return [
        pltpu.VMEM((rows, share), jnp.bfloat16),
        pltpu.SemaphoreType.DMA((GROUP - 1,)),
        pltpu.SemaphoreType.DMA((GROUP - 1,)),
        pltpu.SemaphoreType.DMA((2,)),
    ]


def spread_shape(weight):
    return jax.ShapeDtypeStruct((GROUP, weight.shape[0], share_width(weight.shape[1])), jnp.bfloat16)


def spread_kernel(count, *refs):
    weights, outs, scratch = refs[:count], refs[count : 2 * count], refs[2 * count :]
    greet(group_peers()[2])
    shares = [
        Spread(weight, out, *scratch[4 * i : 4 * i + 4])
        for i, (weight, out) in enumerate(zip(weights, outs))
    ]
    for each in shares:
        each.finish()


def spread(*weights):
    anywhere = pl.BlockSpec(memory_space=pl.ANY)
    scratch = []
    for weight in weights:
        scratch += spread_scratch(weight.shape[0], share_width(weight.shape[1]))
    return pl.pallas_call(
        functools.partial(spread_kernel, len(weights)),
        name="spread",
        out_shape=[spread_shape(weight) for weight in weights],
        in_specs=[anywhere for _ in weights],
        out_specs=[anywhere for _ in weights],
        scratch_shapes=scratch,
        compiler_params=pltpu.CompilerParams(collective_id=6, has_side_effects=True),
    )(*weights)


class Collect:
    def __init__(self, part_ref, out_ref, slots, send_sem, recv_sem, own_sem):
        spot, spots, peers = group_peers()
        self.out, self.slots = out_ref, slots
        self.copies = [
            send(part_ref.at[spots[m]], slots.at[spot], send_sem.at[m], recv_sem.at[m], peers[m])
            for m in range(GROUP - 1)
        ]
        self.own = pltpu.make_async_copy(part_ref.at[spot], slots.at[spot], own_sem)
        self.own.start()

    def finish(self):
        self.own.wait()
        for copy in self.copies:
            copy.wait()
        rows, width = self.out.shape
        share, over = share_width(width), overlap_of(width)

        def strip(i, carry):
            at = pl.ds(pl.multiple_of(i * STRIP, STRIP), STRIP)
            for place in range(GROUP):
                skip = over * (place // (GROUP - 1))
                self.out[at, share * place : min(share * (place + 1), width)] = self.slots[
                    place, at, skip:share
                ].astype(jnp.float32)
            return carry

        lax.fori_loop(0, rows // STRIP, strip, 0)


def collect_scratch(rows, share):
    return [
        pltpu.VMEM((GROUP, rows, share), jnp.bfloat16),
        pltpu.SemaphoreType.DMA((GROUP - 1,)),
        pltpu.SemaphoreType.DMA((GROUP - 1,)),
        pltpu.SemaphoreType.DMA,
    ]


def final_kernel(
    n, bits, small_ref, gain1_ref, gain2_ref, part_ref, all_ref, gains_ref, grad_ref,
    came, ssem, rsem, gs, gr, *collect_sems
):
    place = lax.axis_index("dp")
    peers = [{"dp": (place + hop) % n} for hop in range(1, n)]
    greet(peers + [across("tensor", bit) for axis, bit in bits if axis == "tensor"])
    copies = [
        send(small_ref, all_ref.at[place], ssem.at[hop], rsem.at[hop], peers[hop])
        for hop in range(n - 1)
    ]
    all_ref[place] = small_ref[...]
    gains_ref[0:1] = gain1_ref[...]
    gains_ref[1:2] = gain2_ref[...]
    moving = None
    for step, (axis, bit) in enumerate(bits):
        copy = send(gains_ref, came.at[step], gs.at[step], gr.at[step], across(axis, bit))
        if moving is None:
            moving = Collect(part_ref, grad_ref, *collect_sems)
        copy.wait()
        gains_ref[...] = gains_ref[...] + came[step]
    moving.finish()
    for copy in copies:
        copy.wait()


def final_pass(small, gain1, gain2, part, hidden_width):
    n = lax.axis_size("dp")
    bits = [
        (axis, bit)
        for axis in ("tensor", "dp")
        for bit in range(lax.axis_size(axis).bit_length() - 1)
    ]
    rows, width = small.shape
    vmem = pl.BlockSpec(memory_space=pltpu.VMEM)
    gains = (2, gain1.shape[1])
    part_rows, share = part.shape[0] // GROUP, part.shape[1]
    return pl.pallas_call(
        functools.partial(final_kernel, n, bits),
        name="final",
        out_shape=(
            jax.ShapeDtypeStruct((n, rows, width), small.dtype),
            jax.ShapeDtypeStruct(gains, jnp.float32),
            jax.ShapeDtypeStruct((part_rows, hidden_width), jnp.float32),
        ),
        in_specs=[vmem] * 3 + [pl.BlockSpec(memory_space=pl.ANY)],
        out_specs=(vmem, vmem, vmem),
        scratch_shapes=[
            pltpu.VMEM((len(bits), *gains), jnp.float32),
            pltpu.SemaphoreType.DMA((n - 1,)),
            pltpu.SemaphoreType.DMA((n - 1,)),
            pltpu.SemaphoreType.DMA((len(bits),)),
            pltpu.SemaphoreType.DMA((len(bits),)),
            *collect_scratch(part_rows, share),
        ],
        compiler_params=pltpu.CompilerParams(
            collective_id=8, has_side_effects=True, vmem_limit_bytes=24 * 2**20
        ),
    )(small, gain1, gain2, part.reshape(GROUP, part_rows, share))


GATHER_SEMS = [
    pltpu.SemaphoreType.DMA((3, 3)),
    pltpu.SemaphoreType.DMA((3, 3)),
    pltpu.SemaphoreType.DMA((10,)),
    pltpu.SemaphoreType.DMA((10,)),
    pltpu.SemaphoreType.DMA,
]


class SumTensor:
    def __init__(self, part_ref, q, core_buf, link_buf, sems_s, sems_r, own_sem):
        high, core = bit_of(*LINKS[2]), bit_of(*CORE)
        core_peer = across(*CORE)
        self.args = high, q, core_buf, link_buf, sems_s, sems_r
        self.own = pltpu.make_async_copy(part_ref.at[:, core], q, own_sem)
        self.own.start()
        self.copies = [
            send(
                part_ref.at[block, 1 - core],
                core_buf.at[block],
                sems_s.at[i],
                sems_r.at[i],
                core_peer,
            )
            for i, block in enumerate((1 - high, high))
        ]

    def pass_on(self):
        high, q, core_buf, link_buf, sems_s, sems_r = self.args
        self.own.wait()
        self.copies[0].wait_recv()
        q[1 - high] = q[1 - high] + core_buf[1 - high]
        self.copies.append(
            send(q.at[1 - high], link_buf, sems_s.at[2], sems_r.at[2], across(*LINKS[2]))
        )

    def arrive(self):
        self.copies[1].wait_recv()
        self.copies[2].wait_recv()

    def rows(self, rows):
        high, q, core_buf, link_buf, _, _ = self.args
        return (
            q[high, rows].astype(jnp.float32)
            + core_buf[high, rows].astype(jnp.float32)
            + link_buf[rows].astype(jnp.float32)
        )

    def finish(self):
        for copy in self.copies:
            copy.wait_send()


SUM_SEMS = [
    pltpu.SemaphoreType.DMA((3,)),
    pltpu.SemaphoreType.DMA((3,)),
    pltpu.SemaphoreType.DMA,
]

def middle_kernel(
    part_ref, tok_ref, gain_ref, resid_ref, all_ref, q, core_buf, link_buf, low, *sems
):
    greet([across(*link) for link in LINKS] + [across(*CORE)])
    total = SumTensor(part_ref, q, core_buf, link_buf, *sems[:3])
    total.pass_on()
    total.arrive()

    def strip(i, carry):
        rows = pl.ds(pl.multiple_of(i * STRIP, STRIP), STRIP)
        resid = tok_ref[rows].astype(jnp.float32) + total.rows(rows)
        resid_ref[rows] = resid
        inv = lax.rsqrt(jnp.mean(resid * resid, axis=-1, keepdims=True) + epsilon)
        low[rows] = (resid * inv * gain_ref[...]).astype(low.dtype)
        return carry

    lax.fori_loop(0, tok_ref.shape[0] // STRIP, strip, 0)
    total.finish()
    blocks = Gather(low, all_ref, *sems[3:])
    for step in range(3):
        blocks.step(step)
    blocks.finish()


def middle(part, tok, gain):
    rows, width = tok.shape
    vmem, anywhere = pl.BlockSpec(memory_space=pltpu.VMEM), pl.BlockSpec(memory_space=pl.ANY)
    return pl.pallas_call(
        middle_kernel,
        name="middle",
        out_shape=(
            jax.ShapeDtypeStruct((rows, width), jnp.float32),
            jax.ShapeDtypeStruct((2, 2, 2, 2, rows, width), jnp.bfloat16),
        ),
        in_specs=[anywhere, vmem, vmem],
        out_specs=(vmem, anywhere),
        scratch_shapes=[
            pltpu.VMEM((2, rows, width), jnp.bfloat16),
            pltpu.VMEM((2, rows, width), jnp.bfloat16),
            pltpu.VMEM((rows, width), jnp.bfloat16),
            pltpu.VMEM((rows, width), jnp.bfloat16),
            *SUM_SEMS,
            *GATHER_SEMS,
        ],
        compiler_params=pltpu.CompilerParams(
            collective_id=1, has_side_effects=True, vmem_limit_bytes=32 * 2**20
        ),
    )(part.reshape(2, 2, rows, width), tok, gain.reshape(1, width))


def norm_back(rows, back, base_ref, gain_ref, keep_ref, gain_acc):
    base = base_ref[rows].astype(jnp.float32)
    inv = lax.rsqrt(jnp.mean(base * base, axis=-1, keepdims=True) + epsilon)
    unit = base * inv
    scaled = gain_ref[...] * back
    grad = inv * (scaled - unit * jnp.mean(unit * scaled, axis=-1, keepdims=True))
    terms = back * unit
    gain_acc[...] += terms[:8] + terms[8:]
    return keep_ref[rows].astype(jnp.float32) + grad


def back_kernel(
    p_ref, resid_ref, cot_ref, gain_ref, grad_ref, all_ref, gain_out,
    q, cb, r0, r1, r2, low, gain_acc, ssem, rsem, fs, fr, own_sem, gs, gr, gather_own
):
    me = [bit_of(*link) for link in LINKS]
    core = bit_of(*CORE)
    peers = [across(*link) for link in LINKS]
    core_peer = across(*CORE)
    spans = thirds(q.shape[-1])
    own = pltpu.make_async_copy(p_ref.at[:, :, :, core], q, own_sem)
    own.start()
    greet(peers + [core_peer])

    def half(k, near):
        first = ORDERS[k][0]
        return [(me[d] if near else 1 - me[d]) if d == first else slice(None) for d in range(3)]

    to_core = []
    for near in (False, True):
        for k in range(3):
            i = half(k, near)
            to_core.append(
                send(
                    p_ref.at[i[0], i[1], i[2], 1 - core, :, pl.ds(*spans[k])],
                    cb.at[i[0], i[1], i[2], :, pl.ds(*spans[k])],
                    fs.at[len(to_core)],
                    fr.at[len(to_core)],
                    core_peer,
                )
            )
    own.wait()

    def add(i, k, other):
        s, n = spans[k]
        q[i[0], i[1], i[2], :, s : s + n] = q[i[0], i[1], i[2], :, s : s + n] + other

    moving, sent = [], []
    for near in (False, True):
        for k in range(3):
            to_core[3 * near + k].wait_recv()
            i = half(k, near)
            s, n = spans[k]
            add(i, k, cb[i[0], i[1], i[2], :, s : s + n])
            if not near:
                moving.append(
                    send(
                        q.at[i[0], i[1], i[2], :, pl.ds(s, n)],
                        r0.at[:, :, :, pl.ds(s, n)],
                        ssem.at[k, 0],
                        rsem.at[k, 0],
                        peers[ORDERS[k][0]],
                    )
                )
    for step in (1, 2):
        for k in range(3):
            s, n = spans[k]
            order = ORDERS[k]
            moving[k].wait_recv()
            sent.append(moving[k])
            kept = [me[d] if d in order[:step] else slice(None) for d in range(3)]
            add(kept, k, r0[:, :, :, s : s + n] if step == 1 else r1[:, :, s : s + n])
            away = [
                me[d] if d in order[:step] else (1 - me[d] if d == order[step] else slice(None))
                for d in range(3)
            ]
            moving[k] = send(
                q.at[away[0], away[1], away[2], :, pl.ds(s, n)],
                r1.at[:, :, pl.ds(s, n)] if step == 1 else r2.at[:, pl.ds(s, n)],
                ssem.at[k, step],
                rsem.at[k, step],
                peers[order[step]],
            )
    for k in range(3):
        moving[k].wait_recv()
        sent.append(moving[k])
    gain_acc[...] = jnp.zeros_like(gain_acc)

    def strip(i, carry):
        rows = pl.ds(pl.multiple_of(i * STRIP, STRIP), STRIP)
        back = q[me[0], me[1], me[2], rows].astype(jnp.float32) + r2[rows].astype(jnp.float32)
        grad = norm_back(rows, back, resid_ref, gain_ref, cot_ref, gain_acc)
        grad_ref[rows] = grad
        low[rows] = grad.astype(low.dtype)
        return carry

    lax.fori_loop(0, low.shape[0] // STRIP, strip, 0)
    for copy in sent + to_core:
        copy.wait_send()
    gain_out[...] = jnp.sum(gain_acc[...], axis=0, keepdims=True)
    mine = all_ref.at[me[2], core]
    local = pltpu.make_async_copy(low, mine, gather_own)
    local.start()
    along = send(low, mine, gs.at[0], gr.at[0], peers[2])
    beside = send(low, mine, gs.at[1], gr.at[1], core_peer)
    along.wait_recv()
    theirs = all_ref.at[1 - me[2], core]
    onward = send(theirs, theirs, gs.at[2], gr.at[2], core_peer)
    local.wait()
    beside.wait()
    onward.wait()
    along.wait_send()


def back_pass(part, resid, cot, gain):
    rows, width = resid.shape
    wide = lambda *lead: pltpu.VMEM((*lead, rows, width), jnp.bfloat16)
    vmem = pl.BlockSpec(memory_space=pltpu.VMEM)
    return pl.pallas_call(
        back_kernel,
        name="back",
        out_shape=(
            jax.ShapeDtypeStruct((rows, width), jnp.float32),
            jax.ShapeDtypeStruct((2, 2, rows, width), jnp.bfloat16),
            jax.ShapeDtypeStruct((1, width), jnp.float32),
        ),
        in_specs=[pl.BlockSpec(memory_space=pl.ANY), vmem, vmem, vmem],
        out_specs=(vmem, pl.BlockSpec(memory_space=pl.ANY), vmem),
        scratch_shapes=[
            wide(2, 2, 2),
            wide(2, 2, 2),
            wide(2, 2),
            wide(2),
            wide(),
            wide(),
            pltpu.VMEM((8, width), jnp.float32),
            pltpu.SemaphoreType.DMA((3, 3)),
            pltpu.SemaphoreType.DMA((3, 3)),
            pltpu.SemaphoreType.DMA((6,)),
            pltpu.SemaphoreType.DMA((6,)),
            pltpu.SemaphoreType.DMA,
            pltpu.SemaphoreType.DMA((3,)),
            pltpu.SemaphoreType.DMA((3,)),
            pltpu.SemaphoreType.DMA,
        ],
        compiler_params=pltpu.CompilerParams(
            collective_id=2, has_side_effects=True, vmem_limit_bytes=40 * 2**20
        ),
    )(part.reshape(2, 2, 2, 2, rows, width), resid, cot, gain.reshape(1, width))


class Halve:
    def __init__(self, held, came, send_sem, recv_sem, orders, spans):
        self.held, self.came, self.sems = held, came, (send_sem, recv_sem)
        self.orders, self.spans = orders, spans
        self.bits = len(orders[0])
        self.me = [bit_of("dp", bit) for bit in range(self.bits)]
        self.moving, self.sent = [None] * len(orders), []

    def index(self, done, away=None):
        picks = []
        for bit in reversed(range(self.bits)):
            if bit in done:
                picks.append(self.me[bit])
            elif bit == away:
                picks.append(1 - self.me[bit])
            else:
                picks.append(slice(None))
        return picks

    def landing(self, c, step):
        return self.came[len(self.orders) * step + c]

    def start(self, step):
        send_sem, recv_sem = self.sems
        for c, order in enumerate(self.orders):
            at, count = self.spans[c]
            self.moving[c] = send(
                self.held.at[(*self.index(order[:step], order[step]), slice(None), pl.ds(at, count))],
                self.landing(c, step),
                send_sem.at[c, step],
                recv_sem.at[c, step],
                across("dp", order[step]),
            )

    def land(self, step):
        for c, order in enumerate(self.orders):
            at, count = self.spans[c]
            self.moving[c].wait_recv()
            self.sent.append(self.moving[c])
            kept = (*self.index(order[: step + 1]), slice(None), slice(at, at + count))
            self.held[kept] = self.held[kept] + self.landing(c, step)[...]

    def result(self):
        return self.held[tuple(self.me[bit] for bit in reversed(range(self.bits)))]

    def finish(self):
        for copy in self.sent:
            copy.wait_send()


def halve_plan(bits, rows, width):
    wide = -(-width // 256) * 128
    orders = [list(range(bits)), [1, 0, *range(2, bits)]]
    spans = [(0, wide), (wide, width - wide)]
    scratch = [pltpu.VMEM((*[2] * bits, rows, width), jnp.bfloat16)]
    for step in range(bits):
        for _, count in spans:
            scratch.append(pltpu.VMEM((*[2] * (bits - 1 - step), rows, count), jnp.bfloat16))
    scratch += [pltpu.SemaphoreType.DMA((2, bits)), pltpu.SemaphoreType.DMA((2, bits))]
    return orders, spans, scratch


def last_kernel(
    plan, part_ref, tok_ref, keep_ref, gain_ref, wide_ref, few_ref, down_ref, gate_ref,
    grad_ref, gain_out, wide_out, few_out, down_out, gate_out,
    q, core_buf, link_buf, gain_acc, *sems
):
    orders, spans, _ = plan
    bits = len(orders[0])
    sum_sems, held, came, sems = sems[:3], sems[3], sems[4 : 4 + 2 * bits], sems[4 + 2 * bits :]
    halve_send, halve_recv, load_sem, *sems = sems
    loads = [
        pltpu.make_async_copy(
            wide_ref, held.at[(*[slice(None)] * bits, pl.ds(0, wide_ref.shape[-2]))], load_sem.at[0]
        ),
        pltpu.make_async_copy(
            few_ref,
            held.at[(*[slice(None)] * bits, pl.ds(wide_ref.shape[-2], few_ref.shape[-2]))],
            load_sem.at[1],
        ),
    ]
    for load in loads:
        load.start()
    peers = [across("dp", bit) for bit in range(bits)]
    greet([across(*LINKS[2]), across(*CORE), group_peers()[2][2]] + peers)
    total = SumTensor(part_ref, q, core_buf, link_buf, *sum_sems)
    blocks = Halve(held, came, halve_send, halve_recv, orders, spans)
    for load in loads:
        load.wait()
    blocks.start(0)
    downs = Collect(down_ref, down_out, *sems[:4])
    gates = Collect(gate_ref, gate_out, *sems[4:])
    total.pass_on()
    gain_acc[...] = jnp.zeros_like(gain_acc)

    def strip(i, carry):
        rows = pl.ds(pl.multiple_of(i * STRIP, STRIP), STRIP)
        back = total.rows(rows)
        grad_ref[rows] = norm_back(rows, back, tok_ref, gain_ref, keep_ref, gain_acc)
        return carry

    total.arrive()
    lax.fori_loop(0, tok_ref.shape[0] // STRIP, strip, 0)
    gain_out[...] = jnp.sum(gain_acc[...], axis=0, keepdims=True)
    for step in range(bits):
        blocks.land(step)
        if step + 1 < bits:
            blocks.start(step + 1)
        if step == 0:
            downs.finish()
        if step == 1:
            gates.finish()
    mine = blocks.result()
    wide_out[...] = mine[: wide_out.shape[0]].astype(jnp.float32)
    few_out[...] = mine[wide_out.shape[0] :]
    blocks.finish()
    total.finish()


def last_pass(part, tok, keep, gain, wide, few, down, gate, hidden_width):
    rows, width = tok.shape
    vmem, anywhere = pl.BlockSpec(memory_space=pltpu.VMEM), pl.BlockSpec(memory_space=pl.ANY)
    bits = wide.shape[0].bit_length() - 1
    plan = halve_plan(bits, wide.shape[1] + few.shape[1], wide.shape[2])
    part_rows, share = down.shape[0] // GROUP, down.shape[1]
    grad = jax.ShapeDtypeStruct((part_rows, hidden_width), jnp.float32)
    leading = [2] * bits
    return pl.pallas_call(
        functools.partial(last_kernel, plan),
        name="last",
        out_shape=(
            jax.ShapeDtypeStruct((rows, width), jnp.float32),
            jax.ShapeDtypeStruct((1, width), jnp.float32),
            jax.ShapeDtypeStruct(wide.shape[1:], jnp.float32),
            jax.ShapeDtypeStruct(few.shape[1:], jnp.bfloat16),
            grad,
            grad,
        ),
        in_specs=[anywhere, vmem, vmem, vmem] + [anywhere] * 4,
        out_specs=(vmem,) * 6,
        scratch_shapes=[
            pltpu.VMEM((2, rows, width), jnp.bfloat16),
            pltpu.VMEM((2, rows, width), jnp.bfloat16),
            pltpu.VMEM((rows, width), jnp.bfloat16),
            pltpu.VMEM((8, width), jnp.float32),
            *SUM_SEMS,
            *plan[2],
            pltpu.SemaphoreType.DMA((2,)),
            *collect_scratch(part_rows, share),
            *collect_scratch(part_rows, share),
        ],
        compiler_params=pltpu.CompilerParams(
            collective_id=3, has_side_effects=True, vmem_limit_bytes=48 * 2**20
        ),
    )(
        part.reshape(2, 2, rows, width),
        tok,
        keep,
        gain.reshape(1, width),
        wide.reshape(*leading, *wide.shape[1:]),
        few.reshape(*leading, *few.shape[1:]),
        down.reshape(GROUP, part_rows, share),
        gate.reshape(GROUP, part_rows, share),
    )


def scan_kernel(n, reverse, *refs):
    if reverse:
        a_ref, b_ref, out_ref, edge_ref, fa, fb, mine, others, ssem, rsem = refs
    else:
        a_ref, b_ref, weight_ref, cot_ref, out_ref, edge_ref, share_ref, cot_all_ref, *refs = refs
        fa, fb, mine, others, ssem, rsem, *refs = refs
        spread_sems, cot_sems = refs[:4], refs[4:]
    place = lax.axis_index("dp")
    sign = -1 if reverse else 1
    barrier = pltpu.get_barrier_semaphore()
    peers = [{"dp": (place + sign * hop + n) % n} for hop in range(1, n)]
    others_met = [] if reverse else [across(*LINKS[2]), across(*CORE)]
    for peer in peers + others_met:
        pl.semaphore_signal(barrier, inc=1, device_id=peer, device_id_type=MESH)
    rows, width = a_ref.shape
    length = rows // 8
    lanes = range(width // 128)
    for k in lanes:
        fa[k * rows : (k + 1) * rows] = a_ref[:, k * 128 : (k + 1) * 128]
        fb[k * rows : (k + 1) * rows] = b_ref[:, k * 128 : (k + 1) * 128]

    def at(k, r):
        return pl.ds(k * rows + (length - 1 - r if reverse else r), 8, stride=length)

    def local(r, carry):
        result = []
        for k in lanes:
            prod, state = carry[k]
            decay = fa[at(k, r), :]
            term = fb[at(k, r), :]
            if reverse:
                fa[at(k, r), :] = prod
                total = term + state
                fb[at(k, r), :] = total
                result.append((prod * decay, decay * total))
            else:
                prod = prod * decay
                state = decay * state + term
                fa[at(k, r), :] = prod
                fb[at(k, r), :] = state
                result.append((prod, state))
        return result

    start = [(jnp.ones((8, 128), jnp.float32), jnp.zeros((8, 128), jnp.float32)) for k in lanes]
    ends = lax.fori_loop(0, length, local, start, unroll=2)
    prod = jnp.concatenate([end[0] for end in ends], axis=1)
    state = jnp.concatenate([end[1] for end in ends], axis=1)
    order = range(7, -1, -1) if reverse else range(8)
    run_a, run_b = jnp.ones((1, width), jnp.float32), jnp.zeros((1, width), jnp.float32)
    before = [None] * 8
    for s in order:
        before[s] = (run_a, run_b)
        pa, pb = prod[s : s + 1], state[s : s + 1]
        run_a, run_b = pa * run_a, pa * run_b + pb
    mine[0:1] = run_a
    mine[1:2] = run_b
    pl.semaphore_wait(barrier, n - 1 + len(others_met))
    copies = [
        send(mine, others.at[hop - 1], ssem.at[hop - 1], rsem.at[hop - 1], peers[hop - 1])
        for hop in range(1, n)
    ]
    if not reverse:
        cots = Gather(cot_ref, cot_all_ref, *cot_sems)
        shares = Spread(weight_ref, share_ref, *spread_sems)
    carry = jnp.zeros((1, width), jnp.float32)
    ahead = n - 1 - place if reverse else place
    for copy in copies:
        copy.wait_recv()
    for hop in range(n - 1, 0, -1):
        step = others[hop - 1, 0:1] * carry + others[hop - 1, 1:2]
        carry = jnp.where(hop <= ahead, step, carry)
    edge_ref[...] = carry
    if not reverse:
        cots.step(0)
    entering = jnp.concatenate([pa * carry + pb for pa, pb in before], axis=0)

    def fix(r, c):
        for k in lanes:
            fb[at(k, r), :] = fb[at(k, r), :] + fa[at(k, r), :] * entering[:, k * 128 : (k + 1) * 128]
        return c

    lax.fori_loop(0, length, fix, 0, unroll=2)
    for k in lanes:
        out_ref[:, k * 128 : (k + 1) * 128] = fb[k * rows : (k + 1) * rows]
    for copy in copies:
        copy.wait_send()
    if not reverse:
        cots.step(1)
        cots.step(2)
        shares.finish()
        cots.finish()


def scan_stream(decay, term, weight=None, cot=None):
    n = lax.axis_size("dp")
    rows, width = decay.shape
    reverse = weight is None
    vmem, anywhere = pl.BlockSpec(memory_space=pltpu.VMEM), pl.BlockSpec(memory_space=pl.ANY)
    out_shape = [
        jax.ShapeDtypeStruct((rows, width), jnp.float32),
        jax.ShapeDtypeStruct((1, width), jnp.float32),
    ]
    scratch = [
        pltpu.VMEM((rows * width // 128, 128), jnp.float32),
        pltpu.VMEM((rows * width // 128, 128), jnp.float32),
        pltpu.VMEM((2, width), jnp.float32),
        pltpu.VMEM((n - 1, 2, width), jnp.float32),
        pltpu.SemaphoreType.DMA((n - 1,)),
        pltpu.SemaphoreType.DMA((n - 1,)),
    ]
    args = [decay, term]
    in_specs, out_specs = [vmem, vmem], [vmem, vmem]
    if not reverse:
        args += [weight, cot]
        in_specs += [anywhere, vmem]
        out_specs += [anywhere, anywhere]
        out_shape += [
            spread_shape(weight),
            jax.ShapeDtypeStruct((2, 2, 2, 2, *cot.shape), cot.dtype),
        ]
        scratch += spread_scratch(weight.shape[0], share_width(weight.shape[1]))
        scratch += GATHER_SEMS
    return pl.pallas_call(
        functools.partial(scan_kernel, n, reverse),
        name="scan_back" if reverse else "scan",
        out_shape=out_shape,
        in_specs=in_specs,
        out_specs=out_specs,
        scratch_shapes=scratch,
        compiler_params=pltpu.CompilerParams(
            collective_id=5 if reverse else 4, has_side_effects=True, vmem_limit_bytes=32 * 2**20
        ),
    )(*args)


def in_order(bit, mine, theirs, axis=0):
    return jnp.where(
        bit == 0, jnp.concatenate([mine, theirs], axis), jnp.concatenate([theirs, mine], axis)
    )


def halve(blocks, order):
    place = lax.axis_index("dp")
    left = sorted(order, reverse=True)
    assert blocks.shape[0] == 1 << len(left)
    held = blocks.reshape(*[2 for _ in left], *blocks.shape[1:])
    for bit in order:
        axis = left.index(bit)
        mine = (place // (1 << bit)) % 2
        keep = lax.dynamic_index_in_dim(held, mine, axis, False)
        away = lax.dynamic_index_in_dim(held, 1 - mine, axis, False)
        came = flipped(away, "dp", 1 << bit)
        held = (keep.astype(jnp.float32) + came.astype(jnp.float32)).astype(jnp.bfloat16)
        left.remove(bit)
    return held


def local(
    tokens,
    doc_start,
    norm1_gain,
    proj_x,
    proj_y,
    conv_weight,
    conv_bias,
    gate_x_weight,
    gate_x_bias,
    gate_a_weight,
    gate_a_bias,
    decay_param,
    proj_out,
    norm2_gain,
    mlp_gate,
    mlp_up,
    mlp_down,
    cotangent,
):
    tok_rows = tokens.shape[0]
    chan_width = proj_x.shape[1]
    block_width = gate_x_weight.shape[0]
    half_width = block_width // 2
    tap_count = conv_weight.shape[0]
    parity = lax.axis_index("tensor") % 2
    full_start = parity * half_width
    shared_start = (1 - parity) * 2 * block_width
    tensor_size = lax.axis_size("tensor")
    share_rows = tok_rows // tensor_size
    own_start = lax.axis_index("tensor") * share_rows
    positions = lax.axis_index("dp") * tok_rows + lax.iota(jnp.int32, tok_rows)
    starting = (doc_start == positions)[:, None]
    groups = [
        [(g * GROUP + i) * tensor_size + t for i in range(GROUP) for t in range(tensor_size)]
        for g in range(lax.axis_size("dp") // GROUP)
    ]
    everyone = ("dp", "tensor")

    dp_size = lax.axis_size("dp")
    dp_bits = range(dp_size.bit_length() - 1)
    spot = lax.axis_index("dp") % GROUP
    across_blocks = [[i + GROUP * g for g in range(dp_size // GROUP)] for i in range(GROUP)]
    hidden_width = mlp_gate.shape[1]
    share = share_width(hidden_width)

    def all_rows(part):
        flat = part.reshape(-1, share)
        return lax.all_gather(flat, "dp", axis_index_groups=across_blocks, tiled=True)

    gate_part, up_part = spread(mlp_gate, mlp_up)
    gate_cols, up_cols = all_rows(gate_part), all_rows(up_part)
    tok_own = lax.dynamic_slice_in_dim(tokens, own_start, share_rows, 0)
    cot_own = lax.dynamic_slice_in_dim(cotangent, own_start, share_rows, 0)

    def normalize(values):
        values = values.astype(jnp.float32)
        inv_rms = lax.rsqrt(jnp.mean(values * values, axis=-1, keepdims=True) + epsilon)
        return (values * inv_rms * norm1_gain).astype(jnp.bfloat16)

    halo = 16
    normed_low = normalize(tokens)
    normed_prev = normalize(shifted(tokens[tok_rows - halo :], "dp", 1))
    branch_y = matmul(normed_low, proj_y)
    branch_x = matmul(normed_low, proj_x).astype(jnp.bfloat16)
    prev_x = matmul(normed_prev, proj_x).astype(jnp.bfloat16)
    extended = jnp.concatenate([prev_x[halo - tap_count + 1 :], branch_x], axis=0).astype(
        jnp.float32
    )

    def conv_apply(ext_rows, weight, bias_vec):
        conv_out = bias_vec + weight[0] * ext_rows[tap_count - 1 :]
        for offset in range(1, tap_count):
            inside = (positions - offset >= doc_start).astype(jnp.float32)[:, None]
            lagged = ext_rows[tap_count - 1 - offset : tap_count - 1 - offset + tok_rows]
            conv_out = conv_out + weight[offset] * lagged * inside
        return conv_out

    conv_out, conv_pull = jax.vjp(conv_apply, extended, conv_weight, conv_bias)
    mixed_low = conv_out.astype(jnp.bfloat16)
    own_half = lax.dynamic_slice_in_dim(mixed_low, shared_start, half_width, 1)
    other_half = flipped(own_half, "tensor", 1)
    shared_in = in_order(parity, own_half, other_half, 1)
    full_in = lax.dynamic_slice_in_dim(mixed_low, full_start, 2 * block_width, 1).reshape(
        tok_rows, 2, block_width
    )

    def place(full_part, shared_part):
        return in_order(parity, full_part, shared_part, 1)

    def full_weight(weight):
        return lax.dynamic_slice_in_dim(weight, full_start, 2 * block_width, 1).reshape(
            block_width, 2, block_width
        )

    def shared_weight(weight):
        return lax.dynamic_slice_in_dim(weight, shared_start, half_width, 1)

    def gate_pre(weight, bias_vec):
        full_out = jnp.einsum(
            "nhi,ihj->nhj", full_in, full_weight(weight), preferred_element_type=jnp.float32
        ).reshape(tok_rows, 2 * block_width)
        shared_out = matmul(shared_in, shared_weight(weight))
        return place(full_out, shared_out) + bias_vec

    def recurrence_in(conv_vals, pre_input, pre_recur, param_vec):
        log_decay = -8.0 * jax.nn.sigmoid(pre_recur) * jax.nn.softplus(param_vec)
        decay = jnp.where(starting, 0.0, jnp.exp(log_decay))
        multiplier = jnp.where(starting, 1.0, jnp.sqrt(-jnp.expm1(2.0 * log_decay)))
        return (decay, multiplier * jax.nn.sigmoid(pre_input) * conv_vals)

    pre_input = gate_pre(gate_x_weight, gate_x_bias)
    pre_recur = gate_pre(gate_a_weight, gate_a_bias)
    (decay, drive), recur_pull = jax.vjp(
        recurrence_in, mixed_low.astype(jnp.float32), pre_input, pre_recur, decay_param
    )
    states, entering, down_part, cot_all = scan_stream(decay, drive, mlp_down, cot_own)
    down_cols = all_rows(down_part)
    previous = jnp.concatenate([entering, states[:-1]], axis=0)
    gelu_y, gelu_pull = jax.vjp(gelu_tanh, branch_y)
    product_low = (states * gelu_y).astype(jnp.bfloat16)
    resid, normed2_all = middle(
        matmul(product_low, proj_out).astype(jnp.bfloat16), tok_own, norm2_gain
    )
    normed2_all = normed2_all.reshape(GROUP * tok_rows, -1)
    cot_all = cot_all.reshape(GROUP * tok_rows, -1)
    counted = lax.iota(jnp.int32, share) >= overlap_of(hidden_width) * (spot // (GROUP - 1))

    def once(values):
        return jnp.where(counted, values, 0.0).astype(jnp.bfloat16)

    gate_act = matmul(normed2_all, gate_cols)
    up_act = matmul(normed2_all, up_cols)
    hidden, act_pull = jax.vjp(gated_product, gate_act, up_act)
    hidden_low = once(hidden)
    grad_hidden = matmul(cot_all, down_cols)
    grad_gate, grad_up = act_pull(grad_hidden)
    grad_gate_low = once(grad_gate)
    grad_up_low = once(grad_up)

    def own_rows(grad):
        return lax.psum_scatter(
            grad.astype(jnp.bfloat16),
            "dp",
            axis_index_groups=across_blocks,
            scatter_dimension=0,
            tiled=True,
        )

    back_part = (
        contract_last(grad_gate_low, gate_cols) + contract_last(grad_up_low, up_cols)
    ).astype(jnp.bfloat16)
    down_grad = contract_first(cot_all, hidden_low).astype(jnp.bfloat16)
    back_part, down_grad = lax.optimization_barrier((back_part, down_grad))
    down_rows = own_rows(down_grad)
    grad_resid, grad_lru_low, grad_gain2 = back_pass(back_part, resid, cot_own, norm2_gain)
    grad_lru_low = grad_lru_low.reshape(tok_rows, -1)
    gate_rows = own_rows(contract_first(normed2_all, grad_gate_low))
    up_rows = own_rows(contract_first(normed2_all, grad_up_low))
    block_out = resid + lax.psum_scatter(
        contract_last(hidden_low, down_cols).astype(jnp.bfloat16),
        everyone,
        axis_index_groups=groups,
        scatter_dimension=0,
        tiled=True,
    ).astype(jnp.float32)

    grad_product = contract_last(grad_lru_low, proj_out)
    grad_states = grad_product * gelu_y
    grad_y_low = gelu_pull(grad_product * states)[0].astype(jnp.bfloat16)
    total_grad, _ = scan_stream(decay, grad_states)
    total_grad, late_y, late_lru = lax.optimization_barrier(
        (total_grad, grad_y_low, grad_lru_low)
    )

    def token_sum(left_rows, right_rows):
        return contract_first(left_rows, right_rows).astype(jnp.bfloat16)

    def per_device(rows):
        return rows.reshape(dp_size, rows.shape[0] // dp_size, rows.shape[1])

    low_first, high_first = list(dp_bits), [1, 0, *dp_bits[2:]]
    grad_proj_y = halve(per_device(token_sum(normed_low, late_y)), low_first).astype(jnp.float32)
    grad_proj_out = (
        halve(per_device(token_sum(late_lru, product_low)), high_first).astype(jnp.float32).T
    )
    conv_direct, grad_pre_input, grad_pre_recur, grad_param = recur_pull(
        (total_grad * previous, total_grad)
    )

    def gate_back(weight, grad_pre):
        grad_pre_low = grad_pre.astype(jnp.bfloat16)
        grad_full = lax.dynamic_slice_in_dim(grad_pre_low, full_start, 2 * block_width, 1).reshape(
            tok_rows, 2, block_width
        )
        grad_share = lax.dynamic_slice_in_dim(grad_pre_low, shared_start, half_width, 1)
        into_full = jnp.einsum(
            "nhj,ihj->nhi", grad_full, full_weight(weight), preferred_element_type=jnp.float32
        ).reshape(tok_rows, 2 * block_width)
        into_share = contract_last(grad_share, shared_weight(weight))
        weight_full = jnp.einsum(
            "nhi,nhj->ihj", full_in, grad_full, preferred_element_type=jnp.float32
        ).reshape(block_width, 2 * block_width)
        weight_share = contract_first(shared_in, grad_share)
        return (into_full, into_share, place(weight_full, weight_share))

    input_full, input_share, grad_gx_weight = gate_back(gate_x_weight, grad_pre_input)
    recur_full, recur_share, grad_ga_weight = gate_back(gate_a_weight, grad_pre_recur)
    full_sum = input_full + recur_full
    share_sum = input_share + recur_share
    own_grad = jnp.where(parity == 0, share_sum[:, :half_width], share_sum[:, half_width:])
    other_grad = jnp.where(parity == 0, share_sum[:, half_width:], share_sum[:, :half_width])
    returned = flipped(other_grad.astype(jnp.bfloat16), "tensor", 1).astype(other_grad.dtype)
    grad_conv = conv_direct + place(full_sum, own_grad + returned)
    grad_extended, grad_conv_weight, grad_conv_bias = conv_pull(grad_conv)
    rim_grad = shifted(grad_extended[: tap_count - 1], "dp", -1)
    grad_branch_x = grad_extended[tap_count - 1 :] + jnp.concatenate(
        [jnp.zeros((tok_rows - tap_count + 1, chan_width), jnp.float32), rim_grad], axis=0
    )
    grad_x_low = grad_branch_x.astype(jnp.bfloat16)
    wide = jnp.concatenate([grad_gx_weight, grad_ga_weight], axis=0)
    sums = jnp.concatenate(
        [
            grad_conv_weight,
            grad_conv_bias[None],
            jnp.sum(grad_pre_input, axis=0)[None],
            jnp.sum(grad_pre_recur, axis=0)[None],
            grad_param[None],
        ],
        axis=0,
    )
    spare = dp_size * 16 - sums.shape[0]
    sums = jnp.concatenate([sums, jnp.zeros((spare, chan_width), jnp.float32)], axis=0)
    few = jnp.concatenate(
        [per_device(wide.astype(jnp.bfloat16)), per_device(sums.astype(jnp.bfloat16))], axis=1
    )
    grad_tokens, grad_gain1, grad_proj_x, reduced, grad_mlp_down, grad_mlp_gate = last_pass(
        (contract_last(grad_x_low, proj_x) + contract_last(grad_y_low, proj_y)).astype(
            jnp.bfloat16
        ),
        tok_own,
        grad_resid,
        norm1_gain,
        per_device(token_sum(normed_low, grad_x_low)),
        few,
        down_rows,
        gate_rows,
        hidden_width,
    )
    shared, gains, grad_mlp_up = final_pass(reduced, grad_gain1, grad_gain2, up_rows, hidden_width)
    wide_rows = 2 * block_width // dp_size
    wide = shared[:, :wide_rows].reshape(2 * block_width, chan_width).astype(jnp.float32)
    small = shared[:, wide_rows:].reshape(dp_size * 16, chan_width).astype(jnp.float32)
    return (
        block_out,
        grad_tokens,
        gains[0],
        grad_proj_x,
        grad_proj_y,
        small[:tap_count],
        small[tap_count],
        wide[:block_width],
        small[tap_count + 1],
        wide[block_width:],
        small[tap_count + 2],
        small[tap_count + 3],
        grad_proj_out,
        gains[1],
        grad_mlp_gate,
        grad_mlp_up,
        grad_mlp_down,
    )


def solution(mesh):
    placed = (
        P("dp", None),
        P("dp"),
        P(),
        P(None, "tensor"),
        P(None, "tensor"),
        P(None, "tensor"),
        P("tensor"),
        P(None, "tensor"),
        P("tensor"),
        P(None, "tensor"),
        P("tensor"),
        P("tensor"),
        P("tensor", None),
        P(),
        P("dp", "tensor"),
        P("dp", "tensor"),
        P("dp", "tensor"),
        P("dp", None),
    )
    return jax.shard_map(
        local,
        mesh=mesh,
        in_specs=placed,
        out_specs=(
            P(("dp", "tensor"), None),
            P(("dp", "tensor"), None),
            P(),
            P("dp", "tensor"),
            P("dp", "tensor"),
            P(None, "tensor"),
            P("tensor"),
            P(None, "tensor"),
            P("tensor"),
            P(None, "tensor"),
            P("tensor"),
            P("tensor"),
            P("tensor", "dp"),
            P(),
            P("dp", "tensor"),
            P("dp", "tensor"),
            P("dp", "tensor"),
        ),
        check_vma=False,
    )
```

```python
import functools

import jax
import jax.numpy as jnp
from jax import lax
from jax.experimental import pallas as pl
from jax.experimental.pallas import tpu as pltpu
from jax.sharding import PartitionSpec as P

epsilon = 1e-06
MESH = pl.DeviceIdType.MESH
GROUP = 4
STRIP = 16
LINKS = (("dp", 1), ("dp", 0), ("tensor", 1))
CORE = ("tensor", 0)
ORDERS = ((0, 1, 2), (0, 2, 1), (1, 2, 0))
SUM_ORDERS = tuple(order[::-1] for order in ORDERS)


def gelu_tanh(values):
    return jax.nn.gelu(values, approximate=True)


def gated_product(gate_vals, up_vals):
    return gelu_tanh(gate_vals) * up_vals


def contract_last(left_rows, right_rows):
    return lax.dot_general(
        left_rows, right_rows, (((1,), (1,)), ((), ())), preferred_element_type=jnp.float32
    )


def contract_first(left_rows, right_rows):
    return lax.dot_general(
        left_rows, right_rows, (((0,), (0,)), ((), ())), preferred_element_type=jnp.float32
    )


def matmul(left_rows, right_rows):
    return jnp.dot(left_rows, right_rows, preferred_element_type=jnp.float32)


def shifted(block, axis, distance):
    devices = range(lax.axis_size(axis))
    route = [(i - distance, i) for i in devices if i - distance in devices]
    return lax.ppermute(block, axis, route)


def flipped(array, axis, mask):
    return lax.ppermute(array, axis, [(i, i ^ mask) for i in range(lax.axis_size(axis))])


def bit_of(axis, bit):
    return (lax.axis_index(axis) // (1 << bit)) % 2


def across(axis, bit):
    index = lax.axis_index(axis)
    return {axis: index + (1 - 2 * ((index // (1 << bit)) % 2)) * (1 << bit)}


def thirds(width):
    tiles = width // 128
    most = tiles * 9 // 20
    spans, start = [], 0
    for count in (most, most, tiles - 2 * most):
        spans.append((start * 128, count * 128))
        start += count
    return spans


def send(src, dst, send_sem, recv_sem, device):
    copy = pltpu.make_async_remote_copy(
        src_ref=src,
        dst_ref=dst,
        send_sem=send_sem,
        recv_sem=recv_sem,
        device_id=device,
        device_id_type=MESH,
    )
    copy.start()
    return copy


def greet(devices):
    barrier = pltpu.get_barrier_semaphore()
    for device in devices:
        pl.semaphore_signal(barrier, inc=1, device_id=device, device_id_type=MESH)
    pl.semaphore_wait(barrier, len(devices))


class Gather:
    def __init__(self, x_ref, out_ref, send_sem, recv_sem, core_send, core_recv, own_sem):
        self.sems = send_sem, recv_sem, core_send, core_recv
        self.out = out_ref
        self.me = [bit_of(*link) for link in LINKS]
        self.core = bit_of(*CORE)
        self.peers = [across(*link) for link in LINKS]
        self.core_peer = across(*CORE)
        self.spans = thirds(x_ref.shape[1])
        me, place = self.me, out_ref.at[self.me[0], self.me[1], self.me[2], self.core]
        self.own = pltpu.make_async_copy(x_ref, place, own_sem)
        self.own.start()
        self.moving = [
            send(
                x_ref.at[:, pl.ds(*self.spans[k])],
                self.region(me, k),
                send_sem.at[k, 0],
                recv_sem.at[k, 0],
                self.peers[ORDERS[k][0]],
            )
            for k in range(3)
        ]
        self.to_core = [send(x_ref, place, core_send.at[9], core_recv.at[9], self.core_peer)]
        self.sent = []

    def region(self, idx, k):
        return self.out.at[idx[0], idx[1], idx[2], self.core, :, pl.ds(*self.spans[k])]

    def step(self, step):
        send_sem, recv_sem, core_send, core_recv = self.sems
        me = self.me
        if step == 0:
            self.own.wait()
        for k in range(3):
            order = ORDERS[k]
            self.moving[k].wait_recv()
            self.sent.append(self.moving[k])
            if step < 2:
                held = [slice(None) if d in order[: step + 1] else me[d] for d in range(3)]
                self.moving[k] = send(
                    self.region(held, k),
                    self.region(held, k),
                    send_sem.at[k, step + 1],
                    recv_sem.at[k, step + 1],
                    self.peers[order[step + 1]],
                )
            fresh = [
                slice(None) if d in order[:step] else (1 - me[d] if d == order[step] else me[d])
                for d in range(3)
            ]
            self.to_core.append(
                send(
                    self.region(fresh, k),
                    self.region(fresh, k),
                    core_send.at[3 * step + k],
                    core_recv.at[3 * step + k],
                    self.core_peer,
                )
            )

    def finish(self):
        for copy in self.sent:
            copy.wait_send()
        for copy in self.to_core:
            copy.wait()


def group_peers():
    index = lax.axis_index("dp")
    spot = index % GROUP
    base = index - spot
    spots = (spot + 1 - 2 * (spot % 2), spot + 2 - 4 * (spot // 2), GROUP - 1 - spot)
    return spot, spots, [{"dp": base + other} for other in spots]


def share_width(width):
    return -(-width // (128 * GROUP)) * 128


def overlap_of(width):
    return GROUP * share_width(width) - width


class Spread:
    def __init__(self, weight_ref, out_ref, stage, send_sem, recv_sem, own_sem):
        spot, spots, peers = group_peers()
        width = weight_ref.shape[1]
        share, over = share_width(width), overlap_of(width)

        def columns(place):
            start = share * place - over * (place // (GROUP - 1))
            return weight_ref.at[:, pl.ds(pl.multiple_of(start, 128), share)]

        self.copies = [
            send(columns(spots[m]), out_ref.at[spot], send_sem.at[m], recv_sem.at[m], peers[m])
            for m in range(GROUP - 1)
        ]
        self.own_in = pltpu.make_async_copy(columns(spot), stage, own_sem.at[0])
        self.own_out = pltpu.make_async_copy(stage, out_ref.at[spot], own_sem.at[1])
        self.own_in.start()

    def finish(self):
        self.own_in.wait()
        self.own_out.start()
        for copy in self.copies:
            copy.wait()
        self.own_out.wait()


def spread_scratch(rows, share):
    return [
        pltpu.VMEM((rows, share), jnp.bfloat16),
        pltpu.SemaphoreType.DMA((GROUP - 1,)),
        pltpu.SemaphoreType.DMA((GROUP - 1,)),
        pltpu.SemaphoreType.DMA((2,)),
    ]


def spread_shape(weight):
    return jax.ShapeDtypeStruct((GROUP, weight.shape[0], share_width(weight.shape[1])), jnp.bfloat16)


def spread_kernel(count, *refs):
    weights, outs, scratch = refs[:count], refs[count : 2 * count], refs[2 * count :]
    greet(group_peers()[2])
    shares = [
        Spread(weight, out, *scratch[4 * i : 4 * i + 4])
        for i, (weight, out) in enumerate(zip(weights, outs))
    ]
    for each in shares:
        each.finish()


def spread(*weights):
    anywhere = pl.BlockSpec(memory_space=pl.ANY)
    scratch = []
    for weight in weights:
        scratch += spread_scratch(weight.shape[0], share_width(weight.shape[1]))
    return pl.pallas_call(
        functools.partial(spread_kernel, len(weights)),
        name="spread",
        out_shape=[spread_shape(weight) for weight in weights],
        in_specs=[anywhere for _ in weights],
        out_specs=[anywhere for _ in weights],
        scratch_shapes=scratch,
        compiler_params=pltpu.CompilerParams(collective_id=6, has_side_effects=True),
    )(*weights)


class Collect:
    def __init__(self, part_ref, out_ref, slots, send_sem, recv_sem, own_sem):
        spot, spots, peers = group_peers()
        self.out, self.slots = out_ref, slots
        self.copies = [
            send(part_ref.at[spots[m]], slots.at[spot], send_sem.at[m], recv_sem.at[m], peers[m])
            for m in range(GROUP - 1)
        ]
        self.own = pltpu.make_async_copy(part_ref.at[spot], slots.at[spot], own_sem)
        self.own.start()

    def finish(self):
        self.own.wait()
        for copy in self.copies:
            copy.wait()
        rows, width = self.out.shape
        share, over = share_width(width), overlap_of(width)

        def strip(i, carry):
            at = pl.ds(pl.multiple_of(i * STRIP, STRIP), STRIP)
            for place in range(GROUP):
                skip = over * (place // (GROUP - 1))
                self.out[at, share * place : min(share * (place + 1), width)] = self.slots[
                    place, at, skip:share
                ].astype(jnp.float32)
            return carry

        lax.fori_loop(0, rows // STRIP, strip, 0)


def collect_scratch(rows, share):
    return [
        pltpu.VMEM((GROUP, rows, share), jnp.bfloat16),
        pltpu.SemaphoreType.DMA((GROUP - 1,)),
        pltpu.SemaphoreType.DMA((GROUP - 1,)),
        pltpu.SemaphoreType.DMA,
    ]


def final_kernel(
    n, bits, small_ref, gain1_ref, gain2_ref, part_ref, all_ref, gains_ref, grad_ref,
    came, ssem, rsem, gs, gr, *collect_sems
):
    place = lax.axis_index("dp")
    peers = [{"dp": (place + hop) % n} for hop in range(1, n)]
    greet(peers + [across("tensor", bit) for axis, bit in bits if axis == "tensor"])
    copies = [
        send(small_ref, all_ref.at[place], ssem.at[hop], rsem.at[hop], peers[hop])
        for hop in range(n - 1)
    ]
    all_ref[place] = small_ref[...]
    gains_ref[0:1] = gain1_ref[...]
    gains_ref[1:2] = gain2_ref[...]
    moving = None
    for step, (axis, bit) in enumerate(bits):
        copy = send(gains_ref, came.at[step], gs.at[step], gr.at[step], across(axis, bit))
        if moving is None:
            moving = Collect(part_ref, grad_ref, *collect_sems)
        copy.wait()
        gains_ref[...] = gains_ref[...] + came[step]
    moving.finish()
    for copy in copies:
        copy.wait()


def final_pass(small, gain1, gain2, part, hidden_width):
    n = lax.axis_size("dp")
    bits = [
        (axis, bit)
        for axis in ("tensor", "dp")
        for bit in range(lax.axis_size(axis).bit_length() - 1)
    ]
    rows, width = small.shape
    vmem = pl.BlockSpec(memory_space=pltpu.VMEM)
    gains = (2, gain1.shape[1])
    part_rows, share = part.shape[0] // GROUP, part.shape[1]
    return pl.pallas_call(
        functools.partial(final_kernel, n, bits),
        name="final",
        out_shape=(
            jax.ShapeDtypeStruct((n, rows, width), small.dtype),
            jax.ShapeDtypeStruct(gains, jnp.float32),
            jax.ShapeDtypeStruct((part_rows, hidden_width), jnp.float32),
        ),
        in_specs=[vmem] * 3 + [pl.BlockSpec(memory_space=pl.ANY)],
        out_specs=(vmem, vmem, vmem),
        scratch_shapes=[
            pltpu.VMEM((len(bits), *gains), jnp.float32),
            pltpu.SemaphoreType.DMA((n - 1,)),
            pltpu.SemaphoreType.DMA((n - 1,)),
            pltpu.SemaphoreType.DMA((len(bits),)),
            pltpu.SemaphoreType.DMA((len(bits),)),
            *collect_scratch(part_rows, share),
        ],
        compiler_params=pltpu.CompilerParams(
            collective_id=8, has_side_effects=True, vmem_limit_bytes=24 * 2**20
        ),
    )(small, gain1, gain2, part.reshape(GROUP, part_rows, share))


GATHER_SEMS = [
    pltpu.SemaphoreType.DMA((3, 3)),
    pltpu.SemaphoreType.DMA((3, 3)),
    pltpu.SemaphoreType.DMA((10,)),
    pltpu.SemaphoreType.DMA((10,)),
    pltpu.SemaphoreType.DMA,
]


class SumTensor:
    def __init__(self, part_ref, q, core_buf, link_buf, sems_s, sems_r, own_sem):
        high, core = bit_of(*LINKS[2]), bit_of(*CORE)
        core_peer = across(*CORE)
        self.args = high, q, core_buf, link_buf, sems_s, sems_r
        self.own = pltpu.make_async_copy(part_ref.at[:, core], q, own_sem)
        self.own.start()
        self.copies = [
            send(
                part_ref.at[block, 1 - core],
                core_buf.at[block],
                sems_s.at[i],
                sems_r.at[i],
                core_peer,
            )
            for i, block in enumerate((1 - high, high))
        ]

    def pass_on(self):
        high, q, core_buf, link_buf, sems_s, sems_r = self.args
        self.own.wait()
        self.copies[0].wait_recv()
        q[1 - high] = q[1 - high] + core_buf[1 - high]
        self.copies.append(
            send(q.at[1 - high], link_buf, sems_s.at[2], sems_r.at[2], across(*LINKS[2]))
        )

    def arrive(self):
        self.copies[1].wait_recv()
        self.copies[2].wait_recv()

    def rows(self, rows):
        high, q, core_buf, link_buf, _, _ = self.args
        return (
            q[high, rows].astype(jnp.float32)
            + core_buf[high, rows].astype(jnp.float32)
            + link_buf[rows].astype(jnp.float32)
        )

    def finish(self):
        for copy in self.copies:
            copy.wait_send()


SUM_SEMS = [
    pltpu.SemaphoreType.DMA((3,)),
    pltpu.SemaphoreType.DMA((3,)),
    pltpu.SemaphoreType.DMA,
]

def middle_kernel(
    part_ref, tok_ref, cot_ref, gain_ref, resid_ref, all_ref, cot_all_ref,
    q, core_buf, link_buf, low, *sems
):
    greet([across(*link) for link in LINKS] + [across(*CORE)])
    total = SumTensor(part_ref, q, core_buf, link_buf, *sems[:3])
    total.pass_on()
    cots = Gather(cot_ref, cot_all_ref, *sems[8:])
    cots.step(0)
    total.arrive()

    def strip(i, carry):
        rows = pl.ds(pl.multiple_of(i * STRIP, STRIP), STRIP)
        resid = tok_ref[rows].astype(jnp.float32) + total.rows(rows)
        resid_ref[rows] = resid
        inv = lax.rsqrt(jnp.mean(resid * resid, axis=-1, keepdims=True) + epsilon)
        low[rows] = (resid * inv * gain_ref[...]).astype(low.dtype)
        return carry

    lax.fori_loop(0, tok_ref.shape[0] // STRIP, strip, 0)
    total.finish()
    blocks = Gather(low, all_ref, *sems[3:8])
    cots.step(1)
    blocks.step(0)
    blocks.step(1)
    cots.step(2)
    blocks.step(2)
    cots.finish()
    blocks.finish()


def middle(part, tok, cot, gain):
    rows, width = tok.shape
    vmem, anywhere = pl.BlockSpec(memory_space=pltpu.VMEM), pl.BlockSpec(memory_space=pl.ANY)
    return pl.pallas_call(
        middle_kernel,
        name="middle",
        out_shape=(
            jax.ShapeDtypeStruct((rows, width), jnp.float32),
            jax.ShapeDtypeStruct((2, 2, 2, 2, rows, width), jnp.bfloat16),
            jax.ShapeDtypeStruct((2, 2, 2, 2, rows, width), jnp.bfloat16),
        ),
        in_specs=[anywhere, vmem, vmem, vmem],
        out_specs=(vmem, anywhere, anywhere),
        scratch_shapes=[
            pltpu.VMEM((2, rows, width), jnp.bfloat16),
            pltpu.VMEM((2, rows, width), jnp.bfloat16),
            pltpu.VMEM((rows, width), jnp.bfloat16),
            pltpu.VMEM((rows, width), jnp.bfloat16),
            *SUM_SEMS,
            *GATHER_SEMS,
            *GATHER_SEMS,
        ],
        compiler_params=pltpu.CompilerParams(
            collective_id=1, has_side_effects=True, vmem_limit_bytes=32 * 2**20
        ),
    )(part.reshape(2, 2, rows, width), tok, cot, gain.reshape(1, width))


def norm_back(rows, back, base_ref, gain_ref, keep_ref, gain_acc):
    base = base_ref[rows].astype(jnp.float32)
    inv = lax.rsqrt(jnp.mean(base * base, axis=-1, keepdims=True) + epsilon)
    unit = base * inv
    scaled = gain_ref[...] * back
    grad = inv * (scaled - unit * jnp.mean(unit * scaled, axis=-1, keepdims=True))
    terms = back * unit
    gain_acc[...] += terms[:8] + terms[8:]
    return keep_ref[rows].astype(jnp.float32) + grad


def back_kernel(
    p_ref, resid_ref, cot_ref, gain_ref, grad_ref, all_ref, gain_out,
    q, cb, r0, r1, r2, low, gain_acc, ssem, rsem, fs, fr, own_sem, gs, gr, gather_own
):
    me = [bit_of(*link) for link in LINKS]
    core = bit_of(*CORE)
    peers = [across(*link) for link in LINKS]
    core_peer = across(*CORE)
    spans = thirds(q.shape[-1])
    own = pltpu.make_async_copy(p_ref.at[:, :, :, core], q, own_sem)
    own.start()
    greet(peers + [core_peer])

    def half(k, near):
        first = SUM_ORDERS[k][0]
        return [(me[d] if near else 1 - me[d]) if d == first else slice(None) for d in range(3)]

    to_core = []
    for near in (False, True):
        for k in range(3):
            i = half(k, near)
            to_core.append(
                send(
                    p_ref.at[i[0], i[1], i[2], 1 - core, :, pl.ds(*spans[k])],
                    cb.at[i[0], i[1], i[2], :, pl.ds(*spans[k])],
                    fs.at[len(to_core)],
                    fr.at[len(to_core)],
                    core_peer,
                )
            )
    own.wait()

    def add(i, k, other):
        s, n = spans[k]
        q[i[0], i[1], i[2], :, s : s + n] = q[i[0], i[1], i[2], :, s : s + n] + other

    moving, sent = [], []
    for near in (False, True):
        for k in range(3):
            to_core[3 * near + k].wait_recv()
            i = half(k, near)
            s, n = spans[k]
            add(i, k, cb[i[0], i[1], i[2], :, s : s + n])
            if not near:
                moving.append(
                    send(
                        q.at[i[0], i[1], i[2], :, pl.ds(s, n)],
                        r0.at[:, :, :, pl.ds(s, n)],
                        ssem.at[k, 0],
                        rsem.at[k, 0],
                        peers[SUM_ORDERS[k][0]],
                    )
                )
    for step in (1, 2):
        for k in range(3):
            s, n = spans[k]
            order = SUM_ORDERS[k]
            moving[k].wait_recv()
            sent.append(moving[k])
            kept = [me[d] if d in order[:step] else slice(None) for d in range(3)]
            add(kept, k, r0[:, :, :, s : s + n] if step == 1 else r1[:, :, s : s + n])
            away = [
                me[d] if d in order[:step] else (1 - me[d] if d == order[step] else slice(None))
                for d in range(3)
            ]
            moving[k] = send(
                q.at[away[0], away[1], away[2], :, pl.ds(s, n)],
                r1.at[:, :, pl.ds(s, n)] if step == 1 else r2.at[:, pl.ds(s, n)],
                ssem.at[k, step],
                rsem.at[k, step],
                peers[order[step]],
            )
    for k in range(3):
        moving[k].wait_recv()
        sent.append(moving[k])
    gain_acc[...] = jnp.zeros_like(gain_acc)

    def strip(i, carry):
        rows = pl.ds(pl.multiple_of(i * STRIP, STRIP), STRIP)
        back = q[me[0], me[1], me[2], rows].astype(jnp.float32) + r2[rows].astype(jnp.float32)
        grad = norm_back(rows, back, resid_ref, gain_ref, cot_ref, gain_acc)
        grad_ref[rows] = grad
        low[rows] = grad.astype(low.dtype)
        return carry

    lax.fori_loop(0, low.shape[0] // STRIP, strip, 0)
    for copy in sent + to_core:
        copy.wait_send()
    gain_out[...] = jnp.sum(gain_acc[...], axis=0, keepdims=True)
    mine = all_ref.at[me[2], core]
    local = pltpu.make_async_copy(low, mine, gather_own)
    local.start()
    along = send(low, mine, gs.at[0], gr.at[0], peers[2])
    beside = send(low, mine, gs.at[1], gr.at[1], core_peer)
    along.wait_recv()
    theirs = all_ref.at[1 - me[2], core]
    onward = send(theirs, theirs, gs.at[2], gr.at[2], core_peer)
    local.wait()
    beside.wait()
    onward.wait()
    along.wait_send()


def back_pass(part, resid, cot, gain):
    rows, width = resid.shape
    wide = lambda *lead: pltpu.VMEM((*lead, rows, width), jnp.bfloat16)
    vmem = pl.BlockSpec(memory_space=pltpu.VMEM)
    return pl.pallas_call(
        back_kernel,
        name="back",
        out_shape=(
            jax.ShapeDtypeStruct((rows, width), jnp.float32),
            jax.ShapeDtypeStruct((2, 2, rows, width), jnp.bfloat16),
            jax.ShapeDtypeStruct((1, width), jnp.float32),
        ),
        in_specs=[pl.BlockSpec(memory_space=pl.ANY), vmem, vmem, vmem],
        out_specs=(vmem, pl.BlockSpec(memory_space=pl.ANY), vmem),
        scratch_shapes=[
            wide(2, 2, 2),
            wide(2, 2, 2),
            wide(2, 2),
            wide(2),
            wide(),
            wide(),
            pltpu.VMEM((8, width), jnp.float32),
            pltpu.SemaphoreType.DMA((3, 3)),
            pltpu.SemaphoreType.DMA((3, 3)),
            pltpu.SemaphoreType.DMA((6,)),
            pltpu.SemaphoreType.DMA((6,)),
            pltpu.SemaphoreType.DMA,
            pltpu.SemaphoreType.DMA((3,)),
            pltpu.SemaphoreType.DMA((3,)),
            pltpu.SemaphoreType.DMA,
        ],
        compiler_params=pltpu.CompilerParams(
            collective_id=2, has_side_effects=True, vmem_limit_bytes=40 * 2**20
        ),
    )(part.reshape(2, 2, 2, 2, rows, width), resid, cot, gain.reshape(1, width))


class Halve:
    def __init__(self, source, held, came, load_sem, send_sem, recv_sem, order):
        self.held, self.came, self.sems, self.order = held, came, (send_sem, recv_sem), order
        self.dims = sorted(order, reverse=True)
        self.sent, self.loads, at = [], [], 0
        for i, part in enumerate(source):
            rows = part.shape[-2]
            spot = (*[slice(None) for _ in order], pl.ds(at, rows))
            self.loads.append(pltpu.make_async_copy(part, held.at[spot], load_sem.at[i]))
            self.loads[-1].start()
            at += rows

    def index(self, done, away=None):
        picks = []
        for bit in self.dims:
            if bit in done:
                picks.append(bit_of("dp", bit))
            elif bit == away:
                picks.append(1 - bit_of("dp", bit))
            else:
                picks.append(slice(None))
        return tuple(picks)

    def start(self, step):
        if step == 0:
            for load in self.loads:
                load.wait()
        bit = self.order[step]
        self.moving = send(
            self.held.at[self.index(self.order[:step], bit)],
            self.came[step],
            self.sems[0].at[step],
            self.sems[1].at[step],
            across("dp", bit),
        )
        self.sent.append(self.moving)

    def land(self, step):
        self.moving.wait_recv()
        kept = self.index(self.order[: step + 1])
        self.held[kept] = self.held[kept] + self.came[step][...]
        if step + 1 < len(self.order):
            self.start(step + 1)

    def result(self):
        return self.held[self.index(self.order)]

    def finish(self):
        for copy in self.sent:
            copy.wait_send()


def halve_scratch(bits, rows, width):
    scratch = [pltpu.VMEM((*[2] * bits, rows, width), jnp.bfloat16)]
    for step in range(bits):
        scratch.append(pltpu.VMEM((*[2] * (bits - 1 - step), rows, width), jnp.bfloat16))
    return scratch + [
        pltpu.SemaphoreType.DMA((2,)),
        pltpu.SemaphoreType.DMA((bits,)),
        pltpu.SemaphoreType.DMA((bits,)),
    ]


def halver(source, refs, order):
    bits = len(order)
    return Halve(source, refs[0], refs[1 : bits + 1], *refs[bits + 1 : bits + 4], order)


def last_kernel(
    bits, part_ref, tok_ref, keep_ref, gain_ref, wide_ref, few_ref, y_ref, o_ref, gate_ref,
    grad_ref, gain_out, wide_out, few_out, y_out, o_out, gate_out,
    q, core_buf, link_buf, gain_acc, *refs
):
    sum_sems, refs = refs[:3], refs[3:]
    gate_refs, refs = refs[:4], refs[4:]
    blocks = halver((wide_ref, few_ref), refs[: bits + 4], list(range(bits)))
    refs = refs[bits + 4 :]
    sides = [
        halver((source,), refs[i * (bits + 3) : (i + 1) * (bits + 3)], list(range(1, bits)))
        for i, source in enumerate((y_ref, o_ref))
    ]
    peers = [across("dp", bit) for bit in range(bits)]
    greet([across(*LINKS[2]), across(*CORE), group_peers()[2][2]] + peers)
    total = SumTensor(part_ref, q, core_buf, link_buf, *sum_sems)
    blocks.start(0)
    for side in sides:
        side.start(0)
    gates = Collect(gate_ref, gate_out, *gate_refs)
    total.pass_on()
    gain_acc[...] = jnp.zeros_like(gain_acc)

    def strip(i, carry):
        rows = pl.ds(pl.multiple_of(i * STRIP, STRIP), STRIP)
        back = total.rows(rows)
        grad_ref[rows] = norm_back(rows, back, tok_ref, gain_ref, keep_ref, gain_acc)
        return carry

    total.arrive()
    lax.fori_loop(0, tok_ref.shape[0] // STRIP, strip, 0)
    gain_out[...] = jnp.sum(gain_acc[...], axis=0, keepdims=True)
    for step in range(bits):
        if step + 1 < bits:
            for side in sides:
                side.land(step)
        blocks.land(step)
    gates.finish()
    mine = blocks.result()
    wide_out[...] = mine[: wide_out.shape[0]].astype(jnp.float32)
    few_out[...] = mine[wide_out.shape[0] :]
    y_out[...] = sides[0].result().astype(jnp.float32)
    o_out[...] = sides[1].result().astype(jnp.float32)
    for each in (blocks, *sides, total):
        each.finish()


def last_pass(part, tok, keep, gain, wide, few, side_y, side_o, gate, hidden_width):
    rows, width = tok.shape
    vmem, anywhere = pl.BlockSpec(memory_space=pltpu.VMEM), pl.BlockSpec(memory_space=pl.ANY)
    bits = wide.shape[0].bit_length() - 1
    part_rows, share = gate.shape[0] // GROUP, gate.shape[1]
    block = jax.ShapeDtypeStruct(wide.shape[1:], jnp.float32)
    leading = [2] * bits
    return pl.pallas_call(
        functools.partial(last_kernel, bits),
        name="last",
        out_shape=(
            jax.ShapeDtypeStruct((rows, width), jnp.float32),
            jax.ShapeDtypeStruct((1, width), jnp.float32),
            block,
            jax.ShapeDtypeStruct(few.shape[1:], jnp.bfloat16),
            block,
            block,
            jax.ShapeDtypeStruct((part_rows, hidden_width), jnp.float32),
        ),
        in_specs=[anywhere, vmem, vmem, vmem] + [anywhere] * 5,
        out_specs=(vmem,) * 7,
        scratch_shapes=[
            pltpu.VMEM((2, rows, width), jnp.bfloat16),
            pltpu.VMEM((2, rows, width), jnp.bfloat16),
            pltpu.VMEM((rows, width), jnp.bfloat16),
            pltpu.VMEM((8, width), jnp.float32),
            *SUM_SEMS,
            *collect_scratch(part_rows, share),
            *halve_scratch(bits, wide.shape[1] + few.shape[1], wide.shape[2]),
            *halve_scratch(bits - 1, *wide.shape[1:]),
            *halve_scratch(bits - 1, *wide.shape[1:]),
        ],
        compiler_params=pltpu.CompilerParams(
            collective_id=3, has_side_effects=True, vmem_limit_bytes=48 * 2**20
        ),
    )(
        part.reshape(2, 2, rows, width),
        tok,
        keep,
        gain.reshape(1, width),
        wide.reshape(*leading, *wide.shape[1:]),
        few.reshape(*leading, *few.shape[1:]),
        side_y,
        side_o,
        gate.reshape(GROUP, part_rows, share),
    )


def scan_kernel(n, reverse, *refs):
    a_ref, b_ref, *refs = refs
    if reverse:
        part_ref, out_ref, edge_ref, grad_ref, *refs = refs
    else:
        up_ref, down_ref, out_ref, edge_ref, up_out, down_out, *refs = refs
    fa, fb, mine, others, ssem, rsem, *moving_refs = refs
    place = lax.axis_index("dp")
    sign = -1 if reverse else 1
    barrier = pltpu.get_barrier_semaphore()
    peers = [{"dp": (place + sign * hop + n) % n} for hop in range(1, n)]
    for peer in peers:
        pl.semaphore_signal(barrier, inc=1, device_id=peer, device_id_type=MESH)
    rows, width = a_ref.shape
    length = rows // 8
    lanes = range(width // 128)
    for k in lanes:
        fa[k * rows : (k + 1) * rows] = a_ref[:, k * 128 : (k + 1) * 128]
        fb[k * rows : (k + 1) * rows] = b_ref[:, k * 128 : (k + 1) * 128]

    def at(k, r):
        return pl.ds(k * rows + (length - 1 - r if reverse else r), 8, stride=length)

    def local(r, carry):
        result = []
        for k in lanes:
            prod, state = carry[k]
            decay = fa[at(k, r), :]
            term = fb[at(k, r), :]
            if reverse:
                fa[at(k, r), :] = prod
                total = term + state
                fb[at(k, r), :] = total
                result.append((prod * decay, decay * total))
            else:
                prod = prod * decay
                state = decay * state + term
                fa[at(k, r), :] = prod
                fb[at(k, r), :] = state
                result.append((prod, state))
        return result

    start = [(jnp.ones((8, 128), jnp.float32), jnp.zeros((8, 128), jnp.float32)) for k in lanes]
    ends = lax.fori_loop(0, length, local, start, unroll=2)
    prod = jnp.concatenate([end[0] for end in ends], axis=1)
    state = jnp.concatenate([end[1] for end in ends], axis=1)
    order = range(7, -1, -1) if reverse else range(8)
    run_a, run_b = jnp.ones((1, width), jnp.float32), jnp.zeros((1, width), jnp.float32)
    before = [None] * 8
    for s in order:
        before[s] = (run_a, run_b)
        pa, pb = prod[s : s + 1], state[s : s + 1]
        run_a, run_b = pa * run_a, pa * run_b + pb
    mine[0:1] = run_a
    mine[1:2] = run_b
    pl.semaphore_wait(barrier, n - 1)
    copies = [
        send(mine, others.at[hop - 1], ssem.at[hop - 1], rsem.at[hop - 1], peers[hop - 1])
        for hop in range(1, n)
    ]
    if reverse:
        moving = [Collect(part_ref, grad_ref, *moving_refs)]
    else:
        moving = [
            Spread(up_ref, up_out, *moving_refs[:4]),
            Spread(down_ref, down_out, *moving_refs[4:]),
        ]
    carry = jnp.zeros((1, width), jnp.float32)
    ahead = n - 1 - place if reverse else place
    for copy in copies:
        copy.wait_recv()
    for hop in range(n - 1, 0, -1):
        step = others[hop - 1, 0:1] * carry + others[hop - 1, 1:2]
        carry = jnp.where(hop <= ahead, step, carry)
    edge_ref[...] = carry
    entering = jnp.concatenate([pa * carry + pb for pa, pb in before], axis=0)

    def fix(r, c):
        for k in lanes:
            fb[at(k, r), :] = fb[at(k, r), :] + fa[at(k, r), :] * entering[:, k * 128 : (k + 1) * 128]
        return c

    lax.fori_loop(0, length, fix, 0, unroll=2)
    for k in lanes:
        out_ref[:, k * 128 : (k + 1) * 128] = fb[k * rows : (k + 1) * rows]
    for copy in copies:
        copy.wait_send()
    for each in moving:
        each.finish()


def scan_stream(decay, term, reverse, moved, hidden_width):
    n = lax.axis_size("dp")
    rows, width = decay.shape
    vmem, anywhere = pl.BlockSpec(memory_space=pltpu.VMEM), pl.BlockSpec(memory_space=pl.ANY)
    out_shape = [
        jax.ShapeDtypeStruct((rows, width), jnp.float32),
        jax.ShapeDtypeStruct((1, width), jnp.float32),
    ]
    scratch = [
        pltpu.VMEM((rows * width // 128, 128), jnp.float32),
        pltpu.VMEM((rows * width // 128, 128), jnp.float32),
        pltpu.VMEM((2, width), jnp.float32),
        pltpu.VMEM((n - 1, 2, width), jnp.float32),
        pltpu.SemaphoreType.DMA((n - 1,)),
        pltpu.SemaphoreType.DMA((n - 1,)),
    ]
    if reverse:
        part_rows, share = moved.shape[0] // GROUP, moved.shape[1]
        moved = (moved.reshape(GROUP, part_rows, share),)
        out_specs = [vmem]
        out_shape.append(jax.ShapeDtypeStruct((part_rows, hidden_width), jnp.float32))
        scratch += collect_scratch(part_rows, share)
    else:
        out_specs = [anywhere, anywhere]
        out_shape += [spread_shape(weight) for weight in moved]
        for weight in moved:
            scratch += spread_scratch(weight.shape[0], share_width(weight.shape[1]))
    return pl.pallas_call(
        functools.partial(scan_kernel, n, reverse),
        name="scan_back" if reverse else "scan",
        out_shape=out_shape,
        in_specs=[vmem, vmem] + [anywhere for _ in moved],
        out_specs=[vmem, vmem] + out_specs,
        scratch_shapes=scratch,
        compiler_params=pltpu.CompilerParams(
            collective_id=5 if reverse else 4, has_side_effects=True, vmem_limit_bytes=32 * 2**20
        ),
    )(decay, term, *moved)


def in_order(bit, mine, theirs, axis=0):
    return jnp.where(
        bit == 0, jnp.concatenate([mine, theirs], axis), jnp.concatenate([theirs, mine], axis)
    )


def halve_once(blocks):
    bits = blocks.shape[0].bit_length() - 1
    mine = lax.axis_index("dp") % 2
    held = blocks.reshape(*[2] * bits, *blocks.shape[1:])
    keep = lax.dynamic_index_in_dim(held, mine, bits - 1, False)
    away = lax.dynamic_index_in_dim(held, 1 - mine, bits - 1, False)
    came = flipped(away, "dp", 1)
    return (keep.astype(jnp.float32) + came.astype(jnp.float32)).astype(jnp.bfloat16)


def local(
    tokens,
    doc_start,
    norm1_gain,
    proj_x,
    proj_y,
    conv_weight,
    conv_bias,
    gate_x_weight,
    gate_x_bias,
    gate_a_weight,
    gate_a_bias,
    decay_param,
    proj_out,
    norm2_gain,
    mlp_gate,
    mlp_up,
    mlp_down,
    cotangent,
):
    tok_rows = tokens.shape[0]
    chan_width = proj_x.shape[1]
    block_width = gate_x_weight.shape[0]
    half_width = block_width // 2
    tap_count = conv_weight.shape[0]
    parity = lax.axis_index("tensor") % 2
    full_start = parity * half_width
    shared_start = (1 - parity) * 2 * block_width
    tensor_size = lax.axis_size("tensor")
    share_rows = tok_rows // tensor_size
    own_start = lax.axis_index("tensor") * share_rows
    positions = lax.axis_index("dp") * tok_rows + lax.iota(jnp.int32, tok_rows)
    starting = (doc_start == positions)[:, None]
    groups = [
        [(g * GROUP + i) * tensor_size + t for i in range(GROUP) for t in range(tensor_size)]
        for g in range(lax.axis_size("dp") // GROUP)
    ]
    everyone = ("dp", "tensor")

    dp_size = lax.axis_size("dp")
    spot = lax.axis_index("dp") % GROUP
    across_blocks = [[i + GROUP * g for g in range(dp_size // GROUP)] for i in range(GROUP)]
    hidden_width = mlp_gate.shape[1]
    share = share_width(hidden_width)

    def all_rows(part):
        flat = part.reshape(-1, share)
        return lax.all_gather(flat, "dp", axis_index_groups=across_blocks, tiled=True)

    gate_cols = all_rows(*spread(mlp_gate))
    tok_own = lax.dynamic_slice_in_dim(tokens, own_start, share_rows, 0)
    cot_own = lax.dynamic_slice_in_dim(cotangent, own_start, share_rows, 0)

    def normalize(values):
        values = values.astype(jnp.float32)
        inv_rms = lax.rsqrt(jnp.mean(values * values, axis=-1, keepdims=True) + epsilon)
        return (values * inv_rms * norm1_gain).astype(jnp.bfloat16)

    halo = 16
    normed_low = normalize(tokens)
    normed_prev = normalize(shifted(tokens[tok_rows - halo :], "dp", 1))
    branch_y = matmul(normed_low, proj_y)
    branch_x = matmul(normed_low, proj_x).astype(jnp.bfloat16)
    prev_x = matmul(normed_prev, proj_x).astype(jnp.bfloat16)
    extended = jnp.concatenate([prev_x[halo - tap_count + 1 :], branch_x], axis=0).astype(
        jnp.float32
    )

    def conv_apply(ext_rows, weight, bias_vec):
        conv_out = bias_vec + weight[0] * ext_rows[tap_count - 1 :]
        for offset in range(1, tap_count):
            inside = (positions - offset >= doc_start).astype(jnp.float32)[:, None]
            lagged = ext_rows[tap_count - 1 - offset : tap_count - 1 - offset + tok_rows]
            conv_out = conv_out + weight[offset] * lagged * inside
        return conv_out

    conv_out, conv_pull = jax.vjp(conv_apply, extended, conv_weight, conv_bias)
    mixed_low = conv_out.astype(jnp.bfloat16)
    own_half = lax.dynamic_slice_in_dim(mixed_low, shared_start, half_width, 1)
    other_half = flipped(own_half, "tensor", 1)
    shared_in = in_order(parity, own_half, other_half, 1)
    full_in = lax.dynamic_slice_in_dim(mixed_low, full_start, 2 * block_width, 1).reshape(
        tok_rows, 2, block_width
    )

    def place(full_part, shared_part):
        return in_order(parity, full_part, shared_part, 1)

    def full_weight(weight):
        return lax.dynamic_slice_in_dim(weight, full_start, 2 * block_width, 1).reshape(
            block_width, 2, block_width
        )

    def shared_weight(weight):
        return lax.dynamic_slice_in_dim(weight, shared_start, half_width, 1)

    def gate_pre(weight, bias_vec):
        full_out = jnp.einsum(
            "nhi,ihj->nhj", full_in, full_weight(weight), preferred_element_type=jnp.float32
        ).reshape(tok_rows, 2 * block_width)
        shared_out = matmul(shared_in, shared_weight(weight))
        return place(full_out, shared_out) + bias_vec

    def recurrence_in(conv_vals, pre_input, pre_recur, param_vec):
        log_decay = -8.0 * jax.nn.sigmoid(pre_recur) * jax.nn.softplus(param_vec)
        decay = jnp.where(starting, 0.0, jnp.exp(log_decay))
        multiplier = jnp.where(starting, 1.0, jnp.sqrt(-jnp.expm1(2.0 * log_decay)))
        return (decay, multiplier * jax.nn.sigmoid(pre_input) * conv_vals)

    pre_input = gate_pre(gate_x_weight, gate_x_bias)
    pre_recur = gate_pre(gate_a_weight, gate_a_bias)
    (decay, drive), recur_pull = jax.vjp(
        recurrence_in, mixed_low.astype(jnp.float32), pre_input, pre_recur, decay_param
    )
    states, entering, up_part, down_part = scan_stream(
        decay, drive, False, (mlp_up, mlp_down), hidden_width
    )
    up_cols, down_cols = all_rows(up_part), all_rows(down_part)
    previous = jnp.concatenate([entering, states[:-1]], axis=0)
    gelu_y, gelu_pull = jax.vjp(gelu_tanh, branch_y)
    product_low = (states * gelu_y).astype(jnp.bfloat16)
    resid, normed2_all, cot_all = middle(
        matmul(product_low, proj_out).astype(jnp.bfloat16), tok_own, cot_own, norm2_gain
    )
    normed2_all = normed2_all.reshape(GROUP * tok_rows, -1)
    cot_all = cot_all.reshape(GROUP * tok_rows, -1)
    counted = lax.iota(jnp.int32, share) >= overlap_of(hidden_width) * (spot // (GROUP - 1))

    def once(values):
        return jnp.where(counted, values, 0.0).astype(jnp.bfloat16)

    gate_act = matmul(normed2_all, gate_cols)
    up_act = matmul(normed2_all, up_cols)
    hidden, act_pull = jax.vjp(gated_product, gate_act, up_act)
    hidden_low = once(hidden)
    grad_hidden = matmul(cot_all, down_cols)
    grad_gate, grad_up = act_pull(grad_hidden)
    grad_gate_low = once(grad_gate)
    grad_up_low = once(grad_up)

    def own_rows(grad):
        return lax.psum_scatter(
            grad.astype(jnp.bfloat16),
            "dp",
            axis_index_groups=across_blocks,
            scatter_dimension=0,
            tiled=True,
        )

    back_part = (
        contract_last(grad_gate_low, gate_cols) + contract_last(grad_up_low, up_cols)
    ).astype(jnp.bfloat16)
    down_grad = contract_first(cot_all, hidden_low).astype(jnp.bfloat16)
    back_part, down_grad = lax.optimization_barrier((back_part, down_grad))
    down_rows = own_rows(down_grad)
    grad_resid, grad_lru_low, grad_gain2 = back_pass(back_part, resid, cot_own, norm2_gain)
    grad_lru_low = grad_lru_low.reshape(tok_rows, -1)
    gate_rows = own_rows(contract_first(normed2_all, grad_gate_low))
    up_rows = own_rows(contract_first(normed2_all, grad_up_low))
    block_out = resid + lax.psum_scatter(
        contract_last(hidden_low, down_cols).astype(jnp.bfloat16),
        everyone,
        axis_index_groups=groups,
        scatter_dimension=0,
        tiled=True,
    ).astype(jnp.float32)

    grad_product = contract_last(grad_lru_low, proj_out)
    grad_states = grad_product * gelu_y
    grad_y_low = gelu_pull(grad_product * states)[0].astype(jnp.bfloat16)
    total_grad, _, grad_mlp_down = scan_stream(decay, grad_states, True, down_rows, hidden_width)
    total_grad, late_y, late_lru = lax.optimization_barrier(
        (total_grad, grad_y_low, grad_lru_low)
    )

    def token_sum(left_rows, right_rows):
        return contract_first(left_rows, right_rows).astype(jnp.bfloat16)

    def per_device(rows):
        return rows.reshape(dp_size, rows.shape[0] // dp_size, rows.shape[1])

    side_y = halve_once(per_device(token_sum(normed_low, late_y)))
    side_o = halve_once(per_device(token_sum(late_lru, product_low)))
    conv_direct, grad_pre_input, grad_pre_recur, grad_param = recur_pull(
        (total_grad * previous, total_grad)
    )

    def gate_back(weight, grad_pre):
        grad_pre_low = grad_pre.astype(jnp.bfloat16)
        grad_full = lax.dynamic_slice_in_dim(grad_pre_low, full_start, 2 * block_width, 1).reshape(
            tok_rows, 2, block_width
        )
        grad_share = lax.dynamic_slice_in_dim(grad_pre_low, shared_start, half_width, 1)
        into_full = jnp.einsum(
            "nhj,ihj->nhi", grad_full, full_weight(weight), preferred_element_type=jnp.float32
        ).reshape(tok_rows, 2 * block_width)
        into_share = contract_last(grad_share, shared_weight(weight))
        weight_full = jnp.einsum(
            "nhi,nhj->ihj", full_in, grad_full, preferred_element_type=jnp.float32
        ).reshape(block_width, 2 * block_width)
        weight_share = contract_first(shared_in, grad_share)
        return (into_full, into_share, place(weight_full, weight_share))

    input_full, input_share, grad_gx_weight = gate_back(gate_x_weight, grad_pre_input)
    recur_full, recur_share, grad_ga_weight = gate_back(gate_a_weight, grad_pre_recur)
    full_sum = input_full + recur_full
    share_sum = input_share + recur_share
    own_grad = jnp.where(parity == 0, share_sum[:, :half_width], share_sum[:, half_width:])
    other_grad = jnp.where(parity == 0, share_sum[:, half_width:], share_sum[:, :half_width])
    returned = flipped(other_grad.astype(jnp.bfloat16), "tensor", 1).astype(other_grad.dtype)
    grad_conv = conv_direct + place(full_sum, own_grad + returned)
    grad_extended, grad_conv_weight, grad_conv_bias = conv_pull(grad_conv)
    rim_grad = shifted(grad_extended[: tap_count - 1], "dp", -1)
    grad_branch_x = grad_extended[tap_count - 1 :] + jnp.concatenate(
        [jnp.zeros((tok_rows - tap_count + 1, chan_width), jnp.float32), rim_grad], axis=0
    )
    grad_x_low = grad_branch_x.astype(jnp.bfloat16)
    wide = jnp.concatenate([grad_gx_weight, grad_ga_weight], axis=0)
    sums = jnp.concatenate(
        [
            grad_conv_weight,
            grad_conv_bias[None],
            jnp.sum(grad_pre_input, axis=0)[None],
            jnp.sum(grad_pre_recur, axis=0)[None],
            grad_param[None],
        ],
        axis=0,
    )
    spare = dp_size * 16 - sums.shape[0]
    sums = jnp.concatenate([sums, jnp.zeros((spare, chan_width), jnp.float32)], axis=0)
    few = jnp.concatenate(
        [per_device(wide.astype(jnp.bfloat16)), per_device(sums.astype(jnp.bfloat16))], axis=1
    )
    grad_tokens, grad_gain1, grad_proj_x, reduced, grad_proj_y, grad_out, grad_mlp_gate = last_pass(
        (contract_last(grad_x_low, proj_x) + contract_last(grad_y_low, proj_y)).astype(
            jnp.bfloat16
        ),
        tok_own,
        grad_resid,
        norm1_gain,
        per_device(token_sum(normed_low, grad_x_low)),
        few,
        side_y,
        side_o,
        gate_rows,
        hidden_width,
    )
    grad_proj_out = grad_out.T
    shared, gains, grad_mlp_up = final_pass(reduced, grad_gain1, grad_gain2, up_rows, hidden_width)
    wide_rows = 2 * block_width // dp_size
    wide = shared[:, :wide_rows].reshape(2 * block_width, chan_width).astype(jnp.float32)
    small = shared[:, wide_rows:].reshape(dp_size * 16, chan_width).astype(jnp.float32)
    return (
        block_out,
        grad_tokens,
        gains[0],
        grad_proj_x,
        grad_proj_y,
        small[:tap_count],
        small[tap_count],
        wide[:block_width],
        small[tap_count + 1],
        wide[block_width:],
        small[tap_count + 2],
        small[tap_count + 3],
        grad_proj_out,
        gains[1],
        grad_mlp_gate,
        grad_mlp_up,
        grad_mlp_down,
    )


def solution(mesh):
    placed = (
        P("dp", None),
        P("dp"),
        P(),
        P(None, "tensor"),
        P(None, "tensor"),
        P(None, "tensor"),
        P("tensor"),
        P(None, "tensor"),
        P("tensor"),
        P(None, "tensor"),
        P("tensor"),
        P("tensor"),
        P("tensor", None),
        P(),
        P("dp", "tensor"),
        P("dp", "tensor"),
        P("dp", "tensor"),
        P("dp", None),
    )
    return jax.shard_map(
        local,
        mesh=mesh,
        in_specs=placed,
        out_specs=(
            P(("dp", "tensor"), None),
            P(("dp", "tensor"), None),
            P(),
            P("dp", "tensor"),
            P("dp", "tensor"),
            P(None, "tensor"),
            P("tensor"),
            P(None, "tensor"),
            P("tensor"),
            P(None, "tensor"),
            P("tensor"),
            P("tensor"),
            P("tensor", "dp"),
            P(),
            P("dp", "tensor"),
            P("dp", "tensor"),
            P("dp", "tensor"),
        ),
        check_vma=False,
    )
```

```python
import functools

import jax
import jax.numpy as jnp
from jax import lax
from jax.experimental import pallas as pl
from jax.experimental.pallas import tpu as pltpu
from jax.sharding import PartitionSpec as P

epsilon = 1e-06
MESH = pl.DeviceIdType.MESH
GROUP = 4
STRIP = 16
FIRST_BIT = 1
LINKS = (("dp", FIRST_BIT + 1), ("dp", FIRST_BIT), ("tensor", 1))
CORE = ("tensor", 0)
ORDERS = ((0, 1, 2), (0, 2, 1))
SUM_ORDERS = tuple(order[::-1] for order in ORDERS)
COLORS = range(len(ORDERS))


def gelu_tanh(values):
    return jax.nn.gelu(values, approximate=True)


def gated_product(gate_vals, up_vals):
    return gelu_tanh(gate_vals) * up_vals


def contract_last(left_rows, right_rows):
    return lax.dot_general(
        left_rows, right_rows, (((1,), (1,)), ((), ())), preferred_element_type=jnp.float32
    )


def contract_first(left_rows, right_rows):
    return lax.dot_general(
        left_rows, right_rows, (((0,), (0,)), ((), ())), preferred_element_type=jnp.float32
    )


def matmul(left_rows, right_rows):
    return jnp.dot(left_rows, right_rows, preferred_element_type=jnp.float32)


def shifted(block, axis, distance):
    devices = range(lax.axis_size(axis))
    route = [(i - distance, i) for i in devices if i - distance in devices]
    return lax.ppermute(block, axis, route)


def flipped(array, axis, mask):
    return lax.ppermute(array, axis, [(i, i ^ mask) for i in range(lax.axis_size(axis))])


def bit_of(axis, bit):
    return (lax.axis_index(axis) // (1 << bit)) % 2


def across(axis, bit):
    index = lax.axis_index(axis)
    return {axis: index + (1 - 2 * ((index // (1 << bit)) % 2)) * (1 << bit)}


def column_spans(width):
    most = width // 128 * 3 // 4 * 128
    return ((0, most), (most, width - most))


def send(src, dst, send_sem, recv_sem, device):
    copy = pltpu.make_async_remote_copy(
        src_ref=src,
        dst_ref=dst,
        send_sem=send_sem,
        recv_sem=recv_sem,
        device_id=device,
        device_id_type=MESH,
    )
    copy.start()
    return copy


def greet(devices):
    barrier = pltpu.get_barrier_semaphore()
    for device in devices:
        pl.semaphore_signal(barrier, inc=1, device_id=device, device_id_type=MESH)
    pl.semaphore_wait(barrier, len(devices))


class Gather:
    def __init__(self, x_ref, out_ref, send_sem, recv_sem, core_send, core_recv, own_sem):
        self.sems = send_sem, recv_sem, core_send, core_recv
        self.out = out_ref
        self.me = [bit_of(*link) for link in LINKS]
        self.core = bit_of(*CORE)
        self.peers = [across(*link) for link in LINKS]
        self.core_peer = across(*CORE)
        self.spans = column_spans(x_ref.shape[1])
        me, place = self.me, out_ref.at[self.me[0], self.me[1], self.me[2], self.core]
        self.own = pltpu.make_async_copy(x_ref, place, own_sem)
        self.own.start()
        self.moving = [
            send(
                x_ref.at[:, pl.ds(*self.spans[k])],
                self.region(me, k),
                send_sem.at[k, 0],
                recv_sem.at[k, 0],
                self.peers[ORDERS[k][0]],
            )
            for k in COLORS
        ]
        self.to_core = [send(x_ref, place, core_send.at[3 * len(ORDERS)], core_recv.at[3 * len(ORDERS)], self.core_peer)]
        self.sent = []

    def region(self, idx, k):
        return self.out.at[idx[0], idx[1], idx[2], self.core, :, pl.ds(*self.spans[k])]

    def step(self, step):
        send_sem, recv_sem, core_send, core_recv = self.sems
        me = self.me
        if step == 0:
            self.own.wait()
        for k in COLORS:
            order = ORDERS[k]
            self.moving[k].wait_recv()
            self.sent.append(self.moving[k])
            if step < 2:
                held = [slice(None) if d in order[: step + 1] else me[d] for d in range(3)]
                self.moving[k] = send(
                    self.region(held, k),
                    self.region(held, k),
                    send_sem.at[k, step + 1],
                    recv_sem.at[k, step + 1],
                    self.peers[order[step + 1]],
                )
            fresh = [
                slice(None) if d in order[:step] else (1 - me[d] if d == order[step] else me[d])
                for d in range(3)
            ]
            self.to_core.append(
                send(
                    self.region(fresh, k),
                    self.region(fresh, k),
                    core_send.at[len(ORDERS) * step + k],
                    core_recv.at[len(ORDERS) * step + k],
                    self.core_peer,
                )
            )

    def finish(self):
        for copy in self.sent:
            copy.wait_send()
        for copy in self.to_core:
            copy.wait()


def spots_of_four():
    spot = lax.axis_index("dp") // (1 << FIRST_BIT) % GROUP
    return spot, spot + 1 - 2 * (spot % 2), spot + 2 - 4 * (spot // 2), GROUP - 1 - spot


def share_width(width):
    return -(-width // (128 * GROUP)) * 128


def overlap_of(width):
    return GROUP * share_width(width) - width


def cut_kernel(count, *refs):
    width = refs[0].shape[1]
    share, over = share_width(width), overlap_of(width)
    for spot, out in zip(spots_of_four(), refs[count:]):
        start = share * spot - over * (spot // (GROUP - 1))
        for i in range(count):
            out[i] = refs[i][:, pl.ds(pl.multiple_of(start, 128), share)]


def cut(*weights):
    rows, share = weights[0].shape[0], share_width(weights[0].shape[1])
    return pl.pallas_call(
        functools.partial(cut_kernel, len(weights)),
        name="cut",
        out_shape=[jax.ShapeDtypeStruct((len(weights), rows, share), jnp.bfloat16)] * GROUP,
        compiler_params=pltpu.CompilerParams(vmem_limit_bytes=24 * 2**20),
    )(*weights)


def place_kernel(count, *refs):
    for spot, piece in zip(spots_of_four(), refs[:GROUP]):
        for i in range(count):
            refs[GROUP + i][spot] = piece[i]


def placed(pieces):
    count, rows, share = pieces[0].shape
    return pl.pallas_call(
        functools.partial(place_kernel, count),
        name="place",
        out_shape=[jax.ShapeDtypeStruct((GROUP, rows, share), jnp.bfloat16)] * count,
        compiler_params=pltpu.CompilerParams(vmem_limit_bytes=24 * 2**20),
    )(*pieces)


def pick_kernel(count, *refs):
    for spot, out in zip(spots_of_four(), refs[count:]):
        for i in range(count):
            out[i] = refs[i][spot]


def picked(*parts):
    _, rows, share = parts[0].shape
    return pl.pallas_call(
        functools.partial(pick_kernel, len(parts)),
        name="pick",
        out_shape=[jax.ShapeDtypeStruct((len(parts), rows, share), jnp.bfloat16)] * GROUP,
        compiler_params=pltpu.CompilerParams(vmem_limit_bytes=24 * 2**20),
    )(*parts)


def join_kernel(count, *refs):
    pieces, outs, slots = refs[:GROUP], refs[GROUP : GROUP + count], refs[GROUP + count]
    for spot, piece in zip(spots_of_four(), pieces):
        for i in range(count):
            slots[i, spot] = piece[i]
    rows, width = outs[0].shape
    share, over = share_width(width), overlap_of(width)

    def strip(step, carry):
        at = pl.ds(pl.multiple_of(step * STRIP, STRIP), STRIP)
        for i in range(count):
            for place in range(GROUP):
                skip = over * (place // (GROUP - 1))
                outs[i][at, share * place : min(share * (place + 1), width)] = slots[
                    i, place, at, skip:share
                ].astype(jnp.float32)
        return carry

    lax.fori_loop(0, rows // STRIP, strip, 0)


def joined(pieces, width):
    count, rows, share = pieces[0].shape
    return pl.pallas_call(
        functools.partial(join_kernel, count),
        name="join",
        out_shape=[jax.ShapeDtypeStruct((rows, width), jnp.float32)] * count,
        scratch_shapes=[pltpu.VMEM((count, GROUP, rows, share), jnp.bfloat16)],
        compiler_params=pltpu.CompilerParams(vmem_limit_bytes=32 * 2**20),
    )(*pieces)


def exchanged(pieces):
    return [pieces[0]] + [flipped(pieces[m], "dp", m << FIRST_BIT) for m in range(1, GROUP)]


def final_kernel(
    n, bits, small_ref, gain1_ref, gain2_ref, all_ref, gains_ref, came, ssem, rsem, gs, gr
):
    place = lax.axis_index("dp")
    peers = [{"dp": (place + hop) % n} for hop in range(1, n)]
    greet(peers + [across("tensor", bit) for axis, bit in bits if axis == "tensor"])
    copies = [
        send(small_ref, all_ref.at[place], ssem.at[hop], rsem.at[hop], peers[hop])
        for hop in range(n - 1)
    ]
    all_ref[place] = small_ref[...]
    gains_ref[0:1] = gain1_ref[...]
    gains_ref[1:2] = gain2_ref[...]
    for step, (axis, bit) in enumerate(bits):
        copy = send(gains_ref, came.at[step], gs.at[step], gr.at[step], across(axis, bit))
        copy.wait()
        gains_ref[...] = gains_ref[...] + came[step]
    for copy in copies:
        copy.wait()


def final_pass(small, gain1, gain2):
    n = lax.axis_size("dp")
    bits = [
        (axis, bit)
        for axis in ("tensor", "dp")
        for bit in range(lax.axis_size(axis).bit_length() - 1)
    ]
    rows, width = small.shape
    vmem = pl.BlockSpec(memory_space=pltpu.VMEM)
    gains = (2, gain1.shape[1])
    return pl.pallas_call(
        functools.partial(final_kernel, n, bits),
        name="final",
        out_shape=(
            jax.ShapeDtypeStruct((n, rows, width), small.dtype),
            jax.ShapeDtypeStruct(gains, jnp.float32),
        ),
        in_specs=[vmem] * 3,
        out_specs=(vmem, vmem),
        scratch_shapes=[
            pltpu.VMEM((len(bits), *gains), jnp.float32),
            pltpu.SemaphoreType.DMA((n - 1,)),
            pltpu.SemaphoreType.DMA((n - 1,)),
            pltpu.SemaphoreType.DMA((len(bits),)),
            pltpu.SemaphoreType.DMA((len(bits),)),
        ],
        compiler_params=pltpu.CompilerParams(
            collective_id=8, has_side_effects=True, vmem_limit_bytes=24 * 2**20
        ),
    )(small, gain1, gain2)


GATHER_SEMS = [
    pltpu.SemaphoreType.DMA((len(ORDERS), 3)),
    pltpu.SemaphoreType.DMA((len(ORDERS), 3)),
    pltpu.SemaphoreType.DMA((3 * len(ORDERS) + 1,)),
    pltpu.SemaphoreType.DMA((3 * len(ORDERS) + 1,)),
    pltpu.SemaphoreType.DMA,
]


class SumTensor:
    def __init__(self, part_ref, q, core_buf, link_buf, sems_s, sems_r, own_sem):
        high, core = bit_of(*LINKS[2]), bit_of(*CORE)
        core_peer = across(*CORE)
        self.args = high, q, core_buf, link_buf, sems_s, sems_r
        self.own = pltpu.make_async_copy(part_ref.at[:, core], q, own_sem)
        self.own.start()
        self.copies = [
            send(
                part_ref.at[block, 1 - core],
                core_buf.at[block],
                sems_s.at[i],
                sems_r.at[i],
                core_peer,
            )
            for i, block in enumerate((1 - high, high))
        ]

    def pass_on(self):
        high, q, core_buf, link_buf, sems_s, sems_r = self.args
        self.own.wait()
        self.copies[0].wait_recv()
        q[1 - high] = q[1 - high] + core_buf[1 - high]
        self.copies.append(
            send(q.at[1 - high], link_buf, sems_s.at[2], sems_r.at[2], across(*LINKS[2]))
        )

    def arrive(self):
        self.copies[1].wait_recv()
        self.copies[2].wait_recv()

    def rows(self, rows):
        high, q, core_buf, link_buf, _, _ = self.args
        return (
            q[high, rows].astype(jnp.float32)
            + core_buf[high, rows].astype(jnp.float32)
            + link_buf[rows].astype(jnp.float32)
        )

    def finish(self):
        for copy in self.copies:
            copy.wait_send()


SUM_SEMS = [
    pltpu.SemaphoreType.DMA((3,)),
    pltpu.SemaphoreType.DMA((3,)),
    pltpu.SemaphoreType.DMA,
]

def middle_kernel(
    part_ref, tok_ref, gain_ref, resid_ref, all_ref, q, core_buf, link_buf, low, *sems
):
    greet([across(*link) for link in LINKS] + [across(*CORE)])
    total = SumTensor(part_ref, q, core_buf, link_buf, *sems[:3])
    total.pass_on()
    total.arrive()

    def strip(i, carry):
        rows = pl.ds(pl.multiple_of(i * STRIP, STRIP), STRIP)
        resid = tok_ref[rows].astype(jnp.float32) + total.rows(rows)
        resid_ref[rows] = resid
        inv = lax.rsqrt(jnp.mean(resid * resid, axis=-1, keepdims=True) + epsilon)
        low[rows] = (resid * inv * gain_ref[...]).astype(low.dtype)
        return carry

    lax.fori_loop(0, tok_ref.shape[0] // STRIP, strip, 0)
    total.finish()
    blocks = Gather(low, all_ref, *sems[3:])
    for step in range(3):
        blocks.step(step)
    blocks.finish()


def middle(part, tok, gain):
    rows, width = tok.shape
    vmem, anywhere = pl.BlockSpec(memory_space=pltpu.VMEM), pl.BlockSpec(memory_space=pl.ANY)
    return pl.pallas_call(
        middle_kernel,
        name="middle",
        out_shape=(
            jax.ShapeDtypeStruct((rows, width), jnp.float32),
            jax.ShapeDtypeStruct((2, 2, 2, 2, rows, width), jnp.bfloat16),
        ),
        in_specs=[anywhere, vmem, vmem],
        out_specs=(vmem, anywhere),
        scratch_shapes=[
            pltpu.VMEM((2, rows, width), jnp.bfloat16),
            pltpu.VMEM((2, rows, width), jnp.bfloat16),
            pltpu.VMEM((rows, width), jnp.bfloat16),
            pltpu.VMEM((rows, width), jnp.bfloat16),
            *SUM_SEMS,
            *GATHER_SEMS,
        ],
        compiler_params=pltpu.CompilerParams(
            collective_id=1, has_side_effects=True, vmem_limit_bytes=32 * 2**20
        ),
    )(part.reshape(2, 2, rows, width), tok, gain.reshape(1, width))


def norm_back(rows, back, base_ref, gain_ref, keep_ref, gain_acc):
    base = base_ref[rows].astype(jnp.float32)
    inv = lax.rsqrt(jnp.mean(base * base, axis=-1, keepdims=True) + epsilon)
    unit = base * inv
    scaled = gain_ref[...] * back
    grad = inv * (scaled - unit * jnp.mean(unit * scaled, axis=-1, keepdims=True))
    terms = back * unit
    gain_acc[...] += terms[:8] + terms[8:]
    return keep_ref[rows].astype(jnp.float32) + grad


def back_kernel(
    p_ref, resid_ref, cot_ref, gain_ref, grad_ref, all_ref, gain_out,
    q, cb, r0, r1, r2, low, gain_acc, ssem, rsem, fs, fr, own_sem, gs, gr, gather_own
):
    me = [bit_of(*link) for link in LINKS]
    core = bit_of(*CORE)
    peers = [across(*link) for link in LINKS]
    core_peer = across(*CORE)
    spans = column_spans(q.shape[-1])
    own = pltpu.make_async_copy(p_ref.at[:, :, :, core], q, own_sem)
    own.start()
    greet(peers + [core_peer])

    def half(k, near):
        first = SUM_ORDERS[k][0]
        return [(me[d] if near else 1 - me[d]) if d == first else slice(None) for d in range(3)]

    to_core = []
    for near in (False, True):
        for k in COLORS:
            i = half(k, near)
            to_core.append(
                send(
                    p_ref.at[i[0], i[1], i[2], 1 - core, :, pl.ds(*spans[k])],
                    cb.at[i[0], i[1], i[2], :, pl.ds(*spans[k])],
                    fs.at[len(to_core)],
                    fr.at[len(to_core)],
                    core_peer,
                )
            )
    own.wait()

    def add(i, k, other):
        s, n = spans[k]
        q[i[0], i[1], i[2], :, s : s + n] = q[i[0], i[1], i[2], :, s : s + n] + other

    moving, sent = [], []
    for near in (False, True):
        for k in COLORS:
            to_core[len(ORDERS) * near + k].wait_recv()
            i = half(k, near)
            s, n = spans[k]
            add(i, k, cb[i[0], i[1], i[2], :, s : s + n])
            if not near:
                moving.append(
                    send(
                        q.at[i[0], i[1], i[2], :, pl.ds(s, n)],
                        r0.at[:, :, :, pl.ds(s, n)],
                        ssem.at[k, 0],
                        rsem.at[k, 0],
                        peers[SUM_ORDERS[k][0]],
                    )
                )
    for step in (1, 2):
        for k in COLORS:
            s, n = spans[k]
            order = SUM_ORDERS[k]
            moving[k].wait_recv()
            sent.append(moving[k])
            kept = [me[d] if d in order[:step] else slice(None) for d in range(3)]
            add(kept, k, r0[:, :, :, s : s + n] if step == 1 else r1[:, :, s : s + n])
            away = [
                me[d] if d in order[:step] else (1 - me[d] if d == order[step] else slice(None))
                for d in range(3)
            ]
            moving[k] = send(
                q.at[away[0], away[1], away[2], :, pl.ds(s, n)],
                r1.at[:, :, pl.ds(s, n)] if step == 1 else r2.at[:, pl.ds(s, n)],
                ssem.at[k, step],
                rsem.at[k, step],
                peers[order[step]],
            )
    for k in COLORS:
        moving[k].wait_recv()
        sent.append(moving[k])
    gain_acc[...] = jnp.zeros_like(gain_acc)

    def strip(i, carry):
        rows = pl.ds(pl.multiple_of(i * STRIP, STRIP), STRIP)
        back = q[me[0], me[1], me[2], rows].astype(jnp.float32) + r2[rows].astype(jnp.float32)
        grad = norm_back(rows, back, resid_ref, gain_ref, cot_ref, gain_acc)
        grad_ref[rows] = grad
        low[rows] = grad.astype(low.dtype)
        return carry

    lax.fori_loop(0, low.shape[0] // STRIP, strip, 0)
    for copy in sent + to_core:
        copy.wait_send()
    gain_out[...] = jnp.sum(gain_acc[...], axis=0, keepdims=True)
    mine = all_ref.at[me[2], core]
    local = pltpu.make_async_copy(low, mine, gather_own)
    local.start()
    along = send(low, mine, gs.at[0], gr.at[0], peers[2])
    beside = send(low, mine, gs.at[1], gr.at[1], core_peer)
    along.wait_recv()
    theirs = all_ref.at[1 - me[2], core]
    onward = send(theirs, theirs, gs.at[2], gr.at[2], core_peer)
    local.wait()
    beside.wait()
    onward.wait()
    along.wait_send()


def back_pass(part, resid, cot, gain):
    rows, width = resid.shape
    wide = lambda *lead: pltpu.VMEM((*lead, rows, width), jnp.bfloat16)
    vmem = pl.BlockSpec(memory_space=pltpu.VMEM)
    return pl.pallas_call(
        back_kernel,
        name="back",
        out_shape=(
            jax.ShapeDtypeStruct((rows, width), jnp.float32),
            jax.ShapeDtypeStruct((2, 2, rows, width), jnp.bfloat16),
            jax.ShapeDtypeStruct((1, width), jnp.float32),
        ),
        in_specs=[pl.BlockSpec(memory_space=pl.ANY), vmem, vmem, vmem],
        out_specs=(vmem, pl.BlockSpec(memory_space=pl.ANY), vmem),
        scratch_shapes=[
            wide(2, 2, 2),
            wide(2, 2, 2),
            wide(2, 2),
            wide(2),
            wide(),
            wide(),
            pltpu.VMEM((8, width), jnp.float32),
            pltpu.SemaphoreType.DMA((len(ORDERS), 3)),
            pltpu.SemaphoreType.DMA((len(ORDERS), 3)),
            pltpu.SemaphoreType.DMA((2 * len(ORDERS),)),
            pltpu.SemaphoreType.DMA((2 * len(ORDERS),)),
            pltpu.SemaphoreType.DMA,
            pltpu.SemaphoreType.DMA((3,)),
            pltpu.SemaphoreType.DMA((3,)),
            pltpu.SemaphoreType.DMA,
        ],
        compiler_params=pltpu.CompilerParams(
            collective_id=2, has_side_effects=True, vmem_limit_bytes=40 * 2**20
        ),
    )(part.reshape(2, 2, 2, 2, rows, width), resid, cot, gain.reshape(1, width))


class Halve:
    def __init__(self, source, held, came, load_sem, send_sem, recv_sem, order):
        self.held, self.came, self.sems, self.order = held, came, (send_sem, recv_sem), order
        self.dims = sorted(order, reverse=True)
        self.sent, self.loads, at = [], [], 0
        for i, part in enumerate(source):
            rows = part.shape[-2]
            spot = (*[slice(None) for _ in order], pl.ds(at, rows))
            self.loads.append(pltpu.make_async_copy(part, held.at[spot], load_sem.at[i]))
            self.loads[-1].start()
            at += rows

    def index(self, done, away=None):
        picks = []
        for bit in self.dims:
            if bit in done:
                picks.append(bit_of("dp", bit))
            elif bit == away:
                picks.append(1 - bit_of("dp", bit))
            else:
                picks.append(slice(None))
        return tuple(picks)

    def start(self, step):
        if step == 0:
            for load in self.loads:
                load.wait()
        bit = self.order[step]
        self.moving = send(
            self.held.at[self.index(self.order[:step], bit)],
            self.came[step],
            self.sems[0].at[step],
            self.sems[1].at[step],
            across("dp", bit),
        )
        self.sent.append(self.moving)

    def land(self, step):
        self.moving.wait_recv()
        kept = self.index(self.order[: step + 1])
        self.held[kept] = self.held[kept] + self.came[step][...]
        if step + 1 < len(self.order):
            self.start(step + 1)

    def result(self):
        return self.held[self.index(self.order)]

    def finish(self):
        for copy in self.sent:
            copy.wait_send()


def halve_scratch(bits, rows, width):
    scratch = [pltpu.VMEM((*[2] * bits, rows, width), jnp.bfloat16)]
    for step in range(bits):
        scratch.append(pltpu.VMEM((*[2] * (bits - 1 - step), rows, width), jnp.bfloat16))
    return scratch + [
        pltpu.SemaphoreType.DMA((2,)),
        pltpu.SemaphoreType.DMA((bits,)),
        pltpu.SemaphoreType.DMA((bits,)),
    ]


def halver(source, refs, order):
    bits = len(order)
    return Halve(source, refs[0], refs[1 : bits + 1], *refs[bits + 1 : bits + 4], order)


def last_kernel(
    bits, part_ref, tok_ref, keep_ref, gain_ref, wide_ref, few_ref, y_ref, o_ref,
    grad_ref, gain_out, wide_out, few_out, y_out, o_out,
    q, core_buf, link_buf, gain_acc, *refs
):
    sum_sems, refs = refs[:3], refs[3:]
    blocks = halver((wide_ref, few_ref), refs[: bits + 4], list(range(bits)))
    refs = refs[bits + 4 :]
    sides = [
        halver((source,), refs[i * (bits + 3) : (i + 1) * (bits + 3)], list(range(1, bits)))
        for i, source in enumerate((y_ref, o_ref))
    ]
    peers = [across("dp", bit) for bit in range(bits)]
    greet([across(*LINKS[2]), across(*CORE)] + peers)
    total = SumTensor(part_ref, q, core_buf, link_buf, *sum_sems)
    blocks.start(0)
    for side in sides:
        side.start(0)
    total.pass_on()
    gain_acc[...] = jnp.zeros_like(gain_acc)

    def strip(i, carry):
        rows = pl.ds(pl.multiple_of(i * STRIP, STRIP), STRIP)
        back = total.rows(rows)
        grad_ref[rows] = norm_back(rows, back, tok_ref, gain_ref, keep_ref, gain_acc)
        return carry

    total.arrive()
    lax.fori_loop(0, tok_ref.shape[0] // STRIP, strip, 0)
    gain_out[...] = jnp.sum(gain_acc[...], axis=0, keepdims=True)
    for step in range(bits):
        if step + 1 < bits:
            for side in sides:
                side.land(step)
        blocks.land(step)
    mine = blocks.result()
    wide_out[...] = mine[: wide_out.shape[0]].astype(jnp.float32)
    few_out[...] = mine[wide_out.shape[0] :]
    y_out[...] = sides[0].result().astype(jnp.float32)
    o_out[...] = sides[1].result().astype(jnp.float32)
    for each in (blocks, *sides, total):
        each.finish()


def last_pass(part, tok, keep, gain, wide, few, side_y, side_o):
    rows, width = tok.shape
    vmem, anywhere = pl.BlockSpec(memory_space=pltpu.VMEM), pl.BlockSpec(memory_space=pl.ANY)
    bits = wide.shape[0].bit_length() - 1
    block = jax.ShapeDtypeStruct(wide.shape[1:], jnp.float32)
    leading = [2] * bits
    return pl.pallas_call(
        functools.partial(last_kernel, bits),
        name="last",
        out_shape=(
            jax.ShapeDtypeStruct((rows, width), jnp.float32),
            jax.ShapeDtypeStruct((1, width), jnp.float32),
            block,
            jax.ShapeDtypeStruct(few.shape[1:], jnp.bfloat16),
            block,
            block,
        ),
        in_specs=[anywhere, vmem, vmem, vmem] + [anywhere] * 4,
        out_specs=(vmem,) * 6,
        scratch_shapes=[
            pltpu.VMEM((2, rows, width), jnp.bfloat16),
            pltpu.VMEM((2, rows, width), jnp.bfloat16),
            pltpu.VMEM((rows, width), jnp.bfloat16),
            pltpu.VMEM((8, width), jnp.float32),
            *SUM_SEMS,
            *halve_scratch(bits, wide.shape[1] + few.shape[1], wide.shape[2]),
            *halve_scratch(bits - 1, *wide.shape[1:]),
            *halve_scratch(bits - 1, *wide.shape[1:]),
        ],
        compiler_params=pltpu.CompilerParams(
            collective_id=3, has_side_effects=True, vmem_limit_bytes=48 * 2**20
        ),
    )(
        part.reshape(2, 2, rows, width),
        tok,
        keep,
        gain.reshape(1, width),
        wide.reshape(*leading, *wide.shape[1:]),
        few.reshape(*leading, *few.shape[1:]),
        side_y,
        side_o,
    )


def scan_kernel(n, reverse, *refs):
    a_ref, b_ref, out_ref, edge_ref, fa, fb, mine, others, ssem, rsem = refs
    place = lax.axis_index("dp")
    sign = -1 if reverse else 1
    barrier = pltpu.get_barrier_semaphore()
    peers = [{"dp": (place + sign * hop + n) % n} for hop in range(1, n)]
    for peer in peers:
        pl.semaphore_signal(barrier, inc=1, device_id=peer, device_id_type=MESH)
    rows, width = a_ref.shape
    length = rows // 8
    lanes = range(width // 128)
    for k in lanes:
        fa[k * rows : (k + 1) * rows] = a_ref[:, k * 128 : (k + 1) * 128]
        fb[k * rows : (k + 1) * rows] = b_ref[:, k * 128 : (k + 1) * 128]

    def at(k, r):
        return pl.ds(k * rows + (length - 1 - r if reverse else r), 8, stride=length)

    def local(r, carry):
        result = []
        for k in lanes:
            prod, state = carry[k]
            decay = fa[at(k, r), :]
            term = fb[at(k, r), :]
            if reverse:
                fa[at(k, r), :] = prod
                total = term + state
                fb[at(k, r), :] = total
                result.append((prod * decay, decay * total))
            else:
                prod = prod * decay
                state = decay * state + term
                fa[at(k, r), :] = prod
                fb[at(k, r), :] = state
                result.append((prod, state))
        return result

    start = [(jnp.ones((8, 128), jnp.float32), jnp.zeros((8, 128), jnp.float32)) for k in lanes]
    ends = lax.fori_loop(0, length, local, start, unroll=2)
    prod = jnp.concatenate([end[0] for end in ends], axis=1)
    state = jnp.concatenate([end[1] for end in ends], axis=1)
    order = range(7, -1, -1) if reverse else range(8)
    run_a, run_b = jnp.ones((1, width), jnp.float32), jnp.zeros((1, width), jnp.float32)
    before = [None] * 8
    for s in order:
        before[s] = (run_a, run_b)
        pa, pb = prod[s : s + 1], state[s : s + 1]
        run_a, run_b = pa * run_a, pa * run_b + pb
    mine[0:1] = run_a
    mine[1:2] = run_b
    pl.semaphore_wait(barrier, n - 1)
    copies = [
        send(mine, others.at[hop - 1], ssem.at[hop - 1], rsem.at[hop - 1], peers[hop - 1])
        for hop in range(1, n)
    ]
    carry = jnp.zeros((1, width), jnp.float32)
    ahead = n - 1 - place if reverse else place
    for copy in copies:
        copy.wait_recv()
    for hop in range(n - 1, 0, -1):
        step = others[hop - 1, 0:1] * carry + others[hop - 1, 1:2]
        carry = jnp.where(hop <= ahead, step, carry)
    edge_ref[...] = carry
    entering = jnp.concatenate([pa * carry + pb for pa, pb in before], axis=0)

    def fix(r, c):
        for k in lanes:
            fb[at(k, r), :] = fb[at(k, r), :] + fa[at(k, r), :] * entering[:, k * 128 : (k + 1) * 128]
        return c

    lax.fori_loop(0, length, fix, 0, unroll=2)
    for k in lanes:
        out_ref[:, k * 128 : (k + 1) * 128] = fb[k * rows : (k + 1) * rows]
    for copy in copies:
        copy.wait_send()


def scan_stream(decay, term, reverse):
    n = lax.axis_size("dp")
    rows, width = decay.shape
    vmem = pl.BlockSpec(memory_space=pltpu.VMEM)
    return pl.pallas_call(
        functools.partial(scan_kernel, n, reverse),
        name="scan_back" if reverse else "scan",
        out_shape=(
            jax.ShapeDtypeStruct((rows, width), jnp.float32),
            jax.ShapeDtypeStruct((1, width), jnp.float32),
        ),
        in_specs=[vmem, vmem],
        out_specs=(vmem, vmem),
        scratch_shapes=[
            pltpu.VMEM((rows * width // 128, 128), jnp.float32),
            pltpu.VMEM((rows * width // 128, 128), jnp.float32),
            pltpu.VMEM((2, width), jnp.float32),
            pltpu.VMEM((n - 1, 2, width), jnp.float32),
            pltpu.SemaphoreType.DMA((n - 1,)),
            pltpu.SemaphoreType.DMA((n - 1,)),
        ],
        compiler_params=pltpu.CompilerParams(
            collective_id=5 if reverse else 4, has_side_effects=True, vmem_limit_bytes=32 * 2**20
        ),
    )(decay, term)


def in_order(bit, mine, theirs, axis=0):
    return jnp.where(
        bit == 0, jnp.concatenate([mine, theirs], axis), jnp.concatenate([theirs, mine], axis)
    )


def halves(blocks):
    bits = blocks.shape[0].bit_length() - 1
    mine = lax.axis_index("dp") % 2
    held = blocks.reshape(*[2] * bits, *blocks.shape[1:])
    return (
        lax.dynamic_index_in_dim(held, mine, bits - 1, False),
        lax.dynamic_index_in_dim(held, 1 - mine, bits - 1, False),
    )


def halved(keep, away):
    came = flipped(away, "dp", 1)
    return (keep.astype(jnp.float32) + came.astype(jnp.float32)).astype(jnp.bfloat16)


def local(
    tokens,
    doc_start,
    norm1_gain,
    proj_x,
    proj_y,
    conv_weight,
    conv_bias,
    gate_x_weight,
    gate_x_bias,
    gate_a_weight,
    gate_a_bias,
    decay_param,
    proj_out,
    norm2_gain,
    mlp_gate,
    mlp_up,
    mlp_down,
    cotangent,
):
    tok_rows = tokens.shape[0]
    chan_width = proj_x.shape[1]
    block_width = gate_x_weight.shape[0]
    half_width = block_width // 2
    tap_count = conv_weight.shape[0]
    parity = lax.axis_index("tensor") % 2
    full_start = parity * half_width
    shared_start = (1 - parity) * 2 * block_width
    tensor_size = lax.axis_size("tensor")
    share_rows = tok_rows // tensor_size
    own_start = lax.axis_index("tensor") * share_rows
    positions = lax.axis_index("dp") * tok_rows + lax.iota(jnp.int32, tok_rows)
    starting = (doc_start == positions)[:, None]
    dp_size = lax.axis_size("dp")
    low_size = 1 << FIRST_BIT
    high_size = dp_size // (GROUP * low_size)

    def dp_index(high, four, low):
        return (high * GROUP + four) * low_size + low

    highs, fours, lows = range(high_size), range(GROUP), range(low_size)
    groups = [
        [dp_index(h, i, l) * tensor_size + t for i in fours for t in range(tensor_size)]
        for h in highs
        for l in lows
    ]
    low_groups = [[dp_index(h, i, l) for l in lows] for h in highs for i in fours]
    high_groups = [[dp_index(h, i, l) for h in highs] for i in fours for l in lows]
    everyone = ("dp", "tensor")

    spot = lax.axis_index("dp") // low_size % GROUP
    hidden_width = mlp_gate.shape[1]
    share = share_width(hidden_width)

    def all_rows(part):
        rows = part.shape[1]
        part = lax.all_gather(
            part[:, None], "dp", axis=1, axis_index_groups=low_groups, tiled=True
        )
        if high_size > 1:
            part = lax.all_gather(part, "dp", axis=0, axis_index_groups=high_groups, tiled=True)
        return part.reshape(dp_size * rows, share)

    def own_rows(grad):
        rows = grad.shape[0] // dp_size
        grad = grad.astype(jnp.bfloat16).reshape(high_size * GROUP, low_size, rows, share)
        if high_size > 1:
            grad = lax.psum_scatter(
                grad, "dp", axis_index_groups=high_groups, scatter_dimension=0, tiled=True
            )
        grad = lax.psum_scatter(
            grad, "dp", axis_index_groups=low_groups, scatter_dimension=1, tiled=True
        )
        return grad.reshape(GROUP, rows, share)

    cot_own = lax.dynamic_slice_in_dim(cotangent, own_start, share_rows, 0)
    cot_all = lax.all_gather(cot_own, everyone, axis_index_groups=groups, tiled=True)
    pieces = exchanged(cut(mlp_gate, mlp_up, mlp_down))
    tok_own = lax.dynamic_slice_in_dim(tokens, own_start, share_rows, 0)

    def normalize(values):
        values = values.astype(jnp.float32)
        inv_rms = lax.rsqrt(jnp.mean(values * values, axis=-1, keepdims=True) + epsilon)
        return (values * inv_rms * norm1_gain).astype(jnp.bfloat16)

    halo = 16
    normed_low = normalize(tokens)
    normed_prev = normalize(shifted(tokens[tok_rows - halo :], "dp", 1))
    branch_y = matmul(normed_low, proj_y)
    branch_x = matmul(normed_low, proj_x).astype(jnp.bfloat16)
    prev_x = matmul(normed_prev, proj_x).astype(jnp.bfloat16)
    extended = jnp.concatenate([prev_x[halo - tap_count + 1 :], branch_x], axis=0).astype(
        jnp.float32
    )

    def conv_apply(ext_rows, weight, bias_vec):
        conv_out = bias_vec + weight[0] * ext_rows[tap_count - 1 :]
        for offset in range(1, tap_count):
            inside = (positions - offset >= doc_start).astype(jnp.float32)[:, None]
            lagged = ext_rows[tap_count - 1 - offset : tap_count - 1 - offset + tok_rows]
            conv_out = conv_out + weight[offset] * lagged * inside
        return conv_out

    conv_out, conv_pull = jax.vjp(conv_apply, extended, conv_weight, conv_bias)
    mixed_low = conv_out.astype(jnp.bfloat16)
    own_half = lax.dynamic_slice_in_dim(mixed_low, shared_start, half_width, 1)
    other_half = flipped(own_half, "tensor", 1)
    shared_in = in_order(parity, own_half, other_half, 1)
    full_in = lax.dynamic_slice_in_dim(mixed_low, full_start, 2 * block_width, 1).reshape(
        tok_rows, 2, block_width
    )

    def place(full_part, shared_part):
        return in_order(parity, full_part, shared_part, 1)

    def full_weight(weight):
        return lax.dynamic_slice_in_dim(weight, full_start, 2 * block_width, 1).reshape(
            block_width, 2, block_width
        )

    def shared_weight(weight):
        return lax.dynamic_slice_in_dim(weight, shared_start, half_width, 1)

    def gate_pre(weight, bias_vec):
        full_out = jnp.einsum(
            "nhi,ihj->nhj", full_in, full_weight(weight), preferred_element_type=jnp.float32
        ).reshape(tok_rows, 2 * block_width)
        shared_out = matmul(shared_in, shared_weight(weight))
        return place(full_out, shared_out) + bias_vec

    def recurrence_in(conv_vals, pre_input, pre_recur, param_vec):
        log_decay = -8.0 * jax.nn.sigmoid(pre_recur) * jax.nn.softplus(param_vec)
        decay = jnp.where(starting, 0.0, jnp.exp(log_decay))
        multiplier = jnp.where(starting, 1.0, jnp.sqrt(-jnp.expm1(2.0 * log_decay)))
        return (decay, multiplier * jax.nn.sigmoid(pre_input) * conv_vals)

    pre_input = gate_pre(gate_x_weight, gate_x_bias)
    pre_recur = gate_pre(gate_a_weight, gate_a_bias)
    (decay, drive), recur_pull = jax.vjp(
        recurrence_in, mixed_low.astype(jnp.float32), pre_input, pre_recur, decay_param
    )
    decay, drive, *pieces = lax.optimization_barrier((decay, drive, *pieces))
    gate_cols, up_cols, down_cols = (all_rows(part) for part in placed(pieces))
    states, entering = scan_stream(decay, drive, False)
    previous = jnp.concatenate([entering, states[:-1]], axis=0)
    gelu_y, gelu_pull = jax.vjp(gelu_tanh, branch_y)
    product_low = (states * gelu_y).astype(jnp.bfloat16)
    lru_part = matmul(product_low, proj_out).astype(jnp.bfloat16)
    lru_part, cot_all = lax.optimization_barrier((lru_part, cot_all))
    resid, normed2_all = middle(lru_part, tok_own, norm2_gain)
    normed2_all = normed2_all.reshape(GROUP * tok_rows, -1)
    counted = lax.iota(jnp.int32, share) >= overlap_of(hidden_width) * (spot // (GROUP - 1))

    def once(values):
        return jnp.where(counted, values, 0.0).astype(jnp.bfloat16)

    gate_act = matmul(normed2_all, gate_cols)
    up_act = matmul(normed2_all, up_cols)
    hidden, act_pull = jax.vjp(gated_product, gate_act, up_act)
    hidden_low = once(hidden)
    grad_hidden = matmul(cot_all, down_cols)
    grad_gate, grad_up = act_pull(grad_hidden)
    grad_gate_low = once(grad_gate)
    grad_up_low = once(grad_up)

    back_part = (
        contract_last(grad_gate_low, gate_cols) + contract_last(grad_up_low, up_cols)
    ).astype(jnp.bfloat16)
    down_grad = contract_first(cot_all, hidden_low).astype(jnp.bfloat16)
    back_part, down_grad = lax.optimization_barrier((back_part, down_grad))
    down_rows = own_rows(down_grad)
    grad_resid, grad_lru_low, grad_gain2 = back_pass(back_part, resid, cot_own, norm2_gain)
    grad_lru_low = grad_lru_low.reshape(tok_rows, -1)
    gate_rows = own_rows(contract_first(normed2_all, grad_gate_low))
    up_rows = own_rows(contract_first(normed2_all, grad_up_low))
    block_out = resid + lax.psum_scatter(
        contract_last(hidden_low, down_cols).astype(jnp.bfloat16),
        everyone,
        axis_index_groups=groups,
        scatter_dimension=0,
        tiled=True,
    ).astype(jnp.float32)

    grad_product = contract_last(grad_lru_low, proj_out)
    grad_states = grad_product * gelu_y
    grad_y_low = gelu_pull(grad_product * states)[0].astype(jnp.bfloat16)
    total_grad, _ = scan_stream(decay, grad_states, True)
    total_grad, late_y, late_lru, *rows = lax.optimization_barrier(
        (total_grad, grad_y_low, grad_lru_low, down_rows, gate_rows, up_rows)
    )

    def token_sum(left_rows, right_rows):
        return contract_first(left_rows, right_rows).astype(jnp.bfloat16)

    def per_device(rows):
        return rows.reshape(dp_size, rows.shape[0] // dp_size, rows.shape[1])

    keep_y, away_y = halves(per_device(token_sum(normed_low, late_y)))
    keep_o, away_o = halves(per_device(token_sum(late_lru, product_low)))
    total_grad, away_y, away_o = lax.optimization_barrier((total_grad, away_y, away_o))
    side_y, side_o = halved(keep_y, away_y), halved(keep_o, away_o)
    row_pieces = exchanged(picked(*rows))
    conv_direct, grad_pre_input, grad_pre_recur, grad_param = recur_pull(
        (total_grad * previous, total_grad)
    )

    def gate_back(weight, grad_pre):
        grad_pre_low = grad_pre.astype(jnp.bfloat16)
        grad_full = lax.dynamic_slice_in_dim(grad_pre_low, full_start, 2 * block_width, 1).reshape(
            tok_rows, 2, block_width
        )
        grad_share = lax.dynamic_slice_in_dim(grad_pre_low, shared_start, half_width, 1)
        into_full = jnp.einsum(
            "nhj,ihj->nhi", grad_full, full_weight(weight), preferred_element_type=jnp.float32
        ).reshape(tok_rows, 2 * block_width)
        into_share = contract_last(grad_share, shared_weight(weight))
        weight_full = jnp.einsum(
            "nhi,nhj->ihj", full_in, grad_full, preferred_element_type=jnp.float32
        ).reshape(block_width, 2 * block_width)
        weight_share = contract_first(shared_in, grad_share)
        return (into_full, into_share, place(weight_full, weight_share))

    input_full, input_share, grad_gx_weight = gate_back(gate_x_weight, grad_pre_input)
    recur_full, recur_share, grad_ga_weight = gate_back(gate_a_weight, grad_pre_recur)
    full_sum = input_full + recur_full
    share_sum = input_share + recur_share
    own_grad = jnp.where(parity == 0, share_sum[:, :half_width], share_sum[:, half_width:])
    other_grad = jnp.where(parity == 0, share_sum[:, half_width:], share_sum[:, :half_width])
    returned = flipped(other_grad.astype(jnp.bfloat16), "tensor", 1).astype(other_grad.dtype)
    grad_conv = conv_direct + place(full_sum, own_grad + returned)
    grad_extended, grad_conv_weight, grad_conv_bias = conv_pull(grad_conv)
    rim_grad = shifted(grad_extended[: tap_count - 1], "dp", -1)
    grad_branch_x = grad_extended[tap_count - 1 :] + jnp.concatenate(
        [jnp.zeros((tok_rows - tap_count + 1, chan_width), jnp.float32), rim_grad], axis=0
    )
    grad_x_low = grad_branch_x.astype(jnp.bfloat16)
    wide = jnp.concatenate([grad_gx_weight, grad_ga_weight], axis=0)
    sums = jnp.concatenate(
        [
            grad_conv_weight,
            grad_conv_bias[None],
            jnp.sum(grad_pre_input, axis=0)[None],
            jnp.sum(grad_pre_recur, axis=0)[None],
            grad_param[None],
        ],
        axis=0,
    )
    spare = dp_size * 16 - sums.shape[0]
    sums = jnp.concatenate([sums, jnp.zeros((spare, chan_width), jnp.float32)], axis=0)
    few = jnp.concatenate(
        [per_device(wide.astype(jnp.bfloat16)), per_device(sums.astype(jnp.bfloat16))], axis=1
    )
    grad_tokens, grad_gain1, grad_proj_x, reduced, grad_proj_y, grad_out = last_pass(
        (contract_last(grad_x_low, proj_x) + contract_last(grad_y_low, proj_y)).astype(
            jnp.bfloat16
        ),
        tok_own,
        grad_resid,
        norm1_gain,
        per_device(token_sum(normed_low, grad_x_low)),
        few,
        side_y,
        side_o,
    )
    grad_proj_out = grad_out.T
    shared, gains = final_pass(reduced, grad_gain1, grad_gain2)
    gains, *row_pieces = lax.optimization_barrier((gains, *row_pieces))
    grad_mlp_down, grad_mlp_gate, grad_mlp_up = joined(row_pieces, hidden_width)
    wide_rows = 2 * block_width // dp_size
    wide = shared[:, :wide_rows].reshape(2 * block_width, chan_width).astype(jnp.float32)
    small = shared[:, wide_rows:].reshape(dp_size * 16, chan_width).astype(jnp.float32)
    return (
        block_out,
        grad_tokens,
        gains[0],
        grad_proj_x,
        grad_proj_y,
        small[:tap_count],
        small[tap_count],
        wide[:block_width],
        small[tap_count + 1],
        wide[block_width:],
        small[tap_count + 2],
        small[tap_count + 3],
        grad_proj_out,
        gains[1],
        grad_mlp_gate,
        grad_mlp_up,
        grad_mlp_down,
    )


def solution(mesh):
    placed = (
        P("dp", None),
        P("dp"),
        P(),
        P(None, "tensor"),
        P(None, "tensor"),
        P(None, "tensor"),
        P("tensor"),
        P(None, "tensor"),
        P("tensor"),
        P(None, "tensor"),
        P("tensor"),
        P("tensor"),
        P("tensor", None),
        P(),
        P("dp", "tensor"),
        P("dp", "tensor"),
        P("dp", "tensor"),
        P("dp", None),
    )
    return jax.shard_map(
        local,
        mesh=mesh,
        in_specs=placed,
        out_specs=(
            P(("dp", "tensor"), None),
            P(("dp", "tensor"), None),
            P(),
            P("dp", "tensor"),
            P("dp", "tensor"),
            P(None, "tensor"),
            P("tensor"),
            P(None, "tensor"),
            P("tensor"),
            P(None, "tensor"),
            P("tensor"),
            P("tensor"),
            P("tensor", "dp"),
            P(),
            P("dp", "tensor"),
            P("dp", "tensor"),
            P("dp", "tensor"),
        ),
        check_vma=False,
    )
```

```python
import functools

import jax
import jax.numpy as jnp
from jax import lax
from jax.experimental import pallas as pl
from jax.experimental.pallas import tpu as pltpu
from jax.sharding import PartitionSpec as P


epsilon = 1e-06
MESH = pl.DeviceIdType.MESH
GROUP = 4
STRIP = 16
FIRST_BIT = 0
LINKS = (("dp", FIRST_BIT + 1), ("dp", FIRST_BIT), ("tensor", 1))
CORE = ("tensor", 0)
ORDERS = ((0, 1, 2), (0, 2, 1), (1, 2, 0), (2, 0, 1))
TILES = (8, 3, 5)
SUM_ORDERS = tuple(order[::-1] for order in ORDERS)
COLORS = range(len(ORDERS))


def gelu_tanh(values):
    return jax.nn.gelu(values, approximate=True)


def gated_product(gate_vals, up_vals):
    return gelu_tanh(gate_vals) * up_vals


def contract_last(left_rows, right_rows):
    return lax.dot_general(
        left_rows, right_rows, (((1,), (1,)), ((), ())), preferred_element_type=jnp.float32
    )


def contract_first(left_rows, right_rows):
    return lax.dot_general(
        left_rows, right_rows, (((0,), (0,)), ((), ())), preferred_element_type=jnp.float32
    )


def matmul(left_rows, right_rows):
    return jnp.dot(left_rows, right_rows, preferred_element_type=jnp.float32)


def shifted(block, axis, distance):
    devices = range(lax.axis_size(axis))
    route = [(i - distance, i) for i in devices if i - distance in devices]
    return lax.ppermute(block, axis, route)


def flipped(array, axis, mask):
    return lax.ppermute(array, axis, [(i, i ^ mask) for i in range(lax.axis_size(axis))])


def bit_of(axis, bit):
    return (lax.axis_index(axis) // (1 << bit)) % 2


def across(axis, bit):
    index = lax.axis_index(axis)
    return {axis: index + (1 - 2 * ((index // (1 << bit)) % 2)) * (1 << bit)}


def column_spans(width):
    tiles = width // 128
    counts = [tiles * part // 20 for part in TILES]
    spans, start = [], 0
    for count in (*counts, tiles - sum(counts)):
        spans.append((start * 128, count * 128))
        start += count
    return spans


def send(src, dst, send_sem, recv_sem, device):
    copy = pltpu.make_async_remote_copy(
        src_ref=src,
        dst_ref=dst,
        send_sem=send_sem,
        recv_sem=recv_sem,
        device_id=device,
        device_id_type=MESH,
    )
    copy.start()
    return copy


def greet(devices):
    barrier = pltpu.get_barrier_semaphore()
    for device in devices:
        pl.semaphore_signal(barrier, inc=1, device_id=device, device_id_type=MESH)
    pl.semaphore_wait(barrier, len(devices))


class Gather:
    def __init__(self, x_ref, out_ref, send_sem, recv_sem, core_send, core_recv, own_sem):
        self.sems = send_sem, recv_sem, core_send, core_recv
        self.out = out_ref
        self.me = [bit_of(*link) for link in LINKS]
        self.core = bit_of(*CORE)
        self.peers = [across(*link) for link in LINKS]
        self.core_peer = across(*CORE)
        self.spans = column_spans(x_ref.shape[1])
        me, place = self.me, out_ref.at[self.me[0], self.me[1], self.me[2], self.core]
        self.own = pltpu.make_async_copy(x_ref, place, own_sem)
        self.own.start()
        self.moving = [
            send(
                x_ref.at[:, pl.ds(*self.spans[k])],
                self.region(me, k),
                send_sem.at[k, 0],
                recv_sem.at[k, 0],
                self.peers[ORDERS[k][0]],
            )
            for k in COLORS
        ]
        self.to_core = [send(x_ref, place, core_send.at[3 * len(ORDERS)], core_recv.at[3 * len(ORDERS)], self.core_peer)]
        self.sent = []

    def region(self, idx, k):
        return self.out.at[idx[0], idx[1], idx[2], self.core, :, pl.ds(*self.spans[k])]

    def step(self, step):
        send_sem, recv_sem, core_send, core_recv = self.sems
        me = self.me
        if step == 0:
            self.own.wait()
        for k in COLORS:
            order = ORDERS[k]
            self.moving[k].wait_recv()
            self.sent.append(self.moving[k])
            if step < 2:
                held = [slice(None) if d in order[: step + 1] else me[d] for d in range(3)]
                self.moving[k] = send(
                    self.region(held, k),
                    self.region(held, k),
                    send_sem.at[k, step + 1],
                    recv_sem.at[k, step + 1],
                    self.peers[order[step + 1]],
                )
            fresh = [
                slice(None) if d in order[:step] else (1 - me[d] if d == order[step] else me[d])
                for d in range(3)
            ]
            self.to_core.append(
                send(
                    self.region(fresh, k),
                    self.region(fresh, k),
                    core_send.at[len(ORDERS) * step + k],
                    core_recv.at[len(ORDERS) * step + k],
                    self.core_peer,
                )
            )

    def finish(self):
        for copy in self.sent:
            copy.wait_send()
        for copy in self.to_core:
            copy.wait()


def spots_of_four():
    spot = lax.axis_index("dp") // (1 << FIRST_BIT) % GROUP
    return spot, spot + 1 - 2 * (spot % 2), spot + 2 - 4 * (spot // 2), GROUP - 1 - spot


def share_width(width):
    return -(-width // (128 * GROUP)) * 128


def overlap_of(width):
    return GROUP * share_width(width) - width


def cut_kernel(count, *refs):
    width = refs[0].shape[1]
    share, over = share_width(width), overlap_of(width)
    for spot, out in zip(spots_of_four(), refs[count:]):
        start = share * spot - over * (spot // (GROUP - 1))
        for i in range(count):
            out[i] = refs[i][:, pl.ds(pl.multiple_of(start, 128), share)]


def cut(*weights):
    rows, share = weights[0].shape[0], share_width(weights[0].shape[1])
    return pl.pallas_call(
        functools.partial(cut_kernel, len(weights)),
        name="cut",
        out_shape=[jax.ShapeDtypeStruct((len(weights), rows, share), jnp.bfloat16)] * GROUP,
        compiler_params=pltpu.CompilerParams(vmem_limit_bytes=24 * 2**20),
    )(*weights)


def place_kernel(count, *refs):
    for spot, piece in zip(spots_of_four(), refs[:GROUP]):
        for i in range(count):
            refs[GROUP + i][spot] = piece[i]


def placed(pieces):
    count, rows, share = pieces[0].shape
    return pl.pallas_call(
        functools.partial(place_kernel, count),
        name="place",
        out_shape=[jax.ShapeDtypeStruct((GROUP, rows, share), jnp.bfloat16)] * count,
        compiler_params=pltpu.CompilerParams(vmem_limit_bytes=24 * 2**20),
    )(*pieces)


class Collect:
    def __init__(self, part_ref, out_ref, slots, send_sem, recv_sem, own_sem):
        spot, *spots = spots_of_four()
        base = lax.axis_index("dp") - (spot << FIRST_BIT)
        self.out, self.slots = out_ref, slots
        self.copies = [
            send(
                part_ref.at[other],
                slots.at[spot],
                send_sem.at[m],
                recv_sem.at[m],
                {"dp": base + other * (1 << FIRST_BIT)},
            )
            for m, other in enumerate(spots)
        ]
        self.own = pltpu.make_async_copy(part_ref.at[spot], slots.at[spot], own_sem)
        self.own.start()

    def finish(self):
        self.own.wait()
        for copy in self.copies:
            copy.wait()
        rows, width = self.out.shape
        share, over = share_width(width), overlap_of(width)

        def strip(step, carry):
            at = pl.ds(pl.multiple_of(step * STRIP, STRIP), STRIP)
            for place in range(GROUP):
                skip = over * (place // (GROUP - 1))
                self.out[at, share * place : min(share * (place + 1), width)] = self.slots[
                    place, at, skip:share
                ].astype(jnp.float32)
            return carry

        lax.fori_loop(0, rows // STRIP, strip, 0)


def collect_scratch(rows, share):
    return [
        pltpu.VMEM((GROUP, rows, share), jnp.bfloat16),
        pltpu.SemaphoreType.DMA((GROUP - 1,)),
        pltpu.SemaphoreType.DMA((GROUP - 1,)),
        pltpu.SemaphoreType.DMA,
    ]


def exchanged(pieces):
    return [pieces[0]] + [flipped(pieces[m], "dp", m << FIRST_BIT) for m in range(1, GROUP)]


def final_kernel(
    n, bits, small_ref, gain1_ref, gain2_ref, all_ref, gains_ref, came, ssem, rsem, gs, gr
):
    place = lax.axis_index("dp")
    peers = [{"dp": (place + hop) % n} for hop in range(1, n)]
    greet(peers + [across("tensor", bit) for axis, bit in bits if axis == "tensor"])
    copies = [
        send(small_ref, all_ref.at[place], ssem.at[hop], rsem.at[hop], peers[hop])
        for hop in range(n - 1)
    ]
    all_ref[place] = small_ref[...]
    gains_ref[0:1] = gain1_ref[...]
    gains_ref[1:2] = gain2_ref[...]
    for step, (axis, bit) in enumerate(bits):
        copy = send(gains_ref, came.at[step], gs.at[step], gr.at[step], across(axis, bit))
        copy.wait()
        gains_ref[...] = gains_ref[...] + came[step]
    for copy in copies:
        copy.wait()


def final_pass(small, gain1, gain2):
    n = lax.axis_size("dp")
    bits = [
        (axis, bit)
        for axis in ("tensor", "dp")
        for bit in range(lax.axis_size(axis).bit_length() - 1)
    ]
    rows, width = small.shape
    vmem = pl.BlockSpec(memory_space=pltpu.VMEM)
    gains = (2, gain1.shape[1])
    return pl.pallas_call(
        functools.partial(final_kernel, n, bits),
        name="final",
        out_shape=(
            jax.ShapeDtypeStruct((n, rows, width), small.dtype),
            jax.ShapeDtypeStruct(gains, jnp.float32),
        ),
        in_specs=[vmem] * 3,
        out_specs=(vmem, vmem),
        scratch_shapes=[
            pltpu.VMEM((len(bits), *gains), jnp.float32),
            pltpu.SemaphoreType.DMA((n - 1,)),
            pltpu.SemaphoreType.DMA((n - 1,)),
            pltpu.SemaphoreType.DMA((len(bits),)),
            pltpu.SemaphoreType.DMA((len(bits),)),
        ],
        compiler_params=pltpu.CompilerParams(
            collective_id=8, has_side_effects=True, vmem_limit_bytes=24 * 2**20
        ),
    )(small, gain1, gain2)


GATHER_SEMS = [
    pltpu.SemaphoreType.DMA((len(ORDERS), 3)),
    pltpu.SemaphoreType.DMA((len(ORDERS), 3)),
    pltpu.SemaphoreType.DMA((3 * len(ORDERS) + 1,)),
    pltpu.SemaphoreType.DMA((3 * len(ORDERS) + 1,)),
    pltpu.SemaphoreType.DMA,
]


class SumTensor:
    def __init__(self, part_ref, q, core_buf, link_buf, sems_s, sems_r, own_sem):
        high, core = bit_of(*LINKS[2]), bit_of(*CORE)
        core_peer = across(*CORE)
        self.args = high, q, core_buf, link_buf, sems_s, sems_r
        self.own = pltpu.make_async_copy(part_ref.at[:, core], q, own_sem)
        self.own.start()
        self.copies = [
            send(
                part_ref.at[block, 1 - core],
                core_buf.at[block],
                sems_s.at[i],
                sems_r.at[i],
                core_peer,
            )
            for i, block in enumerate((1 - high, high))
        ]

    def pass_on(self):
        high, q, core_buf, link_buf, sems_s, sems_r = self.args
        self.own.wait()
        self.copies[0].wait_recv()
        q[1 - high] = q[1 - high] + core_buf[1 - high]
        self.copies.append(
            send(q.at[1 - high], link_buf, sems_s.at[2], sems_r.at[2], across(*LINKS[2]))
        )

    def arrive(self):
        self.copies[1].wait_recv()
        self.copies[2].wait_recv()

    def rows(self, rows):
        high, q, core_buf, link_buf, _, _ = self.args
        return (
            q[high, rows].astype(jnp.float32)
            + core_buf[high, rows].astype(jnp.float32)
            + link_buf[rows].astype(jnp.float32)
        )

    def finish(self):
        for copy in self.copies:
            copy.wait_send()


SUM_SEMS = [
    pltpu.SemaphoreType.DMA((3,)),
    pltpu.SemaphoreType.DMA((3,)),
    pltpu.SemaphoreType.DMA,
]


def middle_kernel(
    part_ref, tok_ref, cot_ref, gain_ref, resid_ref, all_ref, cot_all_ref,
    q, core_buf, link_buf, low, *sems
):
    greet([across(*link) for link in LINKS] + [across(*CORE)])
    total = SumTensor(part_ref, q, core_buf, link_buf, *sems[:3])
    total.pass_on()
    cots = Gather(cot_ref, cot_all_ref, *sems[8:])
    cots.step(0)
    total.arrive()

    def strip(i, carry):
        rows = pl.ds(pl.multiple_of(i * STRIP, STRIP), STRIP)
        resid = tok_ref[rows].astype(jnp.float32) + total.rows(rows)
        resid_ref[rows] = resid
        inv = lax.rsqrt(jnp.mean(resid * resid, axis=-1, keepdims=True) + epsilon)
        low[rows] = (resid * inv * gain_ref[...]).astype(low.dtype)
        return carry

    lax.fori_loop(0, tok_ref.shape[0] // STRIP, strip, 0)
    total.finish()
    blocks = Gather(low, all_ref, *sems[3:8])
    cots.step(1)
    blocks.step(0)
    blocks.step(1)
    cots.step(2)
    blocks.step(2)
    cots.finish()
    blocks.finish()


def middle(part, tok, cot, gain):
    rows, width = tok.shape
    vmem, anywhere = pl.BlockSpec(memory_space=pltpu.VMEM), pl.BlockSpec(memory_space=pl.ANY)
    return pl.pallas_call(
        middle_kernel,
        name="middle",
        out_shape=(
            jax.ShapeDtypeStruct((rows, width), jnp.float32),
            jax.ShapeDtypeStruct((2, 2, 2, 2, rows, width), jnp.bfloat16),
            jax.ShapeDtypeStruct((2, 2, 2, 2, rows, width), jnp.bfloat16),
        ),
        in_specs=[anywhere, vmem, vmem, vmem],
        out_specs=(vmem, anywhere, anywhere),
        scratch_shapes=[
            pltpu.VMEM((2, rows, width), jnp.bfloat16),
            pltpu.VMEM((2, rows, width), jnp.bfloat16),
            pltpu.VMEM((rows, width), jnp.bfloat16),
            pltpu.VMEM((rows, width), jnp.bfloat16),
            *SUM_SEMS,
            *GATHER_SEMS,
            *GATHER_SEMS,
        ],
        compiler_params=pltpu.CompilerParams(
            collective_id=1, has_side_effects=True, vmem_limit_bytes=32 * 2**20
        ),
    )(part.reshape(2, 2, rows, width), tok, cot, gain.reshape(1, width))


def norm_back(rows, back, base_ref, gain_ref, keep_ref, gain_acc):
    base = base_ref[rows].astype(jnp.float32)
    inv = lax.rsqrt(jnp.mean(base * base, axis=-1, keepdims=True) + epsilon)
    unit = base * inv
    scaled = gain_ref[...] * back
    grad = inv * (scaled - unit * jnp.mean(unit * scaled, axis=-1, keepdims=True))
    terms = back * unit
    gain_acc[...] += terms[:8] + terms[8:]
    return keep_ref[rows].astype(jnp.float32) + grad


def back_kernel(
    p_ref, resid_ref, cot_ref, gain_ref, grad_ref, all_ref, gain_out,
    q, cb, r0, r1, r2, low, gain_acc, ssem, rsem, fs, fr, own_sem, gs, gr, gather_own
):
    me = [bit_of(*link) for link in LINKS]
    core = bit_of(*CORE)
    peers = [across(*link) for link in LINKS]
    core_peer = across(*CORE)
    spans = column_spans(q.shape[-1])
    own = pltpu.make_async_copy(p_ref.at[:, :, :, core], q, own_sem)
    own.start()
    greet(peers + [core_peer])

    def half(k, near):
        first = SUM_ORDERS[k][0]
        return [(me[d] if near else 1 - me[d]) if d == first else slice(None) for d in range(3)]

    to_core = []
    for near in (False, True):
        for k in COLORS:
            i = half(k, near)
            to_core.append(
                send(
                    p_ref.at[i[0], i[1], i[2], 1 - core, :, pl.ds(*spans[k])],
                    cb.at[i[0], i[1], i[2], :, pl.ds(*spans[k])],
                    fs.at[len(to_core)],
                    fr.at[len(to_core)],
                    core_peer,
                )
            )
    own.wait()

    def add(i, k, other):
        s, n = spans[k]
        q[i[0], i[1], i[2], :, s : s + n] = q[i[0], i[1], i[2], :, s : s + n] + other

    moving, sent = [], []
    for near in (False, True):
        for k in COLORS:
            to_core[len(ORDERS) * near + k].wait_recv()
            i = half(k, near)
            s, n = spans[k]
            add(i, k, cb[i[0], i[1], i[2], :, s : s + n])
            if not near:
                moving.append(
                    send(
                        q.at[i[0], i[1], i[2], :, pl.ds(s, n)],
                        r0.at[:, :, :, pl.ds(s, n)],
                        ssem.at[k, 0],
                        rsem.at[k, 0],
                        peers[SUM_ORDERS[k][0]],
                    )
                )
    for step in (1, 2):
        for k in COLORS:
            s, n = spans[k]
            order = SUM_ORDERS[k]
            moving[k].wait_recv()
            sent.append(moving[k])
            kept = [me[d] if d in order[:step] else slice(None) for d in range(3)]
            add(kept, k, r0[:, :, :, s : s + n] if step == 1 else r1[:, :, s : s + n])
            away = [
                me[d] if d in order[:step] else (1 - me[d] if d == order[step] else slice(None))
                for d in range(3)
            ]
            moving[k] = send(
                q.at[away[0], away[1], away[2], :, pl.ds(s, n)],
                r1.at[:, :, pl.ds(s, n)] if step == 1 else r2.at[:, pl.ds(s, n)],
                ssem.at[k, step],
                rsem.at[k, step],
                peers[order[step]],
            )
    for k in COLORS:
        moving[k].wait_recv()
        sent.append(moving[k])
    gain_acc[...] = jnp.zeros_like(gain_acc)

    def strip(i, carry):
        rows = pl.ds(pl.multiple_of(i * STRIP, STRIP), STRIP)
        back = q[me[0], me[1], me[2], rows].astype(jnp.float32) + r2[rows].astype(jnp.float32)
        grad = norm_back(rows, back, resid_ref, gain_ref, cot_ref, gain_acc)
        grad_ref[rows] = grad
        low[rows] = grad.astype(low.dtype)
        return carry

    lax.fori_loop(0, low.shape[0] // STRIP, strip, 0)
    for copy in sent + to_core:
        copy.wait_send()
    gain_out[...] = jnp.sum(gain_acc[...], axis=0, keepdims=True)
    mine = all_ref.at[me[2], core]
    local = pltpu.make_async_copy(low, mine, gather_own)
    local.start()
    along = send(low, mine, gs.at[0], gr.at[0], peers[2])
    beside = send(low, mine, gs.at[1], gr.at[1], core_peer)
    along.wait_recv()
    theirs = all_ref.at[1 - me[2], core]
    onward = send(theirs, theirs, gs.at[2], gr.at[2], core_peer)
    local.wait()
    beside.wait()
    onward.wait()
    along.wait_send()


def back_pass(part, resid, cot, gain):
    rows, width = resid.shape
    wide = lambda *lead: pltpu.VMEM((*lead, rows, width), jnp.bfloat16)
    vmem = pl.BlockSpec(memory_space=pltpu.VMEM)
    return pl.pallas_call(
        back_kernel,
        name="back",
        out_shape=(
            jax.ShapeDtypeStruct((rows, width), jnp.float32),
            jax.ShapeDtypeStruct((2, 2, rows, width), jnp.bfloat16),
            jax.ShapeDtypeStruct((1, width), jnp.float32),
        ),
        in_specs=[pl.BlockSpec(memory_space=pl.ANY), vmem, vmem, vmem],
        out_specs=(vmem, pl.BlockSpec(memory_space=pl.ANY), vmem),
        scratch_shapes=[
            wide(2, 2, 2),
            wide(2, 2, 2),
            wide(2, 2),
            wide(2),
            wide(),
            wide(),
            pltpu.VMEM((8, width), jnp.float32),
            pltpu.SemaphoreType.DMA((len(ORDERS), 3)),
            pltpu.SemaphoreType.DMA((len(ORDERS), 3)),
            pltpu.SemaphoreType.DMA((2 * len(ORDERS),)),
            pltpu.SemaphoreType.DMA((2 * len(ORDERS),)),
            pltpu.SemaphoreType.DMA,
            pltpu.SemaphoreType.DMA((3,)),
            pltpu.SemaphoreType.DMA((3,)),
            pltpu.SemaphoreType.DMA,
        ],
        compiler_params=pltpu.CompilerParams(
            collective_id=2, has_side_effects=True, vmem_limit_bytes=40 * 2**20
        ),
    )(part.reshape(2, 2, 2, 2, rows, width), resid, cot, gain.reshape(1, width))


class Halve:
    def __init__(self, source, held, came, load_sem, send_sem, recv_sem, order, at_column=0):
        self.held, self.came, self.sems, self.order = held, came, (send_sem, recv_sem), order
        self.dims = sorted(order, reverse=True)
        self.sent, self.loads, at = [], [], 0
        lead = [slice(None) for _ in order]
        columns = pl.ds(at_column, held.shape[-1])
        for i, part in enumerate(source):
            rows = part.shape[-2]
            self.loads.append(
                pltpu.make_async_copy(
                    part.at[(*lead, slice(None), columns)],
                    held.at[(*lead, pl.ds(at, rows))],
                    load_sem.at[i],
                )
            )
            self.loads[-1].start()
            at += rows

    def index(self, done, away=None):
        picks = []
        for bit in self.dims:
            if bit in done:
                picks.append(bit_of("dp", bit))
            elif bit == away:
                picks.append(1 - bit_of("dp", bit))
            else:
                picks.append(slice(None))
        return tuple(picks)

    def start(self, step):
        if step == 0:
            for load in self.loads:
                load.wait()
        bit = self.order[step]
        self.moving = send(
            self.held.at[self.index(self.order[:step], bit)],
            self.came[step],
            self.sems[0].at[step],
            self.sems[1].at[step],
            across("dp", bit),
        )
        self.sent.append(self.moving)

    def land(self, step):
        self.moving.wait_recv()
        kept = self.index(self.order[: step + 1])
        self.held[kept] = self.held[kept] + self.came[step][...]
        if step + 1 < len(self.order):
            self.start(step + 1)

    def result(self):
        return self.held[self.index(self.order)]

    def finish(self):
        for copy in self.sent:
            copy.wait_send()


def halve_scratch(bits, rows, width):
    scratch = [pltpu.VMEM((*[2] * bits, rows, width), jnp.bfloat16)]
    for step in range(bits):
        scratch.append(pltpu.VMEM((*[2] * (bits - 1 - step), rows, width), jnp.bfloat16))
    return scratch + [
        pltpu.SemaphoreType.DMA((2,)),
        pltpu.SemaphoreType.DMA((bits,)),
        pltpu.SemaphoreType.DMA((bits,)),
    ]


def last_plan(bits, rows, few_rows, width):
    wide = width // 128 * 4 // 5 * 128
    swapped = [1, 0, *range(2, bits)]
    return [
        (list(range(bits)), 0, halve_scratch(bits, rows + few_rows, wide)),
        (swapped, wide, halve_scratch(bits, rows + few_rows, width - wide)),
        (list(range(1, bits)), 0, halve_scratch(bits - 1, rows, width)),
        ([0, *range(2, bits)], 0, halve_scratch(bits - 1, rows, width)),
    ]


def last_kernel(
    plan, part_ref, tok_ref, keep_ref, gain_ref, wide_ref, few_ref, y_ref, o_ref,
    row1_ref, row2_ref, row3_ref,
    grad_ref, gain_out, wide_out, few_out, y_out, o_out, row1_out, row2_out, row3_out,
    q, core_buf, link_buf, gain_acc, *refs
):
    sum_sems, refs = refs[:3], refs[3:]
    sources = ((wide_ref, few_ref), (wide_ref, few_ref), (y_ref,), (o_ref,))
    halvings = []
    for source, (order, column, scratch) in zip(sources, plan):
        mine, refs = refs[: len(scratch)], refs[len(scratch) :]
        came = mine[1 : 1 + len(order)]
        halvings.append(Halve(source, mine[0], came, *mine[1 + len(order) :], order, column))
    bits = len(plan[0][0])
    peers = [across("dp", bit) for bit in range(bits)]
    spot, *spots = spots_of_four()
    both = {"dp": lax.axis_index("dp") + (spots[2] - spot) * (1 << FIRST_BIT)}
    greet([across(*LINKS[2]), across(*CORE), both] + peers)
    total = SumTensor(part_ref, q, core_buf, link_buf, *sum_sems)
    for each in halvings:
        each.start(0)
    rows = zip((row1_ref, row2_ref, row3_ref), (row1_out, row2_out, row3_out))
    collects = [Collect(part, out, *refs[4 * i : 4 * i + 4]) for i, (part, out) in enumerate(rows)]
    total.pass_on()
    gain_acc[...] = jnp.zeros_like(gain_acc)

    def strip(i, carry):
        rows = pl.ds(pl.multiple_of(i * STRIP, STRIP), STRIP)
        back = total.rows(rows)
        grad_ref[rows] = norm_back(rows, back, tok_ref, gain_ref, keep_ref, gain_acc)
        return carry

    total.arrive()
    lax.fori_loop(0, tok_ref.shape[0] // STRIP, strip, 0)
    gain_out[...] = jnp.sum(gain_acc[...], axis=0, keepdims=True)
    for step in range(bits):
        for each in halvings:
            if step < len(each.order):
                each.land(step)
    rows = wide_out.shape[0]
    for each, (_, column, _) in zip(halvings[:2], plan):
        mine = each.result()
        columns = slice(column, column + mine.shape[1])
        wide_out[:, columns] = mine[:rows].astype(jnp.float32)
        few_out[:, columns] = mine[rows:]
    for each in collects:
        each.finish()
    y_out[...] = halvings[2].result().astype(jnp.float32)
    o_out[...] = halvings[3].result().astype(jnp.float32)
    for each in (*halvings, total):
        each.finish()


def last_pass(part, tok, keep, gain, wide, few, side_y, side_o, parts, hidden_width):
    rows, width = tok.shape
    vmem, anywhere = pl.BlockSpec(memory_space=pltpu.VMEM), pl.BlockSpec(memory_space=pl.ANY)
    bits = wide.shape[0].bit_length() - 1
    plan = last_plan(bits, wide.shape[1], few.shape[1], wide.shape[2])
    block = jax.ShapeDtypeStruct(wide.shape[1:], jnp.float32)
    leading = [2] * bits
    return pl.pallas_call(
        functools.partial(last_kernel, plan),
        name="last",
        out_shape=(
            jax.ShapeDtypeStruct((rows, width), jnp.float32),
            jax.ShapeDtypeStruct((1, width), jnp.float32),
            block,
            jax.ShapeDtypeStruct(few.shape[1:], jnp.bfloat16),
            block,
            block,
            *[jax.ShapeDtypeStruct((parts[0].shape[1], hidden_width), jnp.float32)] * 3,
        ),
        in_specs=[anywhere, vmem, vmem, vmem] + [anywhere] * 7,
        out_specs=(vmem,) * 9,
        scratch_shapes=[
            pltpu.VMEM((2, rows, width), jnp.bfloat16),
            pltpu.VMEM((2, rows, width), jnp.bfloat16),
            pltpu.VMEM((rows, width), jnp.bfloat16),
            pltpu.VMEM((8, width), jnp.float32),
            *SUM_SEMS,
            *[ref for _, _, scratch in plan for ref in scratch],
            *collect_scratch(*parts[0].shape[1:]) * 3,
        ],
        compiler_params=pltpu.CompilerParams(
            collective_id=3, has_side_effects=True, vmem_limit_bytes=48 * 2**20
        ),
    )(
        part.reshape(2, 2, rows, width),
        tok,
        keep,
        gain.reshape(1, width),
        wide.reshape(*leading, *wide.shape[1:]),
        few.reshape(*leading, *few.shape[1:]),
        side_y,
        side_o,
        *parts,
    )


def scan_kernel(n, reverse, *refs):
    a_ref, b_ref, out_ref, edge_ref, fa, fb, mine, others, ssem, rsem = refs
    place = lax.axis_index("dp")
    sign = -1 if reverse else 1
    barrier = pltpu.get_barrier_semaphore()
    peers = [{"dp": (place + sign * hop + n) % n} for hop in range(1, n)]
    for peer in peers:
        pl.semaphore_signal(barrier, inc=1, device_id=peer, device_id_type=MESH)
    rows, width = a_ref.shape
    length = rows // 8
    lanes = range(width // 128)
    for k in lanes:
        fa[k * rows : (k + 1) * rows] = a_ref[:, k * 128 : (k + 1) * 128]
        fb[k * rows : (k + 1) * rows] = b_ref[:, k * 128 : (k + 1) * 128]

    def at(k, r):
        return pl.ds(k * rows + (length - 1 - r if reverse else r), 8, stride=length)

    def local(r, carry):
        result = []
        for k in lanes:
            prod, state = carry[k]
            decay = fa[at(k, r), :]
            term = fb[at(k, r), :]
            if reverse:
                fa[at(k, r), :] = prod
                total = term + state
                fb[at(k, r), :] = total
                result.append((prod * decay, decay * total))
            else:
                prod = prod * decay
                state = decay * state + term
                fa[at(k, r), :] = prod
                fb[at(k, r), :] = state
                result.append((prod, state))
        return result

    start = [(jnp.ones((8, 128), jnp.float32), jnp.zeros((8, 128), jnp.float32)) for k in lanes]
    ends = lax.fori_loop(0, length, local, start, unroll=2)
    prod = jnp.concatenate([end[0] for end in ends], axis=1)
    state = jnp.concatenate([end[1] for end in ends], axis=1)
    order = range(7, -1, -1) if reverse else range(8)
    run_a, run_b = jnp.ones((1, width), jnp.float32), jnp.zeros((1, width), jnp.float32)
    before = [None] * 8
    for s in order:
        before[s] = (run_a, run_b)
        pa, pb = prod[s : s + 1], state[s : s + 1]
        run_a, run_b = pa * run_a, pa * run_b + pb
    mine[0:1] = run_a
    mine[1:2] = run_b
    pl.semaphore_wait(barrier, n - 1)
    copies = [
        send(mine, others.at[hop - 1], ssem.at[hop - 1], rsem.at[hop - 1], peers[hop - 1])
        for hop in range(1, n)
    ]
    carry = jnp.zeros((1, width), jnp.float32)
    ahead = n - 1 - place if reverse else place
    for copy in copies:
        copy.wait_recv()
    for hop in range(n - 1, 0, -1):
        step = others[hop - 1, 0:1] * carry + others[hop - 1, 1:2]
        carry = jnp.where(hop <= ahead, step, carry)
    edge_ref[...] = carry
    entering = jnp.concatenate([pa * carry + pb for pa, pb in before], axis=0)

    def fix(r, c):
        for k in lanes:
            fb[at(k, r), :] = fb[at(k, r), :] + fa[at(k, r), :] * entering[:, k * 128 : (k + 1) * 128]
        return c

    lax.fori_loop(0, length, fix, 0, unroll=2)
    for k in lanes:
        out_ref[:, k * 128 : (k + 1) * 128] = fb[k * rows : (k + 1) * rows]
    for copy in copies:
        copy.wait_send()


def scan_stream(decay, term, reverse):
    n = lax.axis_size("dp")
    rows, width = decay.shape
    vmem = pl.BlockSpec(memory_space=pltpu.VMEM)
    return pl.pallas_call(
        functools.partial(scan_kernel, n, reverse),
        name="scan_back" if reverse else "scan",
        out_shape=(
            jax.ShapeDtypeStruct((rows, width), jnp.float32),
            jax.ShapeDtypeStruct((1, width), jnp.float32),
        ),
        in_specs=[vmem, vmem],
        out_specs=(vmem, vmem),
        scratch_shapes=[
            pltpu.VMEM((rows * width // 128, 128), jnp.float32),
            pltpu.VMEM((rows * width // 128, 128), jnp.float32),
            pltpu.VMEM((2, width), jnp.float32),
            pltpu.VMEM((n - 1, 2, width), jnp.float32),
            pltpu.SemaphoreType.DMA((n - 1,)),
            pltpu.SemaphoreType.DMA((n - 1,)),
        ],
        compiler_params=pltpu.CompilerParams(
            collective_id=5 if reverse else 4, has_side_effects=True, vmem_limit_bytes=32 * 2**20
        ),
    )(decay, term)


def in_order(bit, mine, theirs, axis=0):
    return jnp.where(
        bit == 0, jnp.concatenate([mine, theirs], axis), jnp.concatenate([theirs, mine], axis)
    )


def parted(held, dims, bit):
    mine = (lax.axis_index("dp") >> bit) % 2
    axis = dims.index(bit)
    return (
        lax.dynamic_index_in_dim(held, mine, axis, False),
        lax.dynamic_index_in_dim(held, 1 - mine, axis, False),
    )


def added(keep, came):
    return (keep.astype(jnp.float32) + came.astype(jnp.float32)).astype(jnp.bfloat16)


def inner(
    tokens,
    doc_start,
    norm1_gain,
    proj_x,
    proj_y,
    conv_weight,
    conv_bias,
    gate_x_weight,
    gate_x_bias,
    gate_a_weight,
    gate_a_bias,
    decay_param,
    proj_out,
    norm2_gain,
    mlp_gate,
    mlp_up,
    mlp_down,
    cotangent,
):
    tok_rows = tokens.shape[0]
    chan_width = proj_x.shape[1]
    block_width = gate_x_weight.shape[0]
    half_width = block_width // 2
    tap_count = conv_weight.shape[0]
    parity = lax.axis_index("tensor") % 2
    full_start = parity * half_width
    shared_start = (1 - parity) * 2 * block_width
    tensor_size = lax.axis_size("tensor")
    share_rows = tok_rows // tensor_size
    own_start = lax.axis_index("tensor") * share_rows
    positions = lax.axis_index("dp") * tok_rows + lax.iota(jnp.int32, tok_rows)
    starting = (doc_start == positions)[:, None]
    dp_size = lax.axis_size("dp")
    low_size = 1 << FIRST_BIT
    high_size = dp_size // (GROUP * low_size)

    def dp_index(high, four, low):
        return (high * GROUP + four) * low_size + low

    highs, fours, lows = range(high_size), range(GROUP), range(low_size)
    groups = [
        [dp_index(h, i, l) * tensor_size + t for i in fours for t in range(tensor_size)]
        for h in highs
        for l in lows
    ]
    low_groups = [[dp_index(h, i, l) for l in lows] for h in highs for i in fours]
    high_groups = [[dp_index(h, i, l) for h in highs] for i in fours for l in lows]
    everyone = ("dp", "tensor")

    spot = lax.axis_index("dp") // low_size % GROUP
    hidden_width = mlp_gate.shape[1]
    share = share_width(hidden_width)

    def all_rows(part):
        rows = part.shape[1]
        if low_size > 1:
            part = lax.all_gather(
                part[:, None], "dp", axis=1, axis_index_groups=low_groups, tiled=True
            )
        if high_size > 1:
            part = lax.all_gather(part, "dp", axis=0, axis_index_groups=high_groups, tiled=True)
        return part.reshape(dp_size * rows, share)

    def own_rows(grad):
        rows = grad.shape[0] // dp_size
        grad = grad.astype(jnp.bfloat16).reshape(high_size * GROUP, low_size, rows, share)
        if high_size > 1:
            grad = lax.psum_scatter(
                grad, "dp", axis_index_groups=high_groups, scatter_dimension=0, tiled=True
            )
        if low_size > 1:
            grad = lax.psum_scatter(
                grad, "dp", axis_index_groups=low_groups, scatter_dimension=1, tiled=True
            )
        return grad.reshape(GROUP, rows, share)

    cot_own = lax.dynamic_slice_in_dim(cotangent, own_start, share_rows, 0)
    gate_pieces = exchanged(cut(mlp_gate))
    pieces = exchanged(cut(mlp_up, mlp_down))
    tok_own = lax.dynamic_slice_in_dim(tokens, own_start, share_rows, 0)

    def normalize(values):
        values = values.astype(jnp.float32)
        inv_rms = lax.rsqrt(jnp.mean(values * values, axis=-1, keepdims=True) + epsilon)
        return (values * inv_rms * norm1_gain).astype(jnp.bfloat16)

    halo = 16
    normed_low = normalize(tokens)
    normed_low, *gate_pieces = lax.optimization_barrier((normed_low, *gate_pieces))
    gate_cols = all_rows(*placed(gate_pieces))
    normed_prev = normalize(shifted(tokens[tok_rows - halo :], "dp", 1))
    branch_y = matmul(normed_low, proj_y)
    branch_x = matmul(normed_low, proj_x).astype(jnp.bfloat16)
    prev_x = matmul(normed_prev, proj_x).astype(jnp.bfloat16)
    extended = jnp.concatenate([prev_x[halo - tap_count + 1 :], branch_x], axis=0).astype(
        jnp.float32
    )

    def conv_apply(ext_rows, weight, bias_vec):
        conv_out = bias_vec + weight[0] * ext_rows[tap_count - 1 :]
        for offset in range(1, tap_count):
            inside = (positions - offset >= doc_start).astype(jnp.float32)[:, None]
            lagged = ext_rows[tap_count - 1 - offset : tap_count - 1 - offset + tok_rows]
            conv_out = conv_out + weight[offset] * lagged * inside
        return conv_out

    conv_out, conv_pull = jax.vjp(conv_apply, extended, conv_weight, conv_bias)
    mixed_low = conv_out.astype(jnp.bfloat16)
    own_half = lax.dynamic_slice_in_dim(mixed_low, shared_start, half_width, 1)
    other_half = flipped(own_half, "tensor", 1)
    shared_in = in_order(parity, own_half, other_half, 1)
    full_in = lax.dynamic_slice_in_dim(mixed_low, full_start, 2 * block_width, 1).reshape(
        tok_rows, 2, block_width
    )

    def place(full_part, shared_part):
        return in_order(parity, full_part, shared_part, 1)

    def full_weight(weight):
        return lax.dynamic_slice_in_dim(weight, full_start, 2 * block_width, 1).reshape(
            block_width, 2, block_width
        )

    def shared_weight(weight):
        return lax.dynamic_slice_in_dim(weight, shared_start, half_width, 1)

    def gate_pre(weight, bias_vec):
        full_out = jnp.einsum(
            "nhi,ihj->nhj", full_in, full_weight(weight), preferred_element_type=jnp.float32
        ).reshape(tok_rows, 2 * block_width)
        shared_out = matmul(shared_in, shared_weight(weight))
        return place(full_out, shared_out) + bias_vec

    def recurrence_in(conv_vals, pre_input, pre_recur, param_vec):
        log_decay = -8.0 * jax.nn.sigmoid(pre_recur) * jax.nn.softplus(param_vec)
        decay = jnp.where(starting, 0.0, jnp.exp(log_decay))
        multiplier = jnp.where(starting, 1.0, jnp.sqrt(-jnp.expm1(2.0 * log_decay)))
        return (decay, multiplier * jax.nn.sigmoid(pre_input) * conv_vals)

    pre_input = gate_pre(gate_x_weight, gate_x_bias)
    pre_recur = gate_pre(gate_a_weight, gate_a_bias)
    (decay, drive), recur_pull = jax.vjp(
        recurrence_in, mixed_low.astype(jnp.float32), pre_input, pre_recur, decay_param
    )
    decay, drive, *pieces = lax.optimization_barrier((decay, drive, *pieces))
    up_cols, down_cols = (all_rows(part) for part in placed(pieces))
    states, entering = scan_stream(decay, drive, False)
    previous = jnp.concatenate([entering, states[:-1]], axis=0)
    gelu_y, gelu_pull = jax.vjp(gelu_tanh, branch_y)
    product_low = (states * gelu_y).astype(jnp.bfloat16)
    lru_part = matmul(product_low, proj_out).astype(jnp.bfloat16)
    resid, normed2_all, cot_all = middle(lru_part, tok_own, cot_own, norm2_gain)
    cot_all = cot_all.reshape(GROUP * tok_rows, -1)
    normed2_all = normed2_all.reshape(GROUP * tok_rows, -1)
    counted = lax.iota(jnp.int32, share) >= overlap_of(hidden_width) * (spot // (GROUP - 1))

    def once(values):
        return jnp.where(counted, values, 0.0).astype(jnp.bfloat16)

    gate_act = matmul(normed2_all, gate_cols)
    up_act = matmul(normed2_all, up_cols)
    hidden, act_pull = jax.vjp(gated_product, gate_act, up_act)
    hidden_low = once(hidden)
    grad_hidden = matmul(cot_all, down_cols)
    grad_gate, grad_up = act_pull(grad_hidden)
    grad_gate_low = once(grad_gate)
    grad_up_low = once(grad_up)

    out_part = contract_last(hidden_low, down_cols).astype(jnp.bfloat16)
    out_part, hidden_low, grad_gate_low, grad_up_low = lax.optimization_barrier(
        (out_part, hidden_low, grad_gate_low, grad_up_low)
    )
    back_part = (
        contract_last(grad_gate_low, gate_cols) + contract_last(grad_up_low, up_cols)
    ).astype(jnp.bfloat16)
    down_grad = contract_first(cot_all, hidden_low).astype(jnp.bfloat16)
    back_part, down_grad = lax.optimization_barrier((back_part, down_grad))
    down_rows = own_rows(down_grad)
    grad_resid, grad_lru_low, grad_gain2 = back_pass(back_part, resid, cot_own, norm2_gain)
    grad_lru_low = grad_lru_low.reshape(tok_rows, -1)
    gate_rows = own_rows(contract_first(normed2_all, grad_gate_low))
    up_rows = own_rows(contract_first(normed2_all, grad_up_low))
    block_out = resid + lax.psum_scatter(
        out_part,
        everyone,
        axis_index_groups=groups,
        scatter_dimension=0,
        tiled=True,
    ).astype(jnp.float32)

    grad_product = contract_last(grad_lru_low, proj_out)
    grad_states = grad_product * gelu_y
    grad_y_low = gelu_pull(grad_product * states)[0].astype(jnp.bfloat16)
    total_grad, _ = scan_stream(decay, grad_states, True)
    total_grad, late_y, late_lru = lax.optimization_barrier(
        (total_grad, grad_y_low, grad_lru_low)
    )

    def token_sum(left_rows, right_rows):
        return contract_first(left_rows, right_rows).astype(jnp.bfloat16)

    def per_device(rows):
        return rows.reshape(dp_size, rows.shape[0] // dp_size, rows.shape[1])

    dims = list(range(dp_size.bit_length() - 1))[::-1]

    def by_bits(grad):
        return grad.reshape(*[2] * len(dims), grad.shape[0] // dp_size, grad.shape[1])

    keep_y, away_y = parted(by_bits(token_sum(normed_low, late_y)), dims, 0)
    keep_o, away_o = parted(by_bits(token_sum(late_lru, product_low)), dims, 1)
    total_grad, away_y, away_o = lax.optimization_barrier((total_grad, away_y, away_o))
    came_y, came_o = flipped(away_y, "dp", 1), flipped(away_o, "dp", 2)
    back_y = contract_last(late_y, proj_y)
    conv_direct, grad_pre_input, grad_pre_recur, grad_param = recur_pull(
        (total_grad * previous, total_grad)
    )

    def gate_back(weight, grad_pre):
        grad_pre_low = grad_pre.astype(jnp.bfloat16)
        grad_full = lax.dynamic_slice_in_dim(grad_pre_low, full_start, 2 * block_width, 1).reshape(
            tok_rows, 2, block_width
        )
        grad_share = lax.dynamic_slice_in_dim(grad_pre_low, shared_start, half_width, 1)
        into_full = jnp.einsum(
            "nhj,ihj->nhi", grad_full, full_weight(weight), preferred_element_type=jnp.float32
        ).reshape(tok_rows, 2 * block_width)
        into_share = contract_last(grad_share, shared_weight(weight))
        weight_full = jnp.einsum(
            "nhi,nhj->ihj", full_in, grad_full, preferred_element_type=jnp.float32
        ).reshape(block_width, 2 * block_width)
        weight_share = contract_first(shared_in, grad_share)
        return (into_full, into_share, place(weight_full, weight_share))

    input_full, input_share, grad_gx_weight = gate_back(gate_x_weight, grad_pre_input)
    recur_full, recur_share, grad_ga_weight = gate_back(gate_a_weight, grad_pre_recur)
    full_sum = input_full + recur_full
    share_sum = input_share + recur_share
    own_grad = jnp.where(parity == 0, share_sum[:, :half_width], share_sum[:, half_width:])
    other_grad = jnp.where(parity == 0, share_sum[:, half_width:], share_sum[:, :half_width])
    returned = flipped(other_grad.astype(jnp.bfloat16), "tensor", 1).astype(other_grad.dtype)
    grad_conv = conv_direct + place(full_sum, own_grad + returned)
    grad_extended, grad_conv_weight, grad_conv_bias = conv_pull(grad_conv)
    rim_rows, came_y, came_o = lax.optimization_barrier(
        (grad_extended[: tap_count - 1], came_y, came_o)
    )
    side_y, side_o = added(keep_y, came_y), added(keep_o, came_o)
    rim_grad = shifted(rim_rows, "dp", -1)
    grad_branch_x = grad_extended[tap_count - 1 :] + jnp.concatenate(
        [jnp.zeros((tok_rows - tap_count + 1, chan_width), jnp.float32), rim_grad], axis=0
    )
    grad_x_low = grad_branch_x.astype(jnp.bfloat16)
    wide = jnp.concatenate([grad_gx_weight, grad_ga_weight], axis=0)
    sums = jnp.concatenate(
        [
            grad_conv_weight,
            grad_conv_bias[None],
            jnp.sum(grad_pre_input, axis=0)[None],
            jnp.sum(grad_pre_recur, axis=0)[None],
            grad_param[None],
        ],
        axis=0,
    )
    spare = dp_size * 16 - sums.shape[0]
    sums = jnp.concatenate([sums, jnp.zeros((spare, chan_width), jnp.float32)], axis=0)
    few = jnp.concatenate(
        [per_device(wide.astype(jnp.bfloat16)), per_device(sums.astype(jnp.bfloat16))], axis=1
    )
    grad_tokens, grad_gain1, grad_proj_x, reduced, grad_proj_y, grad_out, *grad_rows = last_pass(
        (contract_last(grad_x_low, proj_x) + back_y).astype(jnp.bfloat16),
        tok_own,
        grad_resid,
        norm1_gain,
        per_device(token_sum(normed_low, grad_x_low)),
        few,
        side_y,
        side_o,
        (down_rows, gate_rows, up_rows),
        hidden_width,
    )
    grad_mlp_down, grad_mlp_gate, grad_mlp_up = grad_rows
    grad_proj_out = grad_out.T
    shared, gains = final_pass(reduced, grad_gain1, grad_gain2)
    wide_rows = 2 * block_width // dp_size
    wide = shared[:, :wide_rows].reshape(2 * block_width, chan_width).astype(jnp.float32)
    small = shared[:, wide_rows:].reshape(dp_size * 16, chan_width).astype(jnp.float32)
    return (
        block_out,
        grad_tokens,
        gains[0],
        grad_proj_x,
        grad_proj_y,
        small[:tap_count],
        small[tap_count],
        wide[:block_width],
        small[tap_count + 1],
        wide[block_width:],
        small[tap_count + 2],
        small[tap_count + 3],
        grad_proj_out,
        gains[1],
        grad_mlp_gate,
        grad_mlp_up,
        grad_mlp_down,
    )


def solution(mesh):
    placed = (
        P("dp", None),
        P("dp"),
        P(),
        P(None, "tensor"),
        P(None, "tensor"),
        P(None, "tensor"),
        P("tensor"),
        P(None, "tensor"),
        P("tensor"),
        P(None, "tensor"),
        P("tensor"),
        P("tensor"),
        P("tensor", None),
        P(),
        P("dp", "tensor"),
        P("dp", "tensor"),
        P("dp", "tensor"),
        P("dp", None),
    )
    return jax.shard_map(
        inner,
        mesh=mesh,
        in_specs=placed,
        out_specs=(
            P(("dp", "tensor"), None),
            P(("dp", "tensor"), None),
            P(),
            P("dp", "tensor"),
            P("dp", "tensor"),
            P(None, "tensor"),
            P("tensor"),
            P(None, "tensor"),
            P("tensor"),
            P(None, "tensor"),
            P("tensor"),
            P("tensor"),
            P("tensor", "dp"),
            P(),
            P("dp", "tensor"),
            P("dp", "tensor"),
            P("dp", "tensor"),
        ),
        check_vma=False,
    )
```

```python
import functools

import jax
import jax.numpy as jnp
from jax import lax
from jax.experimental import pallas as pl
from jax.experimental.pallas import tpu as pltpu
from jax.sharding import PartitionSpec as P


epsilon = 1e-06
MESH = pl.DeviceIdType.MESH
GROUP = 4
STRIP = 16
FIRST_BIT = 0
LINKS = (("dp", FIRST_BIT + 1), ("dp", FIRST_BIT), ("tensor", 1))
CORE = ("tensor", 0)
ORDERS = ((0, 1, 2), (0, 2, 1), (1, 2, 0), (2, 0, 1))
TILES = (8, 3, 5)
SUM_ORDERS = tuple(order[::-1] for order in ORDERS)
COLORS = range(len(ORDERS))


def gelu_tanh(values):
    return jax.nn.gelu(values, approximate=True)


def gated_product(gate_vals, up_vals):
    return gelu_tanh(gate_vals) * up_vals


def contract_last(left_rows, right_rows):
    return lax.dot_general(
        left_rows, right_rows, (((1,), (1,)), ((), ())), preferred_element_type=jnp.float32
    )


def contract_first(left_rows, right_rows):
    return lax.dot_general(
        left_rows, right_rows, (((0,), (0,)), ((), ())), preferred_element_type=jnp.float32
    )


def matmul(left_rows, right_rows):
    return jnp.dot(left_rows, right_rows, preferred_element_type=jnp.float32)


def shifted(block, axis, distance):
    devices = range(lax.axis_size(axis))
    route = [(i - distance, i) for i in devices if i - distance in devices]
    return lax.ppermute(block, axis, route)


def flipped(array, axis, mask):
    return lax.ppermute(array, axis, [(i, i ^ mask) for i in range(lax.axis_size(axis))])


def bit_of(axis, bit):
    return (lax.axis_index(axis) // (1 << bit)) % 2


def across(axis, bit):
    index = lax.axis_index(axis)
    return {axis: index + (1 - 2 * ((index // (1 << bit)) % 2)) * (1 << bit)}


def column_spans(width):
    tiles = width // 128
    counts = [tiles * part // 20 for part in TILES]
    spans, start = [], 0
    for count in (*counts, tiles - sum(counts)):
        spans.append((start * 128, count * 128))
        start += count
    return spans


def send(src, dst, send_sem, recv_sem, device):
    copy = pltpu.make_async_remote_copy(
        src_ref=src,
        dst_ref=dst,
        send_sem=send_sem,
        recv_sem=recv_sem,
        device_id=device,
        device_id_type=MESH,
    )
    copy.start()
    return copy


def greet(devices):
    barrier = pltpu.get_barrier_semaphore()
    for device in devices:
        pl.semaphore_signal(barrier, inc=1, device_id=device, device_id_type=MESH)
    pl.semaphore_wait(barrier, len(devices))


class Gather:
    def __init__(self, x_ref, out_ref, send_sem, recv_sem, core_send, core_recv, own_sem):
        self.sems = send_sem, recv_sem, core_send, core_recv
        self.out = out_ref
        self.me = [bit_of(*link) for link in LINKS]
        self.core = bit_of(*CORE)
        self.peers = [across(*link) for link in LINKS]
        self.core_peer = across(*CORE)
        self.spans = column_spans(x_ref.shape[1])
        me, place = self.me, out_ref.at[self.me[0], self.me[1], self.me[2], self.core]
        self.own = pltpu.make_async_copy(x_ref, place, own_sem)
        self.own.start()
        self.moving = [
            send(
                x_ref.at[:, pl.ds(*self.spans[k])],
                self.region(me, k),
                send_sem.at[k, 0],
                recv_sem.at[k, 0],
                self.peers[ORDERS[k][0]],
            )
            for k in COLORS
        ]
        self.to_core = [send(x_ref, place, core_send.at[3 * len(ORDERS)], core_recv.at[3 * len(ORDERS)], self.core_peer)]
        self.sent = []

    def region(self, idx, k):
        return self.out.at[idx[0], idx[1], idx[2], self.core, :, pl.ds(*self.spans[k])]

    def step(self, step):
        send_sem, recv_sem, core_send, core_recv = self.sems
        me = self.me
        if step == 0:
            self.own.wait()
        for k in COLORS:
            order = ORDERS[k]
            self.moving[k].wait_recv()
            self.sent.append(self.moving[k])
            if step < 2:
                held = [slice(None) if d in order[: step + 1] else me[d] for d in range(3)]
                self.moving[k] = send(
                    self.region(held, k),
                    self.region(held, k),
                    send_sem.at[k, step + 1],
                    recv_sem.at[k, step + 1],
                    self.peers[order[step + 1]],
                )
            fresh = [
                slice(None) if d in order[:step] else (1 - me[d] if d == order[step] else me[d])
                for d in range(3)
            ]
            self.to_core.append(
                send(
                    self.region(fresh, k),
                    self.region(fresh, k),
                    core_send.at[len(ORDERS) * step + k],
                    core_recv.at[len(ORDERS) * step + k],
                    self.core_peer,
                )
            )

    def finish(self):
        for copy in self.sent:
            copy.wait_send()
        for copy in self.to_core:
            copy.wait()


def spots_of_four():
    spot = lax.axis_index("dp") // (1 << FIRST_BIT) % GROUP
    return spot, spot + 1 - 2 * (spot % 2), spot + 2 - 4 * (spot // 2), GROUP - 1 - spot


def share_width(width):
    return -(-width // (128 * GROUP)) * 128


def overlap_of(width):
    return GROUP * share_width(width) - width


def cut_kernel(count, *refs):
    width = refs[0].shape[1]
    share, over = share_width(width), overlap_of(width)
    for spot, out in zip(spots_of_four(), refs[count:]):
        start = share * spot - over * (spot // (GROUP - 1))
        for i in range(count):
            out[i] = refs[i][:, pl.ds(pl.multiple_of(start, 128), share)]


def cut(*weights):
    rows, share = weights[0].shape[0], share_width(weights[0].shape[1])
    return pl.pallas_call(
        functools.partial(cut_kernel, len(weights)),
        name="cut",
        out_shape=[jax.ShapeDtypeStruct((len(weights), rows, share), jnp.bfloat16)] * GROUP,
        compiler_params=pltpu.CompilerParams(vmem_limit_bytes=24 * 2**20),
    )(*weights)


def place_kernel(count, *refs):
    for spot, piece in zip(spots_of_four(), refs[:GROUP]):
        for i in range(count):
            refs[GROUP + i][spot] = piece[i]


def placed(pieces):
    count, rows, share = pieces[0].shape
    return pl.pallas_call(
        functools.partial(place_kernel, count),
        name="place",
        out_shape=[jax.ShapeDtypeStruct((GROUP, rows, share), jnp.bfloat16)] * count,
        compiler_params=pltpu.CompilerParams(vmem_limit_bytes=24 * 2**20),
    )(*pieces)


def pick_kernel(count, *refs):
    for spot, out in zip(spots_of_four(), refs[count:]):
        for i in range(count):
            out[i] = refs[i][spot]


def picked(*parts):
    _, rows, share = parts[0].shape
    return pl.pallas_call(
        functools.partial(pick_kernel, len(parts)),
        name="pick",
        out_shape=[jax.ShapeDtypeStruct((len(parts), rows, share), jnp.bfloat16)] * GROUP,
        compiler_params=pltpu.CompilerParams(vmem_limit_bytes=24 * 2**20),
    )(*parts)


def join_kernel(count, *refs):
    pieces, outs, slots = refs[:GROUP], refs[GROUP : GROUP + count], refs[GROUP + count]
    for spot, piece in zip(spots_of_four(), pieces):
        for i in range(count):
            slots[i, spot] = piece[i]
    rows, width = outs[0].shape
    share, over = share_width(width), overlap_of(width)

    def strip(step, carry):
        at = pl.ds(pl.multiple_of(step * STRIP, STRIP), STRIP)
        for i in range(count):
            for place in range(GROUP):
                skip = over * (place // (GROUP - 1))
                outs[i][at, share * place : min(share * (place + 1), width)] = slots[
                    i, place, at, skip:share
                ].astype(jnp.float32)
        return carry

    lax.fori_loop(0, rows // STRIP, strip, 0)


def joined(pieces, width):
    count, rows, share = pieces[0].shape
    return pl.pallas_call(
        functools.partial(join_kernel, count),
        name="join",
        out_shape=[jax.ShapeDtypeStruct((rows, width), jnp.float32)] * count,
        scratch_shapes=[pltpu.VMEM((count, GROUP, rows, share), jnp.bfloat16)],
        compiler_params=pltpu.CompilerParams(vmem_limit_bytes=32 * 2**20),
    )(*pieces)


class Collect:
    def __init__(self, part_ref, out_ref, slots, send_sem, recv_sem, own_sem):
        spot, *spots = spots_of_four()
        base = lax.axis_index("dp") - (spot << FIRST_BIT)
        self.out, self.slots = out_ref, slots
        self.copies = [
            send(
                part_ref.at[other],
                slots.at[spot],
                send_sem.at[m],
                recv_sem.at[m],
                {"dp": base + other * (1 << FIRST_BIT)},
            )
            for m, other in enumerate(spots)
        ]
        self.own = pltpu.make_async_copy(part_ref.at[spot], slots.at[spot], own_sem)
        self.own.start()

    def finish(self):
        self.own.wait()
        for copy in self.copies:
            copy.wait()
        rows, width = self.out.shape
        share, over = share_width(width), overlap_of(width)

        def strip(step, carry):
            at = pl.ds(pl.multiple_of(step * STRIP, STRIP), STRIP)
            for place in range(GROUP):
                skip = over * (place // (GROUP - 1))
                self.out[at, share * place : min(share * (place + 1), width)] = self.slots[
                    place, at, skip:share
                ].astype(jnp.float32)
            return carry

        lax.fori_loop(0, rows // STRIP, strip, 0)


def collect_scratch(rows, share):
    return [
        pltpu.VMEM((GROUP, rows, share), jnp.bfloat16),
        pltpu.SemaphoreType.DMA((GROUP - 1,)),
        pltpu.SemaphoreType.DMA((GROUP - 1,)),
        pltpu.SemaphoreType.DMA,
    ]


def exchanged(pieces):
    return [pieces[0]] + [flipped(pieces[m], "dp", m << FIRST_BIT) for m in range(1, GROUP)]


def final_kernel(
    n, bits, small_ref, gain1_ref, gain2_ref, all_ref, gains_ref, came, ssem, rsem, gs, gr
):
    place = lax.axis_index("dp")
    peers = [{"dp": (place + hop) % n} for hop in range(1, n)]
    greet(peers + [across("tensor", bit) for axis, bit in bits if axis == "tensor"])
    copies = [
        send(small_ref, all_ref.at[place], ssem.at[hop], rsem.at[hop], peers[hop])
        for hop in range(n - 1)
    ]
    all_ref[place] = small_ref[...]
    gains_ref[0:1] = gain1_ref[...]
    gains_ref[1:2] = gain2_ref[...]
    for step, (axis, bit) in enumerate(bits):
        copy = send(gains_ref, came.at[step], gs.at[step], gr.at[step], across(axis, bit))
        copy.wait()
        gains_ref[...] = gains_ref[...] + came[step]
    for copy in copies:
        copy.wait()


def final_pass(small, gain1, gain2):
    n = lax.axis_size("dp")
    bits = [
        (axis, bit)
        for axis in ("tensor", "dp")
        for bit in range(lax.axis_size(axis).bit_length() - 1)
    ]
    rows, width = small.shape
    vmem = pl.BlockSpec(memory_space=pltpu.VMEM)
    gains = (2, gain1.shape[1])
    return pl.pallas_call(
        functools.partial(final_kernel, n, bits),
        name="final",
        out_shape=(
            jax.ShapeDtypeStruct((n, rows, width), small.dtype),
            jax.ShapeDtypeStruct(gains, jnp.float32),
        ),
        in_specs=[vmem] * 3,
        out_specs=(vmem, vmem),
        scratch_shapes=[
            pltpu.VMEM((len(bits), *gains), jnp.float32),
            pltpu.SemaphoreType.DMA((n - 1,)),
            pltpu.SemaphoreType.DMA((n - 1,)),
            pltpu.SemaphoreType.DMA((len(bits),)),
            pltpu.SemaphoreType.DMA((len(bits),)),
        ],
        compiler_params=pltpu.CompilerParams(
            collective_id=8, has_side_effects=True, vmem_limit_bytes=24 * 2**20
        ),
    )(small, gain1, gain2)


GATHER_SEMS = [
    pltpu.SemaphoreType.DMA((len(ORDERS), 3)),
    pltpu.SemaphoreType.DMA((len(ORDERS), 3)),
    pltpu.SemaphoreType.DMA((3 * len(ORDERS) + 1,)),
    pltpu.SemaphoreType.DMA((3 * len(ORDERS) + 1,)),
    pltpu.SemaphoreType.DMA,
]


class SumTensor:
    def __init__(self, part_ref, q, core_buf, link_buf, sems_s, sems_r, own_sem):
        high, core = bit_of(*LINKS[2]), bit_of(*CORE)
        core_peer = across(*CORE)
        self.args = high, q, core_buf, link_buf, sems_s, sems_r
        self.own = pltpu.make_async_copy(part_ref.at[:, core], q, own_sem)
        self.own.start()
        self.copies = [
            send(
                part_ref.at[block, 1 - core],
                core_buf.at[block],
                sems_s.at[i],
                sems_r.at[i],
                core_peer,
            )
            for i, block in enumerate((1 - high, high))
        ]

    def pass_on(self):
        high, q, core_buf, link_buf, sems_s, sems_r = self.args
        self.own.wait()
        self.copies[0].wait_recv()
        q[1 - high] = q[1 - high] + core_buf[1 - high]
        self.copies.append(
            send(q.at[1 - high], link_buf, sems_s.at[2], sems_r.at[2], across(*LINKS[2]))
        )

    def arrive(self):
        self.copies[1].wait_recv()
        self.copies[2].wait_recv()

    def rows(self, rows):
        high, q, core_buf, link_buf, _, _ = self.args
        return (
            q[high, rows].astype(jnp.float32)
            + core_buf[high, rows].astype(jnp.float32)
            + link_buf[rows].astype(jnp.float32)
        )

    def finish(self):
        for copy in self.copies:
            copy.wait_send()


SUM_SEMS = [
    pltpu.SemaphoreType.DMA((3,)),
    pltpu.SemaphoreType.DMA((3,)),
    pltpu.SemaphoreType.DMA,
]


def middle_kernel(
    part_ref, tok_ref, cot_ref, gain_ref, resid_ref, all_ref, cot_all_ref,
    q, core_buf, link_buf, low, *sems
):
    greet([across(*link) for link in LINKS] + [across(*CORE)])
    total = SumTensor(part_ref, q, core_buf, link_buf, *sems[:3])
    total.pass_on()
    cots = Gather(cot_ref, cot_all_ref, *sems[8:])
    cots.step(0)
    total.arrive()

    def strip(i, carry):
        rows = pl.ds(pl.multiple_of(i * STRIP, STRIP), STRIP)
        resid = tok_ref[rows].astype(jnp.float32) + total.rows(rows)
        resid_ref[rows] = resid
        inv = lax.rsqrt(jnp.mean(resid * resid, axis=-1, keepdims=True) + epsilon)
        low[rows] = (resid * inv * gain_ref[...]).astype(low.dtype)
        return carry

    lax.fori_loop(0, tok_ref.shape[0] // STRIP, strip, 0)
    total.finish()
    blocks = Gather(low, all_ref, *sems[3:8])
    cots.step(1)
    blocks.step(0)
    blocks.step(1)
    cots.step(2)
    blocks.step(2)
    cots.finish()
    blocks.finish()


def middle(part, tok, cot, gain):
    rows, width = tok.shape
    vmem, anywhere = pl.BlockSpec(memory_space=pltpu.VMEM), pl.BlockSpec(memory_space=pl.ANY)
    return pl.pallas_call(
        middle_kernel,
        name="middle",
        out_shape=(
            jax.ShapeDtypeStruct((rows, width), jnp.float32),
            jax.ShapeDtypeStruct((2, 2, 2, 2, rows, width), jnp.bfloat16),
            jax.ShapeDtypeStruct((2, 2, 2, 2, rows, width), jnp.bfloat16),
        ),
        in_specs=[anywhere, vmem, vmem, vmem],
        out_specs=(vmem, anywhere, anywhere),
        scratch_shapes=[
            pltpu.VMEM((2, rows, width), jnp.bfloat16),
            pltpu.VMEM((2, rows, width), jnp.bfloat16),
            pltpu.VMEM((rows, width), jnp.bfloat16),
            pltpu.VMEM((rows, width), jnp.bfloat16),
            *SUM_SEMS,
            *GATHER_SEMS,
            *GATHER_SEMS,
        ],
        compiler_params=pltpu.CompilerParams(
            collective_id=1, has_side_effects=True, vmem_limit_bytes=32 * 2**20
        ),
    )(part.reshape(2, 2, rows, width), tok, cot, gain.reshape(1, width))


def product_pair_kernel(left1_ref, left2_ref, right1_ref, right2_ref, out_ref):
    tile = 512
    for at in range(0, out_ref.shape[1], tile):
        part = slice(at, at + tile)
        total = contract_last(left1_ref[...], right1_ref[part])
        total += contract_last(left2_ref[...], right2_ref[part])
        out_ref[:, part] = total.astype(out_ref.dtype)


def product_pair(left1, left2, right1, right2):
    rows, depth = left1.shape
    width = right1.shape[0]
    block = 256
    left = pl.BlockSpec((block, depth), lambda i: (i, 0))
    right = pl.BlockSpec((width, depth), lambda i: (0, 0))
    return pl.pallas_call(
        product_pair_kernel,
        name="product_pair",
        grid=(rows // block,),
        out_shape=jax.ShapeDtypeStruct((rows, width), jnp.bfloat16),
        in_specs=[left, left, right, right],
        out_specs=pl.BlockSpec((block, width), lambda i: (i, 0)),
        cost_estimate=pl.CostEstimate(
            flops=4 * rows * depth * width,
            bytes_accessed=2 * (2 * rows * depth + 2 * width * depth + rows * width),
            transcendentals=0,
        ),
        compiler_params=pltpu.CompilerParams(vmem_limit_bytes=32 * 2**20),
    )(left1, left2, right1, right2)


def norm_back(rows, back, base_ref, gain_ref, keep_ref, gain_acc):
    base = base_ref[rows].astype(jnp.float32)
    inv = lax.rsqrt(jnp.mean(base * base, axis=-1, keepdims=True) + epsilon)
    unit = base * inv
    scaled = gain_ref[...] * back
    grad = inv * (scaled - unit * jnp.mean(unit * scaled, axis=-1, keepdims=True))
    terms = back * unit
    gain_acc[...] += terms[:8] + terms[8:]
    return keep_ref[rows].astype(jnp.float32) + grad


def back_kernel(
    p_ref, resid_ref, cot_ref, gain_ref, grad_ref, all_ref, gain_out,
    q, cb, r0, r1, r2, low, gain_acc, ssem, rsem, fs, fr, own_sem, gs, gr, gather_own
):
    me = [bit_of(*link) for link in LINKS]
    core = bit_of(*CORE)
    peers = [across(*link) for link in LINKS]
    core_peer = across(*CORE)
    spans = column_spans(q.shape[-1])
    own = pltpu.make_async_copy(p_ref.at[:, :, :, core], q, own_sem)
    own.start()
    greet(peers + [core_peer])

    def half(k, near):
        first = SUM_ORDERS[k][0]
        return [(me[d] if near else 1 - me[d]) if d == first else slice(None) for d in range(3)]

    to_core = []
    for near in (False, True):
        for k in COLORS:
            i = half(k, near)
            to_core.append(
                send(
                    p_ref.at[i[0], i[1], i[2], 1 - core, :, pl.ds(*spans[k])],
                    cb.at[i[0], i[1], i[2], :, pl.ds(*spans[k])],
                    fs.at[len(to_core)],
                    fr.at[len(to_core)],
                    core_peer,
                )
            )
    own.wait()

    def add(i, k, other):
        s, n = spans[k]
        q[i[0], i[1], i[2], :, s : s + n] = q[i[0], i[1], i[2], :, s : s + n] + other

    moving, sent = [], []
    for near in (False, True):
        for k in COLORS:
            to_core[len(ORDERS) * near + k].wait_recv()
            i = half(k, near)
            s, n = spans[k]
            add(i, k, cb[i[0], i[1], i[2], :, s : s + n])
            if not near:
                moving.append(
                    send(
                        q.at[i[0], i[1], i[2], :, pl.ds(s, n)],
                        r0.at[:, :, :, pl.ds(s, n)],
                        ssem.at[k, 0],
                        rsem.at[k, 0],
                        peers[SUM_ORDERS[k][0]],
                    )
                )
    for step in (1, 2):
        for k in COLORS:
            s, n = spans[k]
            order = SUM_ORDERS[k]
            moving[k].wait_recv()
            sent.append(moving[k])
            kept = [me[d] if d in order[:step] else slice(None) for d in range(3)]
            add(kept, k, r0[:, :, :, s : s + n] if step == 1 else r1[:, :, s : s + n])
            away = [
                me[d] if d in order[:step] else (1 - me[d] if d == order[step] else slice(None))
                for d in range(3)
            ]
            moving[k] = send(
                q.at[away[0], away[1], away[2], :, pl.ds(s, n)],
                r1.at[:, :, pl.ds(s, n)] if step == 1 else r2.at[:, pl.ds(s, n)],
                ssem.at[k, step],
                rsem.at[k, step],
                peers[order[step]],
            )
    for k in COLORS:
        moving[k].wait_recv()
        sent.append(moving[k])
    gain_acc[...] = jnp.zeros_like(gain_acc)

    def strip(i, carry):
        rows = pl.ds(pl.multiple_of(i * STRIP, STRIP), STRIP)
        back = q[me[0], me[1], me[2], rows].astype(jnp.float32) + r2[rows].astype(jnp.float32)
        grad = norm_back(rows, back, resid_ref, gain_ref, cot_ref, gain_acc)
        grad_ref[rows] = grad
        low[rows] = grad.astype(low.dtype)
        return carry

    lax.fori_loop(0, low.shape[0] // STRIP, strip, 0)
    for copy in sent + to_core:
        copy.wait_send()
    gain_out[...] = jnp.sum(gain_acc[...], axis=0, keepdims=True)
    mine = all_ref.at[me[2], core]
    local = pltpu.make_async_copy(low, mine, gather_own)
    local.start()
    along = send(low, mine, gs.at[0], gr.at[0], peers[2])
    beside = send(low, mine, gs.at[1], gr.at[1], core_peer)
    along.wait_recv()
    theirs = all_ref.at[1 - me[2], core]
    onward = send(theirs, theirs, gs.at[2], gr.at[2], core_peer)
    local.wait()
    beside.wait()
    onward.wait()
    along.wait_send()


def back_pass(part, resid, cot, gain):
    rows, width = resid.shape
    wide = lambda *lead: pltpu.VMEM((*lead, rows, width), jnp.bfloat16)
    vmem = pl.BlockSpec(memory_space=pltpu.VMEM)
    return pl.pallas_call(
        back_kernel,
        name="back",
        out_shape=(
            jax.ShapeDtypeStruct((rows, width), jnp.float32),
            jax.ShapeDtypeStruct((2, 2, rows, width), jnp.bfloat16),
            jax.ShapeDtypeStruct((1, width), jnp.float32),
        ),
        in_specs=[pl.BlockSpec(memory_space=pl.ANY), vmem, vmem, vmem],
        out_specs=(vmem, pl.BlockSpec(memory_space=pl.ANY), vmem),
        scratch_shapes=[
            wide(2, 2, 2),
            wide(2, 2, 2),
            wide(2, 2),
            wide(2),
            wide(),
            wide(),
            pltpu.VMEM((8, width), jnp.float32),
            pltpu.SemaphoreType.DMA((len(ORDERS), 3)),
            pltpu.SemaphoreType.DMA((len(ORDERS), 3)),
            pltpu.SemaphoreType.DMA((2 * len(ORDERS),)),
            pltpu.SemaphoreType.DMA((2 * len(ORDERS),)),
            pltpu.SemaphoreType.DMA,
            pltpu.SemaphoreType.DMA((3,)),
            pltpu.SemaphoreType.DMA((3,)),
            pltpu.SemaphoreType.DMA,
        ],
        compiler_params=pltpu.CompilerParams(
            collective_id=2, has_side_effects=True, vmem_limit_bytes=40 * 2**20
        ),
    )(part.reshape(2, 2, 2, 2, rows, width), resid, cot, gain.reshape(1, width))


class Halve:
    def __init__(self, source, held, came, load_sem, send_sem, recv_sem, order, at_column=0):
        self.held, self.came, self.sems, self.order = held, came, (send_sem, recv_sem), order
        self.dims = sorted(order, reverse=True)
        self.sent, self.loads, at = [], [], 0
        lead = [slice(None) for _ in order]
        columns = pl.ds(at_column, held.shape[-1])
        for i, part in enumerate(source):
            rows = part.shape[-2]
            self.loads.append(
                pltpu.make_async_copy(
                    part.at[(*lead, slice(None), columns)],
                    held.at[(*lead, pl.ds(at, rows))],
                    load_sem.at[i],
                )
            )
            self.loads[-1].start()
            at += rows

    def index(self, done, away=None):
        picks = []
        for bit in self.dims:
            if bit in done:
                picks.append(bit_of("dp", bit))
            elif bit == away:
                picks.append(1 - bit_of("dp", bit))
            else:
                picks.append(slice(None))
        return tuple(picks)

    def start(self, step):
        if step == 0:
            for load in self.loads:
                load.wait()
        bit = self.order[step]
        self.moving = send(
            self.held.at[self.index(self.order[:step], bit)],
            self.came[step],
            self.sems[0].at[step],
            self.sems[1].at[step],
            across("dp", bit),
        )
        self.sent.append(self.moving)

    def land(self, step):
        self.moving.wait_recv()
        kept = self.index(self.order[: step + 1])
        self.held[kept] = self.held[kept] + self.came[step][...]
        if step + 1 < len(self.order):
            self.start(step + 1)

    def result(self):
        return self.held[self.index(self.order)]

    def finish(self):
        for copy in self.sent:
            copy.wait_send()


def halve_scratch(bits, rows, width):
    scratch = [pltpu.VMEM((*[2] * bits, rows, width), jnp.bfloat16)]
    for step in range(bits):
        scratch.append(pltpu.VMEM((*[2] * (bits - 1 - step), rows, width), jnp.bfloat16))
    return scratch + [
        pltpu.SemaphoreType.DMA((2,)),
        pltpu.SemaphoreType.DMA((bits,)),
        pltpu.SemaphoreType.DMA((bits,)),
    ]


def last_plan(bits, rows, few_rows, width):
    wide = -(-width // 256) * 128
    swapped = [1, 0, *range(2, bits)]
    return [
        (list(range(bits)), 0, halve_scratch(bits, rows + few_rows, wide)),
        (swapped, wide, halve_scratch(bits, rows + few_rows, width - wide)),
        (list(range(1, bits)), 0, halve_scratch(bits - 1, rows, width)),
        ([0, *range(2, bits)], 0, halve_scratch(bits - 1, rows, width)),
    ]


def last_kernel(
    plan, part_ref, tok_ref, keep_ref, gain_ref, wide_ref, few_ref, y_ref, o_ref,
    row_ref,
    grad_ref, gain_out, wide_out, few_out, y_out, o_out, row_out,
    q, core_buf, link_buf, gain_acc, *refs
):
    sum_sems, refs = refs[:3], refs[3:]
    sources = ((wide_ref, few_ref), (wide_ref, few_ref), (y_ref,), (o_ref,))
    halvings = []
    for source, (order, column, scratch) in zip(sources, plan):
        mine, refs = refs[: len(scratch)], refs[len(scratch) :]
        came = mine[1 : 1 + len(order)]
        halvings.append(Halve(source, mine[0], came, *mine[1 + len(order) :], order, column))
    bits = len(plan[0][0])
    peers = [across("dp", bit) for bit in range(bits)]
    spot, *spots = spots_of_four()
    both = {"dp": lax.axis_index("dp") + (spots[2] - spot) * (1 << FIRST_BIT)}
    greet([across(*LINKS[2]), across(*CORE), both] + peers)
    total = SumTensor(part_ref, q, core_buf, link_buf, *sum_sems)
    turns = [halvings[i] for i in (2, 3, 1, 0)]
    for each in turns:
        each.start(0)
    collects = [Collect(row_ref, row_out, *refs)]
    total.pass_on()
    gain_acc[...] = jnp.zeros_like(gain_acc)

    def strip(i, carry):
        rows = pl.ds(pl.multiple_of(i * STRIP, STRIP), STRIP)
        back = total.rows(rows)
        grad_ref[rows] = norm_back(rows, back, tok_ref, gain_ref, keep_ref, gain_acc)
        return carry

    total.arrive()
    lax.fori_loop(0, tok_ref.shape[0] // STRIP, strip, 0)
    gain_out[...] = jnp.sum(gain_acc[...], axis=0, keepdims=True)
    for step in range(bits):
        for each in turns:
            if step < len(each.order):
                each.land(step)
    rows = wide_out.shape[0]
    for each, (_, column, _) in zip(halvings[:2], plan):
        mine = each.result()
        columns = slice(column, column + mine.shape[1])
        wide_out[:, columns] = mine[:rows].astype(jnp.float32)
        few_out[:, columns] = mine[rows:]
    for each in collects:
        each.finish()
    y_out[...] = halvings[2].result().astype(jnp.float32)
    o_out[...] = halvings[3].result().astype(jnp.float32)
    for each in (*halvings, total):
        each.finish()


def last_pass(part, tok, keep, gain, wide, few, side_y, side_o, rows_part, hidden_width):
    rows, width = tok.shape
    vmem, anywhere = pl.BlockSpec(memory_space=pltpu.VMEM), pl.BlockSpec(memory_space=pl.ANY)
    bits = wide.shape[0].bit_length() - 1
    plan = last_plan(bits, wide.shape[1], few.shape[1], wide.shape[2])
    block = jax.ShapeDtypeStruct(wide.shape[1:], jnp.float32)
    leading = [2] * bits
    return pl.pallas_call(
        functools.partial(last_kernel, plan),
        name="last",
        out_shape=(
            jax.ShapeDtypeStruct((rows, width), jnp.float32),
            jax.ShapeDtypeStruct((1, width), jnp.float32),
            block,
            jax.ShapeDtypeStruct(few.shape[1:], jnp.bfloat16),
            block,
            block,
            jax.ShapeDtypeStruct((rows_part.shape[1], hidden_width), jnp.float32),
        ),
        in_specs=[anywhere, vmem, vmem, vmem] + [anywhere] * 5,
        out_specs=(vmem,) * 7,
        scratch_shapes=[
            pltpu.VMEM((2, rows, width), jnp.bfloat16),
            pltpu.VMEM((2, rows, width), jnp.bfloat16),
            pltpu.VMEM((rows, width), jnp.bfloat16),
            pltpu.VMEM((8, width), jnp.float32),
            *SUM_SEMS,
            *[ref for _, _, scratch in plan for ref in scratch],
            *collect_scratch(*rows_part.shape[1:]),
        ],
        compiler_params=pltpu.CompilerParams(
            collective_id=3, has_side_effects=True, vmem_limit_bytes=48 * 2**20
        ),
    )(
        part.reshape(2, 2, rows, width),
        tok,
        keep,
        gain.reshape(1, width),
        wide.reshape(*leading, *wide.shape[1:]),
        few.reshape(*leading, *few.shape[1:]),
        side_y,
        side_o,
        rows_part,
    )


def scan_kernel(n, reverse, *refs):
    a_ref, b_ref, out_ref, edge_ref, fa, fb, mine, others, ssem, rsem = refs
    place = lax.axis_index("dp")
    sign = -1 if reverse else 1
    barrier = pltpu.get_barrier_semaphore()
    peers = [{"dp": (place + sign * hop + n) % n} for hop in range(1, n)]
    for peer in peers:
        pl.semaphore_signal(barrier, inc=1, device_id=peer, device_id_type=MESH)
    rows, width = a_ref.shape
    length = rows // 8
    lanes = range(width // 128)
    for k in lanes:
        fa[k * rows : (k + 1) * rows] = a_ref[:, k * 128 : (k + 1) * 128]
        fb[k * rows : (k + 1) * rows] = b_ref[:, k * 128 : (k + 1) * 128]

    def at(k, r):
        return pl.ds(k * rows + (length - 1 - r if reverse else r), 8, stride=length)

    def local(r, carry):
        result = []
        for k in lanes:
            prod, state = carry[k]
            decay = fa[at(k, r), :]
            term = fb[at(k, r), :]
            if reverse:
                fa[at(k, r), :] = prod
                total = term + state
                fb[at(k, r), :] = total
                result.append((prod * decay, decay * total))
            else:
                prod = prod * decay
                state = decay * state + term
                fa[at(k, r), :] = prod
                fb[at(k, r), :] = state
                result.append((prod, state))
        return result

    start = [(jnp.ones((8, 128), jnp.float32), jnp.zeros((8, 128), jnp.float32)) for k in lanes]
    ends = lax.fori_loop(0, length, local, start, unroll=2)
    prod = jnp.concatenate([end[0] for end in ends], axis=1)
    state = jnp.concatenate([end[1] for end in ends], axis=1)
    order = range(7, -1, -1) if reverse else range(8)
    run_a, run_b = jnp.ones((1, width), jnp.float32), jnp.zeros((1, width), jnp.float32)
    before = [None] * 8
    for s in order:
        before[s] = (run_a, run_b)
        pa, pb = prod[s : s + 1], state[s : s + 1]
        run_a, run_b = pa * run_a, pa * run_b + pb
    mine[0:1] = run_a
    mine[1:2] = run_b
    pl.semaphore_wait(barrier, n - 1)
    copies = [
        send(mine, others.at[hop - 1], ssem.at[hop - 1], rsem.at[hop - 1], peers[hop - 1])
        for hop in range(1, n)
    ]
    carry = jnp.zeros((1, width), jnp.float32)
    ahead = n - 1 - place if reverse else place
    for copy in copies:
        copy.wait_recv()
    for hop in range(n - 1, 0, -1):
        step = others[hop - 1, 0:1] * carry + others[hop - 1, 1:2]
        carry = jnp.where(hop <= ahead, step, carry)
    edge_ref[...] = carry
    entering = jnp.concatenate([pa * carry + pb for pa, pb in before], axis=0)

    def fix(r, c):
        for k in lanes:
            fb[at(k, r), :] = fb[at(k, r), :] + fa[at(k, r), :] * entering[:, k * 128 : (k + 1) * 128]
        return c

    lax.fori_loop(0, length, fix, 0, unroll=2)
    for k in lanes:
        out_ref[:, k * 128 : (k + 1) * 128] = fb[k * rows : (k + 1) * rows]
    for copy in copies:
        copy.wait_send()


def scan_stream(decay, term, reverse):
    n = lax.axis_size("dp")
    rows, width = decay.shape
    vmem = pl.BlockSpec(memory_space=pltpu.VMEM)
    return pl.pallas_call(
        functools.partial(scan_kernel, n, reverse),
        name="scan_back" if reverse else "scan",
        out_shape=(
            jax.ShapeDtypeStruct((rows, width), jnp.float32),
            jax.ShapeDtypeStruct((1, width), jnp.float32),
        ),
        in_specs=[vmem, vmem],
        out_specs=(vmem, vmem),
        scratch_shapes=[
            pltpu.VMEM((rows * width // 128, 128), jnp.float32),
            pltpu.VMEM((rows * width // 128, 128), jnp.float32),
            pltpu.VMEM((2, width), jnp.float32),
            pltpu.VMEM((n - 1, 2, width), jnp.float32),
            pltpu.SemaphoreType.DMA((n - 1,)),
            pltpu.SemaphoreType.DMA((n - 1,)),
        ],
        compiler_params=pltpu.CompilerParams(
            collective_id=5 if reverse else 4, has_side_effects=True, vmem_limit_bytes=32 * 2**20
        ),
    )(decay, term)


def in_order(bit, mine, theirs, axis=0):
    return jnp.where(
        bit == 0, jnp.concatenate([mine, theirs], axis), jnp.concatenate([theirs, mine], axis)
    )


def parted(held, dims, bit):
    mine = (lax.axis_index("dp") >> bit) % 2
    axis = dims.index(bit)
    return (
        lax.dynamic_index_in_dim(held, mine, axis, False),
        lax.dynamic_index_in_dim(held, 1 - mine, axis, False),
    )


def added(keep, came):
    return (keep.astype(jnp.float32) + came.astype(jnp.float32)).astype(jnp.bfloat16)


def inner(
    tokens,
    doc_start,
    norm1_gain,
    proj_x,
    proj_y,
    conv_weight,
    conv_bias,
    gate_x_weight,
    gate_x_bias,
    gate_a_weight,
    gate_a_bias,
    decay_param,
    proj_out,
    norm2_gain,
    mlp_gate,
    mlp_up,
    mlp_down,
    cotangent,
):
    tok_rows = tokens.shape[0]
    chan_width = proj_x.shape[1]
    block_width = gate_x_weight.shape[0]
    half_width = block_width // 2
    tap_count = conv_weight.shape[0]
    parity = lax.axis_index("tensor") % 2
    full_start = parity * half_width
    shared_start = (1 - parity) * 2 * block_width
    tensor_size = lax.axis_size("tensor")
    share_rows = tok_rows // tensor_size
    own_start = lax.axis_index("tensor") * share_rows
    positions = lax.axis_index("dp") * tok_rows + lax.iota(jnp.int32, tok_rows)
    starting = (doc_start == positions)[:, None]
    dp_size = lax.axis_size("dp")
    low_size = 1 << FIRST_BIT
    high_size = dp_size // (GROUP * low_size)

    def dp_index(high, four, low):
        return (high * GROUP + four) * low_size + low

    highs, fours, lows = range(high_size), range(GROUP), range(low_size)
    groups = [
        [dp_index(h, i, l) * tensor_size + t for i in fours for t in range(tensor_size)]
        for h in highs
        for l in lows
    ]
    low_groups = [[dp_index(h, i, l) for l in lows] for h in highs for i in fours]
    high_groups = [[dp_index(h, i, l) for h in highs] for i in fours for l in lows]
    everyone = ("dp", "tensor")

    spot = lax.axis_index("dp") // low_size % GROUP
    hidden_width = mlp_gate.shape[1]
    share = share_width(hidden_width)

    def all_rows(part):
        rows = part.shape[1]
        if low_size > 1:
            part = lax.all_gather(
                part[:, None], "dp", axis=1, axis_index_groups=low_groups, tiled=True
            )
        if high_size > 1:
            part = lax.all_gather(part, "dp", axis=0, axis_index_groups=high_groups, tiled=True)
        return part.reshape(dp_size * rows, share)

    def own_rows(grad):
        rows = grad.shape[0] // dp_size
        grad = grad.astype(jnp.bfloat16).reshape(high_size * GROUP, low_size, rows, share)
        if high_size > 1:
            grad = lax.psum_scatter(
                grad, "dp", axis_index_groups=high_groups, scatter_dimension=0, tiled=True
            )
        if low_size > 1:
            grad = lax.psum_scatter(
                grad, "dp", axis_index_groups=low_groups, scatter_dimension=1, tiled=True
            )
        return grad.reshape(GROUP, rows, share)

    cot_own = lax.dynamic_slice_in_dim(cotangent, own_start, share_rows, 0)
    gate_pieces = exchanged(cut(mlp_gate))
    pieces = exchanged(cut(mlp_up, mlp_down))
    tok_own = lax.dynamic_slice_in_dim(tokens, own_start, share_rows, 0)

    def normalize(values):
        values = values.astype(jnp.float32)
        inv_rms = lax.rsqrt(jnp.mean(values * values, axis=-1, keepdims=True) + epsilon)
        return (values * inv_rms * norm1_gain).astype(jnp.bfloat16)

    halo = 16
    normed_low = normalize(tokens)
    normed_low, *gate_pieces = lax.optimization_barrier((normed_low, *gate_pieces))
    gate_cols = all_rows(*placed(gate_pieces))
    normed_prev = normalize(shifted(tokens[tok_rows - halo :], "dp", 1))
    branch_y = matmul(normed_low, proj_y)
    branch_x = matmul(normed_low, proj_x).astype(jnp.bfloat16)
    prev_x = matmul(normed_prev, proj_x).astype(jnp.bfloat16)
    extended = jnp.concatenate([prev_x[halo - tap_count + 1 :], branch_x], axis=0).astype(
        jnp.float32
    )

    def conv_apply(ext_rows, weight, bias_vec):
        conv_out = bias_vec + weight[0] * ext_rows[tap_count - 1 :]
        for offset in range(1, tap_count):
            inside = (positions - offset >= doc_start).astype(jnp.float32)[:, None]
            lagged = ext_rows[tap_count - 1 - offset : tap_count - 1 - offset + tok_rows]
            conv_out = conv_out + weight[offset] * lagged * inside
        return conv_out

    conv_out, conv_pull = jax.vjp(conv_apply, extended, conv_weight, conv_bias)
    mixed_low = conv_out.astype(jnp.bfloat16)
    own_half = lax.dynamic_slice_in_dim(mixed_low, shared_start, half_width, 1)
    other_half = flipped(own_half, "tensor", 1)
    shared_in = in_order(parity, own_half, other_half, 1)
    full_in = lax.dynamic_slice_in_dim(mixed_low, full_start, 2 * block_width, 1).reshape(
        tok_rows, 2, block_width
    )

    def place(full_part, shared_part):
        return in_order(parity, full_part, shared_part, 1)

    def full_weight(weight):
        return lax.dynamic_slice_in_dim(weight, full_start, 2 * block_width, 1).reshape(
            block_width, 2, block_width
        )

    def shared_weight(weight):
        return lax.dynamic_slice_in_dim(weight, shared_start, half_width, 1)

    def gate_pre(weight, bias_vec):
        full_out = jnp.einsum(
            "nhi,ihj->nhj", full_in, full_weight(weight), preferred_element_type=jnp.float32
        ).reshape(tok_rows, 2 * block_width)
        shared_out = matmul(shared_in, shared_weight(weight))
        return place(full_out, shared_out) + bias_vec

    def recurrence_in(conv_vals, pre_input, pre_recur, param_vec):
        log_decay = -8.0 * jax.nn.sigmoid(pre_recur) * jax.nn.softplus(param_vec)
        decay = jnp.where(starting, 0.0, jnp.exp(log_decay))
        multiplier = jnp.where(starting, 1.0, jnp.sqrt(-jnp.expm1(2.0 * log_decay)))
        return (decay, multiplier * jax.nn.sigmoid(pre_input) * conv_vals)

    pre_input = gate_pre(gate_x_weight, gate_x_bias)
    pre_recur = gate_pre(gate_a_weight, gate_a_bias)
    (decay, drive), recur_pull = jax.vjp(
        recurrence_in, mixed_low.astype(jnp.float32), pre_input, pre_recur, decay_param
    )
    decay, drive, *pieces = lax.optimization_barrier((decay, drive, *pieces))
    up_cols, down_cols = (all_rows(part) for part in placed(pieces))
    states, entering = scan_stream(decay, drive, False)
    previous = jnp.concatenate([entering, states[:-1]], axis=0)
    gelu_y, gelu_pull = jax.vjp(gelu_tanh, branch_y)
    product_low = (states * gelu_y).astype(jnp.bfloat16)
    lru_part = matmul(product_low, proj_out).astype(jnp.bfloat16)
    resid, normed2_all, cot_all = middle(lru_part, tok_own, cot_own, norm2_gain)
    cot_all = cot_all.reshape(GROUP * tok_rows, -1)
    normed2_all = normed2_all.reshape(GROUP * tok_rows, -1)
    counted = lax.iota(jnp.int32, share) >= overlap_of(hidden_width) * (spot // (GROUP - 1))

    def once(values):
        return jnp.where(counted, values, 0.0).astype(jnp.bfloat16)

    gate_act = matmul(normed2_all, gate_cols)
    up_act = matmul(normed2_all, up_cols)
    hidden, act_pull = jax.vjp(gated_product, gate_act, up_act)
    hidden_low = once(hidden)
    grad_hidden = matmul(cot_all, down_cols)
    grad_gate, grad_up = act_pull(grad_hidden)
    grad_gate_low = once(grad_gate)
    grad_up_low = once(grad_up)

    back_part = product_pair(grad_gate_low, grad_up_low, gate_cols, up_cols)
    down_grad = contract_first(cot_all, hidden_low).astype(jnp.bfloat16)
    gate_grad = contract_first(normed2_all, grad_gate_low).astype(jnp.bfloat16)
    down_rows, gate_rows = own_rows(down_grad), own_rows(gate_grad)
    back_part, _, _ = lax.optimization_barrier((back_part, down_grad, gate_grad))
    grad_resid, grad_lru_low, grad_gain2 = back_pass(back_part, resid, cot_own, norm2_gain)
    grad_lru_low = grad_lru_low.reshape(tok_rows, -1)
    grad_product = contract_last(grad_lru_low, proj_out)
    grad_states = grad_product * gelu_y
    grad_y_low = gelu_pull(grad_product * states)[0].astype(jnp.bfloat16)
    total_grad, _ = scan_stream(decay, grad_states, True)
    total_grad, late_y, late_lru = lax.optimization_barrier(
        (total_grad, grad_y_low, grad_lru_low)
    )

    def token_sum(left_rows, right_rows):
        return contract_first(left_rows, right_rows).astype(jnp.bfloat16)

    def per_device(rows):
        return rows.reshape(dp_size, rows.shape[0] // dp_size, rows.shape[1])

    dims = list(range(dp_size.bit_length() - 1))[::-1]

    def by_bits(grad):
        return grad.reshape(*[2] * len(dims), grad.shape[0] // dp_size, grad.shape[1])

    keep_y, away_y = parted(by_bits(token_sum(normed_low, late_y)), dims, 0)
    keep_o, away_o = parted(by_bits(token_sum(late_lru, product_low)), dims, 1)
    total_grad, away_y, away_o, late_up, late_hidden = lax.optimization_barrier(
        (total_grad, away_y, away_o, grad_up_low, hidden_low)
    )
    came_y, came_o = flipped(away_y, "dp", 1), flipped(away_o, "dp", 2)
    up_grad = contract_first(normed2_all, late_up)
    out_part = contract_last(late_hidden, down_cols).astype(jnp.bfloat16)
    up_rows = own_rows(up_grad)
    block_out = resid + lax.psum_scatter(
        out_part,
        everyone,
        axis_index_groups=groups,
        scatter_dimension=0,
        tiled=True,
    ).astype(jnp.float32)
    back_y = contract_last(late_y, proj_y)
    conv_direct, grad_pre_input, grad_pre_recur, grad_param = recur_pull(
        (total_grad * previous, total_grad)
    )

    grad_pre_input, grad_pre_recur, *rows = lax.optimization_barrier(
        (grad_pre_input, grad_pre_recur, down_rows, gate_rows)
    )
    row_pieces = picked(*rows)
    row_pieces = exchanged(row_pieces)

    def gate_back(weight, grad_pre):
        grad_pre_low = grad_pre.astype(jnp.bfloat16)
        grad_full = lax.dynamic_slice_in_dim(grad_pre_low, full_start, 2 * block_width, 1).reshape(
            tok_rows, 2, block_width
        )
        grad_share = lax.dynamic_slice_in_dim(grad_pre_low, shared_start, half_width, 1)
        into_full = jnp.einsum(
            "nhj,ihj->nhi", grad_full, full_weight(weight), preferred_element_type=jnp.float32
        ).reshape(tok_rows, 2 * block_width)
        into_share = contract_last(grad_share, shared_weight(weight))
        weight_full = jnp.einsum(
            "nhi,nhj->ihj", full_in, grad_full, preferred_element_type=jnp.float32
        ).reshape(block_width, 2 * block_width)
        weight_share = contract_first(shared_in, grad_share)
        return (into_full, into_share, place(weight_full, weight_share))

    input_full, input_share, grad_gx_weight = gate_back(gate_x_weight, grad_pre_input)
    recur_full, recur_share, grad_ga_weight = gate_back(gate_a_weight, grad_pre_recur)
    full_sum = input_full + recur_full
    share_sum = input_share + recur_share
    own_grad = jnp.where(parity == 0, share_sum[:, :half_width], share_sum[:, half_width:])
    other_grad = jnp.where(parity == 0, share_sum[:, half_width:], share_sum[:, :half_width])
    returned = flipped(other_grad.astype(jnp.bfloat16), "tensor", 1).astype(other_grad.dtype)
    grad_conv = conv_direct + place(full_sum, own_grad + returned)
    grad_extended, grad_conv_weight, grad_conv_bias = conv_pull(grad_conv)
    rim_rows, came_y, came_o = lax.optimization_barrier(
        (grad_extended[: tap_count - 1], came_y, came_o)
    )
    side_y, side_o = added(keep_y, came_y), added(keep_o, came_o)
    rim_grad = shifted(rim_rows, "dp", -1)
    grad_branch_x = grad_extended[tap_count - 1 :] + jnp.concatenate(
        [jnp.zeros((tok_rows - tap_count + 1, chan_width), jnp.float32), rim_grad], axis=0
    )
    grad_x_low = grad_branch_x.astype(jnp.bfloat16)
    wide = jnp.concatenate([grad_gx_weight, grad_ga_weight], axis=0)
    sums = jnp.concatenate(
        [
            grad_conv_weight,
            grad_conv_bias[None],
            jnp.sum(grad_pre_input, axis=0)[None],
            jnp.sum(grad_pre_recur, axis=0)[None],
            grad_param[None],
        ],
        axis=0,
    )
    spare = dp_size * 16 - sums.shape[0]
    sums = jnp.concatenate([sums, jnp.zeros((spare, chan_width), jnp.float32)], axis=0)
    few = jnp.concatenate(
        [per_device(wide.astype(jnp.bfloat16)), per_device(sums.astype(jnp.bfloat16))], axis=1
    )
    grad_tokens, grad_gain1, grad_proj_x, reduced, grad_proj_y, grad_out, grad_mlp_up = last_pass(
        (contract_last(grad_x_low, proj_x) + back_y).astype(jnp.bfloat16),
        tok_own,
        grad_resid,
        norm1_gain,
        per_device(token_sum(normed_low, grad_x_low)),
        few,
        side_y,
        side_o,
        up_rows,
        hidden_width,
    )
    grad_proj_out = grad_out.T
    shared, gains = final_pass(reduced, grad_gain1, grad_gain2)
    gains, *row_pieces = lax.optimization_barrier((gains, *row_pieces))
    grad_mlp_down, grad_mlp_gate = joined(row_pieces, hidden_width)
    wide_rows = 2 * block_width // dp_size
    wide = shared[:, :wide_rows].reshape(2 * block_width, chan_width).astype(jnp.float32)
    small = shared[:, wide_rows:].reshape(dp_size * 16, chan_width).astype(jnp.float32)
    return (
        block_out,
        grad_tokens,
        gains[0],
        grad_proj_x,
        grad_proj_y,
        small[:tap_count],
        small[tap_count],
        wide[:block_width],
        small[tap_count + 1],
        wide[block_width:],
        small[tap_count + 2],
        small[tap_count + 3],
        grad_proj_out,
        gains[1],
        grad_mlp_gate,
        grad_mlp_up,
        grad_mlp_down,
    )


def solution(mesh):
    placed = (
        P("dp", None),
        P("dp"),
        P(),
        P(None, "tensor"),
        P(None, "tensor"),
        P(None, "tensor"),
        P("tensor"),
        P(None, "tensor"),
        P("tensor"),
        P(None, "tensor"),
        P("tensor"),
        P("tensor"),
        P("tensor", None),
        P(),
        P("dp", "tensor"),
        P("dp", "tensor"),
        P("dp", "tensor"),
        P("dp", None),
    )
    return jax.shard_map(
        inner,
        mesh=mesh,
        in_specs=placed,
        out_specs=(
            P(("dp", "tensor"), None),
            P(("dp", "tensor"), None),
            P(),
            P("dp", "tensor"),
            P("dp", "tensor"),
            P(None, "tensor"),
            P("tensor"),
            P(None, "tensor"),
            P("tensor"),
            P(None, "tensor"),
            P("tensor"),
            P("tensor"),
            P("tensor", "dp"),
            P(),
            P("dp", "tensor"),
            P("dp", "tensor"),
            P("dp", "tensor"),
        ),
        check_vma=False,
    )
```

```python
import functools

import jax
import jax.numpy as jnp
from jax import lax
from jax.experimental import pallas as pl
from jax.experimental.pallas import tpu as pltpu
from jax.sharding import PartitionSpec as P


epsilon = 1e-06
MESH = pl.DeviceIdType.MESH
GROUP = 4
STRIP = 16
FIRST_BIT = 0
LINKS = (("dp", FIRST_BIT + 1), ("dp", FIRST_BIT), ("tensor", 1))
CORE = ("tensor", 0)
ORDERS = ((0, 1, 2), (0, 2, 1), (1, 2, 0), (2, 0, 1))
TILES = (9, 5, 3)
SUM_ORDERS = tuple(order[::-1] for order in ORDERS)
COLORS = range(len(ORDERS))


def gelu_tanh(values):
    return jax.nn.gelu(values, approximate=True)


def gated_product(gate_vals, up_vals):
    return gelu_tanh(gate_vals) * up_vals


def contract_last(left_rows, right_rows):
    return lax.dot_general(
        left_rows, right_rows, (((1,), (1,)), ((), ())), preferred_element_type=jnp.float32
    )


def contract_first(left_rows, right_rows):
    return lax.dot_general(
        left_rows, right_rows, (((0,), (0,)), ((), ())), preferred_element_type=jnp.float32
    )


def matmul(left_rows, right_rows):
    return jnp.dot(left_rows, right_rows, preferred_element_type=jnp.float32)


def shifted(block, axis, distance):
    devices = range(lax.axis_size(axis))
    route = [(i - distance, i) for i in devices if i - distance in devices]
    return lax.ppermute(block, axis, route)


def flipped(array, axis, mask):
    return lax.ppermute(array, axis, [(i, i ^ mask) for i in range(lax.axis_size(axis))])


def bit_of(axis, bit):
    return (lax.axis_index(axis) // (1 << bit)) % 2


def across(axis, bit):
    index = lax.axis_index(axis)
    return {axis: index + (1 - 2 * ((index // (1 << bit)) % 2)) * (1 << bit)}


def column_spans(width):
    tiles = width // 128
    counts = [tiles * part // 20 for part in TILES]
    spans, start = [], 0
    for count in (*counts, tiles - sum(counts)):
        spans.append((start * 128, count * 128))
        start += count
    return spans


def send(src, dst, send_sem, recv_sem, device):
    copy = pltpu.make_async_remote_copy(
        src_ref=src,
        dst_ref=dst,
        send_sem=send_sem,
        recv_sem=recv_sem,
        device_id=device,
        device_id_type=MESH,
    )
    copy.start()
    return copy


def greet(devices):
    barrier = pltpu.get_barrier_semaphore()
    for device in devices:
        pl.semaphore_signal(barrier, inc=1, device_id=device, device_id_type=MESH)
    pl.semaphore_wait(barrier, len(devices))


class Gather:
    def __init__(self, x_ref, out_ref, send_sem, recv_sem, core_send, core_recv, own_sem):
        self.sems = send_sem, recv_sem, core_send, core_recv
        self.out = out_ref
        self.me = [bit_of(*link) for link in LINKS]
        self.core = bit_of(*CORE)
        self.peers = [across(*link) for link in LINKS]
        self.core_peer = across(*CORE)
        self.spans = column_spans(x_ref.shape[1])
        me, place = self.me, out_ref.at[self.me[0], self.me[1], self.me[2], self.core]
        self.own = pltpu.make_async_copy(x_ref, place, own_sem)
        self.own.start()
        self.moving = [
            send(
                x_ref.at[:, pl.ds(*self.spans[k])],
                self.region(me, k),
                send_sem.at[k, 0],
                recv_sem.at[k, 0],
                self.peers[ORDERS[k][0]],
            )
            for k in COLORS
        ]
        self.to_core = [send(x_ref, place, core_send.at[3 * len(ORDERS)], core_recv.at[3 * len(ORDERS)], self.core_peer)]
        self.sent = []

    def region(self, idx, k):
        return self.out.at[idx[0], idx[1], idx[2], self.core, :, pl.ds(*self.spans[k])]

    def step(self, step):
        send_sem, recv_sem, core_send, core_recv = self.sems
        me = self.me
        if step == 0:
            self.own.wait()
        for k in COLORS:
            order = ORDERS[k]
            self.moving[k].wait_recv()
            self.sent.append(self.moving[k])
            if step < 2:
                held = [slice(None) if d in order[: step + 1] else me[d] for d in range(3)]
                self.moving[k] = send(
                    self.region(held, k),
                    self.region(held, k),
                    send_sem.at[k, step + 1],
                    recv_sem.at[k, step + 1],
                    self.peers[order[step + 1]],
                )
            fresh = [
                slice(None) if d in order[:step] else (1 - me[d] if d == order[step] else me[d])
                for d in range(3)
            ]
            self.to_core.append(
                send(
                    self.region(fresh, k),
                    self.region(fresh, k),
                    core_send.at[len(ORDERS) * step + k],
                    core_recv.at[len(ORDERS) * step + k],
                    self.core_peer,
                )
            )

    def finish(self):
        for copy in self.sent:
            copy.wait_send()
        for copy in self.to_core:
            copy.wait()


def spots_of_four():
    spot = lax.axis_index("dp") // (1 << FIRST_BIT) % GROUP
    return spot, spot + 1 - 2 * (spot % 2), spot + 2 - 4 * (spot // 2), GROUP - 1 - spot


def share_width(width):
    return -(-width // (128 * GROUP)) * 128


def overlap_of(width):
    return GROUP * share_width(width) - width


def cut_kernel(count, *refs):
    width = refs[0].shape[1]
    share, over = share_width(width), overlap_of(width)
    for spot, out in zip(spots_of_four(), refs[count:]):
        start = share * spot - over * (spot // (GROUP - 1))
        for i in range(count):
            out[i] = refs[i][:, pl.ds(pl.multiple_of(start, 128), share)]


def cut(*weights):
    rows, share = weights[0].shape[0], share_width(weights[0].shape[1])
    return pl.pallas_call(
        functools.partial(cut_kernel, len(weights)),
        name="cut",
        out_shape=[jax.ShapeDtypeStruct((len(weights), rows, share), jnp.bfloat16)] * GROUP,
        compiler_params=pltpu.CompilerParams(vmem_limit_bytes=24 * 2**20),
    )(*weights)


def place_kernel(count, *refs):
    for spot, piece in zip(spots_of_four(), refs[:GROUP]):
        for i in range(count):
            refs[GROUP][i, spot] = piece[i]


def placed(pieces):
    count, rows, share = pieces[0].shape
    return pl.pallas_call(
        functools.partial(place_kernel, count),
        name="place",
        out_shape=jax.ShapeDtypeStruct((count, GROUP, rows, share), jnp.bfloat16),
        compiler_params=pltpu.CompilerParams(vmem_limit_bytes=24 * 2**20),
    )(*pieces)


def pick_kernel(count, *refs):
    for spot, out in zip(spots_of_four(), refs[count:]):
        for i in range(count):
            out[i] = refs[i][spot]


def picked(*parts):
    _, rows, share = parts[0].shape
    return pl.pallas_call(
        functools.partial(pick_kernel, len(parts)),
        name="pick",
        out_shape=[jax.ShapeDtypeStruct((len(parts), rows, share), jnp.bfloat16)] * GROUP,
        compiler_params=pltpu.CompilerParams(vmem_limit_bytes=24 * 2**20),
    )(*parts)


def join_kernel(count, *refs):
    pieces, outs, slots = refs[:GROUP], refs[GROUP : GROUP + count], refs[GROUP + count]
    for spot, piece in zip(spots_of_four(), pieces):
        for i in range(count):
            slots[i, spot] = piece[i]
    rows, width = outs[0].shape
    share, over = share_width(width), overlap_of(width)

    def strip(step, carry):
        at = pl.ds(pl.multiple_of(step * STRIP, STRIP), STRIP)
        for i in range(count):
            for place in range(GROUP):
                skip = over * (place // (GROUP - 1))
                outs[i][at, share * place : min(share * (place + 1), width)] = slots[
                    i, place, at, skip:share
                ].astype(jnp.float32)
        return carry

    lax.fori_loop(0, rows // STRIP, strip, 0)


def joined(pieces, width):
    count, rows, share = pieces[0].shape
    return pl.pallas_call(
        functools.partial(join_kernel, count),
        name="join",
        out_shape=[jax.ShapeDtypeStruct((rows, width), jnp.float32)] * count,
        scratch_shapes=[pltpu.VMEM((count, GROUP, rows, share), jnp.bfloat16)],
        compiler_params=pltpu.CompilerParams(vmem_limit_bytes=32 * 2**20),
    )(*pieces)


class Collect:
    def __init__(self, part_ref, out_ref, slots, send_sem, recv_sem, own_sem):
        spot, *spots = spots_of_four()
        base = lax.axis_index("dp") - (spot << FIRST_BIT)
        self.out, self.slots = out_ref, slots
        self.copies = [
            send(
                part_ref.at[other],
                slots.at[spot],
                send_sem.at[m],
                recv_sem.at[m],
                {"dp": base + other * (1 << FIRST_BIT)},
            )
            for m, other in enumerate(spots)
        ]
        self.own = pltpu.make_async_copy(part_ref.at[spot], slots.at[spot], own_sem)
        self.own.start()

    def finish(self):
        self.own.wait()
        for copy in self.copies:
            copy.wait()
        rows, width = self.out.shape
        share, over = share_width(width), overlap_of(width)

        def strip(step, carry):
            at = pl.ds(pl.multiple_of(step * STRIP, STRIP), STRIP)
            for place in range(GROUP):
                skip = over * (place // (GROUP - 1))
                self.out[at, share * place : min(share * (place + 1), width)] = self.slots[
                    place, at, skip:share
                ].astype(jnp.float32)
            return carry

        lax.fori_loop(0, rows // STRIP, strip, 0)


def collect_scratch(rows, share):
    return [
        pltpu.VMEM((GROUP, rows, share), jnp.bfloat16),
        pltpu.SemaphoreType.DMA((GROUP - 1,)),
        pltpu.SemaphoreType.DMA((GROUP - 1,)),
        pltpu.SemaphoreType.DMA,
    ]


def exchanged(pieces):
    return [pieces[0]] + [flipped(pieces[m], "dp", m << FIRST_BIT) for m in range(1, GROUP)]


def final_kernel(
    n, bits, small_ref, gain1_ref, gain2_ref, all_ref, gains_ref, came, ssem, rsem, gs, gr
):
    place = lax.axis_index("dp")
    peers = [{"dp": (place + hop) % n} for hop in range(1, n)]
    greet(peers + [across("tensor", bit) for axis, bit in bits if axis == "tensor"])
    copies = [
        send(small_ref, all_ref.at[place], ssem.at[hop], rsem.at[hop], peers[hop])
        for hop in range(n - 1)
    ]
    all_ref[place] = small_ref[...]
    gains_ref[0:1] = gain1_ref[...]
    gains_ref[1:2] = gain2_ref[...]
    for step, (axis, bit) in enumerate(bits):
        copy = send(gains_ref, came.at[step], gs.at[step], gr.at[step], across(axis, bit))
        copy.wait()
        gains_ref[...] = gains_ref[...] + came[step]
    for copy in copies:
        copy.wait()


def final_pass(small, gain1, gain2):
    n = lax.axis_size("dp")
    bits = [
        (axis, bit)
        for axis in ("tensor", "dp")
        for bit in range(lax.axis_size(axis).bit_length() - 1)
    ]
    rows, width = small.shape
    vmem = pl.BlockSpec(memory_space=pltpu.VMEM)
    gains = (2, gain1.shape[1])
    return pl.pallas_call(
        functools.partial(final_kernel, n, bits),
        name="final",
        out_shape=(
            jax.ShapeDtypeStruct((n, rows, width), small.dtype),
            jax.ShapeDtypeStruct(gains, jnp.float32),
        ),
        in_specs=[vmem] * 3,
        out_specs=(vmem, vmem),
        scratch_shapes=[
            pltpu.VMEM((len(bits), *gains), jnp.float32),
            pltpu.SemaphoreType.DMA((n - 1,)),
            pltpu.SemaphoreType.DMA((n - 1,)),
            pltpu.SemaphoreType.DMA((len(bits),)),
            pltpu.SemaphoreType.DMA((len(bits),)),
        ],
        compiler_params=pltpu.CompilerParams(
            collective_id=8, has_side_effects=True, vmem_limit_bytes=24 * 2**20
        ),
    )(small, gain1, gain2)


GATHER_SEMS = [
    pltpu.SemaphoreType.DMA((len(ORDERS), 3)),
    pltpu.SemaphoreType.DMA((len(ORDERS), 3)),
    pltpu.SemaphoreType.DMA((3 * len(ORDERS) + 1,)),
    pltpu.SemaphoreType.DMA((3 * len(ORDERS) + 1,)),
    pltpu.SemaphoreType.DMA,
]


class SumTensor:
    def __init__(self, part_ref, q, core_buf, link_buf, sems_s, sems_r, own_sem):
        high, core = bit_of(*LINKS[2]), bit_of(*CORE)
        core_peer = across(*CORE)
        self.args = high, q, core_buf, link_buf, sems_s, sems_r
        self.own = pltpu.make_async_copy(part_ref.at[:, core], q, own_sem)
        self.own.start()
        self.copies = [
            send(
                part_ref.at[block, 1 - core],
                core_buf.at[block],
                sems_s.at[i],
                sems_r.at[i],
                core_peer,
            )
            for i, block in enumerate((1 - high, high))
        ]

    def pass_on(self):
        high, q, core_buf, link_buf, sems_s, sems_r = self.args
        self.own.wait()
        self.copies[0].wait_recv()
        q[1 - high] = q[1 - high] + core_buf[1 - high]
        self.copies.append(
            send(q.at[1 - high], link_buf, sems_s.at[2], sems_r.at[2], across(*LINKS[2]))
        )

    def arrive(self):
        self.copies[1].wait_recv()
        self.copies[2].wait_recv()

    def rows(self, rows):
        high, q, core_buf, link_buf, _, _ = self.args
        return (
            q[high, rows].astype(jnp.float32)
            + core_buf[high, rows].astype(jnp.float32)
            + link_buf[rows].astype(jnp.float32)
        )

    def finish(self):
        for copy in self.copies:
            copy.wait_send()


SUM_SEMS = [
    pltpu.SemaphoreType.DMA((3,)),
    pltpu.SemaphoreType.DMA((3,)),
    pltpu.SemaphoreType.DMA,
]


def middle_kernel(
    part_ref, tok_ref, cot_ref, gain_ref, resid_ref, all_ref, cot_all_ref,
    q, core_buf, link_buf, low, *sems
):
    greet([across(*link) for link in LINKS] + [across(*CORE)])
    total = SumTensor(part_ref, q, core_buf, link_buf, *sems[:3])
    total.pass_on()
    cots = Gather(cot_ref, cot_all_ref, *sems[8:])
    cots.step(0)
    total.arrive()

    def strip(i, carry):
        rows = pl.ds(pl.multiple_of(i * STRIP, STRIP), STRIP)
        resid = tok_ref[rows].astype(jnp.float32) + total.rows(rows)
        resid_ref[rows] = resid
        inv = lax.rsqrt(jnp.mean(resid * resid, axis=-1, keepdims=True) + epsilon)
        low[rows] = (resid * inv * gain_ref[...]).astype(low.dtype)
        return carry

    lax.fori_loop(0, tok_ref.shape[0] // STRIP, strip, 0)
    total.finish()
    blocks = Gather(low, all_ref, *sems[3:8])
    cots.step(1)
    blocks.step(0)
    blocks.step(1)
    cots.step(2)
    blocks.step(2)
    cots.finish()
    blocks.finish()


def middle(part, tok, cot, gain):
    rows, width = tok.shape
    vmem, anywhere = pl.BlockSpec(memory_space=pltpu.VMEM), pl.BlockSpec(memory_space=pl.ANY)
    return pl.pallas_call(
        middle_kernel,
        name="middle",
        out_shape=(
            jax.ShapeDtypeStruct((rows, width), jnp.float32),
            jax.ShapeDtypeStruct((2, 2, 2, 2, rows, width), jnp.bfloat16),
            jax.ShapeDtypeStruct((2, 2, 2, 2, rows, width), jnp.bfloat16),
        ),
        in_specs=[anywhere, vmem, vmem, vmem],
        out_specs=(vmem, anywhere, anywhere),
        scratch_shapes=[
            pltpu.VMEM((2, rows, width), jnp.bfloat16),
            pltpu.VMEM((2, rows, width), jnp.bfloat16),
            pltpu.VMEM((rows, width), jnp.bfloat16),
            pltpu.VMEM((rows, width), jnp.bfloat16),
            *SUM_SEMS,
            *GATHER_SEMS,
            *GATHER_SEMS,
        ],
        compiler_params=pltpu.CompilerParams(
            collective_id=1, has_side_effects=True, vmem_limit_bytes=32 * 2**20
        ),
    )(part.reshape(2, 2, rows, width), tok, cot, gain.reshape(1, width))


def product_pair_kernel(left1_ref, left2_ref, right1_ref, right2_ref, out_ref):
    tile = 512
    for at in range(0, out_ref.shape[1], tile):
        part = slice(at, at + tile)
        total = contract_last(left1_ref[...], right1_ref[part])
        total += contract_last(left2_ref[...], right2_ref[part])
        out_ref[:, part] = total.astype(out_ref.dtype)


def product_pair(left1, left2, right1, right2):
    rows, depth = left1.shape
    width = right1.shape[0]
    block = 256
    left = pl.BlockSpec((block, depth), lambda i: (i, 0))
    right = pl.BlockSpec((width, depth), lambda i: (0, 0))
    return pl.pallas_call(
        product_pair_kernel,
        name="product_pair",
        grid=(rows // block,),
        out_shape=jax.ShapeDtypeStruct((rows, width), jnp.bfloat16),
        in_specs=[left, left, right, right],
        out_specs=pl.BlockSpec((block, width), lambda i: (i, 0)),
        cost_estimate=pl.CostEstimate(
            flops=4 * rows * depth * width,
            bytes_accessed=2 * (2 * rows * depth + 2 * width * depth + rows * width),
            transcendentals=0,
        ),
        compiler_params=pltpu.CompilerParams(vmem_limit_bytes=32 * 2**20),
    )(left1, left2, right1, right2)


def norm_back(rows, back, base_ref, gain_ref, keep_ref, gain_acc):
    base = base_ref[rows].astype(jnp.float32)
    inv = lax.rsqrt(jnp.mean(base * base, axis=-1, keepdims=True) + epsilon)
    unit = base * inv
    scaled = gain_ref[...] * back
    grad = inv * (scaled - unit * jnp.mean(unit * scaled, axis=-1, keepdims=True))
    terms = back * unit
    gain_acc[...] += terms[:8] + terms[8:]
    return keep_ref[rows].astype(jnp.float32) + grad


def back_kernel(
    p_ref, resid_ref, cot_ref, gain_ref, grad_ref, all_ref, gain_out,
    q, cb, r0, r1, r2, low, gain_acc, ssem, rsem, fs, fr, own_sem, gs, gr, gather_own
):
    me = [bit_of(*link) for link in LINKS]
    core = bit_of(*CORE)
    peers = [across(*link) for link in LINKS]
    core_peer = across(*CORE)
    spans = column_spans(q.shape[-1])
    own = pltpu.make_async_copy(p_ref.at[:, :, :, core], q, own_sem)
    own.start()
    greet(peers + [core_peer])

    def half(k, near):
        first = SUM_ORDERS[k][0]
        return [(me[d] if near else 1 - me[d]) if d == first else slice(None) for d in range(3)]

    to_core = []
    for near in (False, True):
        for k in COLORS:
            i = half(k, near)
            to_core.append(
                send(
                    p_ref.at[i[0], i[1], i[2], 1 - core, :, pl.ds(*spans[k])],
                    cb.at[i[0], i[1], i[2], :, pl.ds(*spans[k])],
                    fs.at[len(to_core)],
                    fr.at[len(to_core)],
                    core_peer,
                )
            )
    own.wait()

    def add(i, k, other):
        s, n = spans[k]
        q[i[0], i[1], i[2], :, s : s + n] = q[i[0], i[1], i[2], :, s : s + n] + other

    moving, sent = [], []
    for near in (False, True):
        for k in COLORS:
            to_core[len(ORDERS) * near + k].wait_recv()
            i = half(k, near)
            s, n = spans[k]
            add(i, k, cb[i[0], i[1], i[2], :, s : s + n])
            if not near:
                moving.append(
                    send(
                        q.at[i[0], i[1], i[2], :, pl.ds(s, n)],
                        r0.at[:, :, :, pl.ds(s, n)],
                        ssem.at[k, 0],
                        rsem.at[k, 0],
                        peers[SUM_ORDERS[k][0]],
                    )
                )
    for step in (1, 2):
        for k in COLORS:
            s, n = spans[k]
            order = SUM_ORDERS[k]
            moving[k].wait_recv()
            sent.append(moving[k])
            kept = [me[d] if d in order[:step] else slice(None) for d in range(3)]
            add(kept, k, r0[:, :, :, s : s + n] if step == 1 else r1[:, :, s : s + n])
            away = [
                me[d] if d in order[:step] else (1 - me[d] if d == order[step] else slice(None))
                for d in range(3)
            ]
            moving[k] = send(
                q.at[away[0], away[1], away[2], :, pl.ds(s, n)],
                r1.at[:, :, pl.ds(s, n)] if step == 1 else r2.at[:, pl.ds(s, n)],
                ssem.at[k, step],
                rsem.at[k, step],
                peers[order[step]],
            )
    for k in COLORS:
        moving[k].wait_recv()
        sent.append(moving[k])
    gain_acc[...] = jnp.zeros_like(gain_acc)

    def strip(i, carry):
        rows = pl.ds(pl.multiple_of(i * STRIP, STRIP), STRIP)
        back = q[me[0], me[1], me[2], rows].astype(jnp.float32) + r2[rows].astype(jnp.float32)
        grad = norm_back(rows, back, resid_ref, gain_ref, cot_ref, gain_acc)
        grad_ref[rows] = grad
        low[rows] = grad.astype(low.dtype)
        return carry

    lax.fori_loop(0, low.shape[0] // STRIP, strip, 0)
    for copy in sent + to_core:
        copy.wait_send()
    gain_out[...] = jnp.sum(gain_acc[...], axis=0, keepdims=True)
    mine = all_ref.at[me[2], core]
    local = pltpu.make_async_copy(low, mine, gather_own)
    local.start()
    along = send(low, mine, gs.at[0], gr.at[0], peers[2])
    beside = send(low, mine, gs.at[1], gr.at[1], core_peer)
    along.wait_recv()
    theirs = all_ref.at[1 - me[2], core]
    onward = send(theirs, theirs, gs.at[2], gr.at[2], core_peer)
    local.wait()
    beside.wait()
    onward.wait()
    along.wait_send()


def back_pass(part, resid, cot, gain):
    rows, width = resid.shape
    wide = lambda *lead: pltpu.VMEM((*lead, rows, width), jnp.bfloat16)
    vmem = pl.BlockSpec(memory_space=pltpu.VMEM)
    return pl.pallas_call(
        back_kernel,
        name="back",
        out_shape=(
            jax.ShapeDtypeStruct((rows, width), jnp.float32),
            jax.ShapeDtypeStruct((2, 2, rows, width), jnp.bfloat16),
            jax.ShapeDtypeStruct((1, width), jnp.float32),
        ),
        in_specs=[pl.BlockSpec(memory_space=pl.ANY), vmem, vmem, vmem],
        out_specs=(vmem, pl.BlockSpec(memory_space=pl.ANY), vmem),
        scratch_shapes=[
            wide(2, 2, 2),
            wide(2, 2, 2),
            wide(2, 2),
            wide(2),
            wide(),
            wide(),
            pltpu.VMEM((8, width), jnp.float32),
            pltpu.SemaphoreType.DMA((len(ORDERS), 3)),
            pltpu.SemaphoreType.DMA((len(ORDERS), 3)),
            pltpu.SemaphoreType.DMA((2 * len(ORDERS),)),
            pltpu.SemaphoreType.DMA((2 * len(ORDERS),)),
            pltpu.SemaphoreType.DMA,
            pltpu.SemaphoreType.DMA((3,)),
            pltpu.SemaphoreType.DMA((3,)),
            pltpu.SemaphoreType.DMA,
        ],
        compiler_params=pltpu.CompilerParams(
            collective_id=2, has_side_effects=True, vmem_limit_bytes=40 * 2**20
        ),
    )(part.reshape(2, 2, 2, 2, rows, width), resid, cot, gain.reshape(1, width))


class Halve:
    def __init__(self, source, held, came, load_sem, send_sem, recv_sem, order, at_column=0):
        self.held, self.came, self.sems, self.order = held, came, (send_sem, recv_sem), order
        self.dims = sorted(order, reverse=True)
        self.sent, self.loads, at = [], [], 0
        lead = [slice(None) for _ in order]
        columns = pl.ds(at_column, held.shape[-1])
        for i, part in enumerate(source):
            rows = part.shape[-2]
            self.loads.append(
                pltpu.make_async_copy(
                    part.at[(*lead, slice(None), columns)],
                    held.at[(*lead, pl.ds(at, rows))],
                    load_sem.at[i],
                )
            )
            self.loads[-1].start()
            at += rows

    def index(self, done, away=None):
        picks = []
        for bit in self.dims:
            if bit in done:
                picks.append(bit_of("dp", bit))
            elif bit == away:
                picks.append(1 - bit_of("dp", bit))
            else:
                picks.append(slice(None))
        return tuple(picks)

    def start(self, step):
        if step == 0:
            for load in self.loads:
                load.wait()
        bit = self.order[step]
        self.moving = send(
            self.held.at[self.index(self.order[:step], bit)],
            self.came[step],
            self.sems[0].at[step],
            self.sems[1].at[step],
            across("dp", bit),
        )
        self.sent.append(self.moving)

    def land(self, step):
        self.moving.wait_recv()
        kept = self.index(self.order[: step + 1])
        self.held[kept] = self.held[kept] + self.came[step][...]
        if step + 1 < len(self.order):
            self.start(step + 1)

    def result(self):
        return self.held[self.index(self.order)]

    def finish(self):
        for copy in self.sent:
            copy.wait_send()


def halve_scratch(bits, rows, width):
    scratch = [pltpu.VMEM((*[2] * bits, rows, width), jnp.bfloat16)]
    for step in range(bits):
        scratch.append(pltpu.VMEM((*[2] * (bits - 1 - step), rows, width), jnp.bfloat16))
    return scratch + [
        pltpu.SemaphoreType.DMA((2,)),
        pltpu.SemaphoreType.DMA((bits,)),
        pltpu.SemaphoreType.DMA((bits,)),
    ]


def last_plan(bits, rows, few_rows, width):
    wide = -(-width // 256) * 128
    swapped = [1, 0, *range(2, bits)]
    return [
        (list(range(bits)), 0, halve_scratch(bits, rows + few_rows, wide)),
        (swapped, wide, halve_scratch(bits, rows + few_rows, width - wide)),
        (list(range(1, bits)), 0, halve_scratch(bits - 1, rows, width)),
        ([0, *range(2, bits)], 0, halve_scratch(bits - 1, rows, width)),
    ]


def last_kernel(
    plan, part_ref, tok_ref, keep_ref, gain_ref, wide_ref, few_ref, y_ref, o_ref,
    row_ref,
    grad_ref, gain_out, wide_out, few_out, y_out, o_out, row_out,
    q, core_buf, link_buf, gain_acc, *refs
):
    sum_sems, refs = refs[:3], refs[3:]
    sources = ((wide_ref, few_ref), (wide_ref, few_ref), (y_ref,), (o_ref,))
    halvings = []
    for source, (order, column, scratch) in zip(sources, plan):
        mine, refs = refs[: len(scratch)], refs[len(scratch) :]
        came = mine[1 : 1 + len(order)]
        halvings.append(Halve(source, mine[0], came, *mine[1 + len(order) :], order, column))
    bits = len(plan[0][0])
    peers = [across("dp", bit) for bit in range(bits)]
    spot, *spots = spots_of_four()
    both = {"dp": lax.axis_index("dp") + (spots[2] - spot) * (1 << FIRST_BIT)}
    greet([across(*LINKS[2]), across(*CORE), both] + peers)
    total = SumTensor(part_ref, q, core_buf, link_buf, *sum_sems)
    turns = [halvings[i] for i in (2, 3, 1, 0)]
    for each in turns:
        each.start(0)
    collects = [Collect(row_ref, row_out, *refs)]
    total.pass_on()
    gain_acc[...] = jnp.zeros_like(gain_acc)

    def strip(i, carry):
        rows = pl.ds(pl.multiple_of(i * STRIP, STRIP), STRIP)
        back = total.rows(rows)
        grad_ref[rows] = norm_back(rows, back, tok_ref, gain_ref, keep_ref, gain_acc)
        return carry

    total.arrive()
    lax.fori_loop(0, tok_ref.shape[0] // STRIP, strip, 0)
    gain_out[...] = jnp.sum(gain_acc[...], axis=0, keepdims=True)
    for step in range(bits):
        for each in turns:
            if step < len(each.order):
                each.land(step)
    rows = wide_out.shape[0]
    for each, (_, column, _) in zip(halvings[:2], plan):
        mine = each.result()
        columns = slice(column, column + mine.shape[1])
        wide_out[:, columns] = mine[:rows].astype(jnp.float32)
        few_out[:, columns] = mine[rows:]
    for each in collects:
        each.finish()
    y_out[...] = halvings[2].result().astype(jnp.float32)
    o_out[...] = halvings[3].result().astype(jnp.float32)
    for each in (*halvings, total):
        each.finish()


def last_pass(part, tok, keep, gain, wide, few, side_y, side_o, rows_part, hidden_width):
    rows, width = tok.shape
    vmem, anywhere = pl.BlockSpec(memory_space=pltpu.VMEM), pl.BlockSpec(memory_space=pl.ANY)
    bits = wide.shape[0].bit_length() - 1
    plan = last_plan(bits, wide.shape[1], few.shape[1], wide.shape[2])
    block = jax.ShapeDtypeStruct(wide.shape[1:], jnp.float32)
    leading = [2] * bits
    return pl.pallas_call(
        functools.partial(last_kernel, plan),
        name="last",
        out_shape=(
            jax.ShapeDtypeStruct((rows, width), jnp.float32),
            jax.ShapeDtypeStruct((1, width), jnp.float32),
            block,
            jax.ShapeDtypeStruct(few.shape[1:], jnp.bfloat16),
            block,
            block,
            jax.ShapeDtypeStruct((rows_part.shape[1], hidden_width), jnp.float32),
        ),
        in_specs=[anywhere, vmem, vmem, vmem] + [anywhere] * 5,
        out_specs=(vmem,) * 7,
        scratch_shapes=[
            pltpu.VMEM((2, rows, width), jnp.bfloat16),
            pltpu.VMEM((2, rows, width), jnp.bfloat16),
            pltpu.VMEM((rows, width), jnp.bfloat16),
            pltpu.VMEM((8, width), jnp.float32),
            *SUM_SEMS,
            *[ref for _, _, scratch in plan for ref in scratch],
            *collect_scratch(*rows_part.shape[1:]),
        ],
        compiler_params=pltpu.CompilerParams(
            collective_id=3, has_side_effects=True, vmem_limit_bytes=48 * 2**20
        ),
    )(
        part.reshape(2, 2, rows, width),
        tok,
        keep,
        gain.reshape(1, width),
        wide.reshape(*leading, *wide.shape[1:]),
        few.reshape(*leading, *few.shape[1:]),
        side_y,
        side_o,
        rows_part,
    )


def scan_kernel(n, reverse, *refs):
    a_ref, b_ref, out_ref, edge_ref, fa, fb, mine, others, ssem, rsem = refs
    place = lax.axis_index("dp")
    sign = -1 if reverse else 1
    barrier = pltpu.get_barrier_semaphore()
    peers = [{"dp": (place + sign * hop + n) % n} for hop in range(1, n)]
    for peer in peers:
        pl.semaphore_signal(barrier, inc=1, device_id=peer, device_id_type=MESH)
    rows, width = a_ref.shape
    length = rows // 8
    lanes = range(width // 128)
    for k in lanes:
        fa[k * rows : (k + 1) * rows] = a_ref[:, k * 128 : (k + 1) * 128]
        fb[k * rows : (k + 1) * rows] = b_ref[:, k * 128 : (k + 1) * 128]

    def at(k, r):
        return pl.ds(k * rows + (length - 1 - r if reverse else r), 8, stride=length)

    def local(r, carry):
        result = []
        for k in lanes:
            prod, state = carry[k]
            decay = fa[at(k, r), :]
            term = fb[at(k, r), :]
            if reverse:
                fa[at(k, r), :] = prod
                total = term + state
                fb[at(k, r), :] = total
                result.append((prod * decay, decay * total))
            else:
                prod = prod * decay
                state = decay * state + term
                fa[at(k, r), :] = prod
                fb[at(k, r), :] = state
                result.append((prod, state))
        return result

    start = [(jnp.ones((8, 128), jnp.float32), jnp.zeros((8, 128), jnp.float32)) for k in lanes]
    ends = lax.fori_loop(0, length, local, start, unroll=2)
    prod = jnp.concatenate([end[0] for end in ends], axis=1)
    state = jnp.concatenate([end[1] for end in ends], axis=1)
    order = range(7, -1, -1) if reverse else range(8)
    run_a, run_b = jnp.ones((1, width), jnp.float32), jnp.zeros((1, width), jnp.float32)
    before = [None] * 8
    for s in order:
        before[s] = (run_a, run_b)
        pa, pb = prod[s : s + 1], state[s : s + 1]
        run_a, run_b = pa * run_a, pa * run_b + pb
    mine[0:1] = run_a
    mine[1:2] = run_b
    pl.semaphore_wait(barrier, n - 1)
    copies = [
        send(mine, others.at[hop - 1], ssem.at[hop - 1], rsem.at[hop - 1], peers[hop - 1])
        for hop in range(1, n)
    ]
    carry = jnp.zeros((1, width), jnp.float32)
    ahead = n - 1 - place if reverse else place
    for copy in copies:
        copy.wait_recv()
    for hop in range(n - 1, 0, -1):
        step = others[hop - 1, 0:1] * carry + others[hop - 1, 1:2]
        carry = jnp.where(hop <= ahead, step, carry)
    edge_ref[...] = carry
    entering = jnp.concatenate([pa * carry + pb for pa, pb in before], axis=0)

    def fix(r, c):
        for k in lanes:
            fb[at(k, r), :] = fb[at(k, r), :] + fa[at(k, r), :] * entering[:, k * 128 : (k + 1) * 128]
        return c

    lax.fori_loop(0, length, fix, 0, unroll=2)
    for k in lanes:
        out_ref[:, k * 128 : (k + 1) * 128] = fb[k * rows : (k + 1) * rows]
    for copy in copies:
        copy.wait_send()


def scan_stream(decay, term, reverse):
    n = lax.axis_size("dp")
    rows, width = decay.shape
    vmem = pl.BlockSpec(memory_space=pltpu.VMEM)
    return pl.pallas_call(
        functools.partial(scan_kernel, n, reverse),
        name="scan_back" if reverse else "scan",
        out_shape=(
            jax.ShapeDtypeStruct((rows, width), jnp.float32),
            jax.ShapeDtypeStruct((1, width), jnp.float32),
        ),
        in_specs=[vmem, vmem],
        out_specs=(vmem, vmem),
        scratch_shapes=[
            pltpu.VMEM((rows * width // 128, 128), jnp.float32),
            pltpu.VMEM((rows * width // 128, 128), jnp.float32),
            pltpu.VMEM((2, width), jnp.float32),
            pltpu.VMEM((n - 1, 2, width), jnp.float32),
            pltpu.SemaphoreType.DMA((n - 1,)),
            pltpu.SemaphoreType.DMA((n - 1,)),
        ],
        compiler_params=pltpu.CompilerParams(
            collective_id=5 if reverse else 4, has_side_effects=True, vmem_limit_bytes=32 * 2**20
        ),
    )(decay, term)


def in_order(bit, mine, theirs, axis=0):
    return jnp.where(
        bit == 0, jnp.concatenate([mine, theirs], axis), jnp.concatenate([theirs, mine], axis)
    )


def parted(held, dims, bit):
    mine = (lax.axis_index("dp") >> bit) % 2
    axis = dims.index(bit)
    return (
        lax.dynamic_index_in_dim(held, mine, axis, False),
        lax.dynamic_index_in_dim(held, 1 - mine, axis, False),
    )


def added(keep, came):
    return (keep.astype(jnp.float32) + came.astype(jnp.float32)).astype(jnp.bfloat16)


def inner(
    tokens,
    doc_start,
    norm1_gain,
    proj_x,
    proj_y,
    conv_weight,
    conv_bias,
    gate_x_weight,
    gate_x_bias,
    gate_a_weight,
    gate_a_bias,
    decay_param,
    proj_out,
    norm2_gain,
    mlp_gate,
    mlp_up,
    mlp_down,
    cotangent,
):
    tok_rows = tokens.shape[0]
    chan_width = proj_x.shape[1]
    block_width = gate_x_weight.shape[0]
    half_width = block_width // 2
    tap_count = conv_weight.shape[0]
    parity = lax.axis_index("tensor") % 2
    full_start = parity * half_width
    shared_start = (1 - parity) * 2 * block_width
    tensor_size = lax.axis_size("tensor")
    share_rows = tok_rows // tensor_size
    own_start = lax.axis_index("tensor") * share_rows
    positions = lax.axis_index("dp") * tok_rows + lax.iota(jnp.int32, tok_rows)
    starting = (doc_start == positions)[:, None]
    dp_size = lax.axis_size("dp")
    low_size = 1 << FIRST_BIT
    high_size = dp_size // (GROUP * low_size)

    def dp_index(high, four, low):
        return (high * GROUP + four) * low_size + low

    highs, fours, lows = range(high_size), range(GROUP), range(low_size)
    groups = [
        [dp_index(h, i, l) * tensor_size + t for i in fours for t in range(tensor_size)]
        for h in highs
        for l in lows
    ]
    low_groups = [[dp_index(h, i, l) for l in lows] for h in highs for i in fours]
    high_groups = [[dp_index(h, i, l) for h in highs] for i in fours for l in lows]
    everyone = ("dp", "tensor")

    spot = lax.axis_index("dp") // low_size % GROUP
    hidden_width = mlp_gate.shape[1]
    share = share_width(hidden_width)

    def all_rows(parts):
        rows = parts.shape[2]
        parts = lax.all_gather(parts, "dp", axis=1, axis_index_groups=high_groups, tiled=True)
        return parts.reshape(parts.shape[0], dp_size * rows, share)

    def own_rows(grad):
        rows = grad.shape[0] // dp_size
        grad = grad.astype(jnp.bfloat16).reshape(high_size * GROUP, low_size, rows, share)
        if high_size > 1:
            grad = lax.psum_scatter(
                grad, "dp", axis_index_groups=high_groups, scatter_dimension=0, tiled=True
            )
        if low_size > 1:
            grad = lax.psum_scatter(
                grad, "dp", axis_index_groups=low_groups, scatter_dimension=1, tiled=True
            )
        return grad.reshape(GROUP, rows, share)

    cot_own = lax.dynamic_slice_in_dim(cotangent, own_start, share_rows, 0)
    gate_pieces = exchanged(cut(mlp_gate))
    pieces = exchanged(cut(mlp_up, mlp_down))
    tok_own = lax.dynamic_slice_in_dim(tokens, own_start, share_rows, 0)

    def normalize(values):
        values = values.astype(jnp.float32)
        inv_rms = lax.rsqrt(jnp.mean(values * values, axis=-1, keepdims=True) + epsilon)
        return (values * inv_rms * norm1_gain).astype(jnp.bfloat16)

    halo = 16
    normed_low = normalize(tokens)
    normed_low, *gate_pieces = lax.optimization_barrier((normed_low, *gate_pieces))
    (gate_cols,) = all_rows(placed(gate_pieces))
    normed_prev = normalize(shifted(tokens[tok_rows - halo :], "dp", 1))
    branch_y = matmul(normed_low, proj_y)
    branch_x = matmul(normed_low, proj_x).astype(jnp.bfloat16)
    prev_x = matmul(normed_prev, proj_x).astype(jnp.bfloat16)
    extended = jnp.concatenate([prev_x[halo - tap_count + 1 :], branch_x], axis=0).astype(
        jnp.float32
    )

    def conv_apply(ext_rows, weight, bias_vec):
        conv_out = bias_vec + weight[0] * ext_rows[tap_count - 1 :]
        for offset in range(1, tap_count):
            inside = (positions - offset >= doc_start).astype(jnp.float32)[:, None]
            lagged = ext_rows[tap_count - 1 - offset : tap_count - 1 - offset + tok_rows]
            conv_out = conv_out + weight[offset] * lagged * inside
        return conv_out

    conv_out, conv_pull = jax.vjp(conv_apply, extended, conv_weight, conv_bias)
    mixed_low = conv_out.astype(jnp.bfloat16)
    own_half = lax.dynamic_slice_in_dim(mixed_low, shared_start, half_width, 1)
    other_half = flipped(own_half, "tensor", 1)
    shared_in = in_order(parity, own_half, other_half, 1)
    full_in = lax.dynamic_slice_in_dim(mixed_low, full_start, 2 * block_width, 1).reshape(
        tok_rows, 2, block_width
    )

    def place(full_part, shared_part):
        return in_order(parity, full_part, shared_part, 1)

    def full_weight(weight):
        return lax.dynamic_slice_in_dim(weight, full_start, 2 * block_width, 1).reshape(
            block_width, 2, block_width
        )

    def shared_weight(weight):
        return lax.dynamic_slice_in_dim(weight, shared_start, half_width, 1)

    def gate_pre(weight, bias_vec):
        full_out = jnp.einsum(
            "nhi,ihj->nhj", full_in, full_weight(weight), preferred_element_type=jnp.float32
        ).reshape(tok_rows, 2 * block_width)
        shared_out = matmul(shared_in, shared_weight(weight))
        return place(full_out, shared_out) + bias_vec

    def recurrence_in(conv_vals, pre_input, pre_recur, param_vec):
        log_decay = -8.0 * jax.nn.sigmoid(pre_recur) * jax.nn.softplus(param_vec)
        decay = jnp.where(starting, 0.0, jnp.exp(log_decay))
        multiplier = jnp.where(starting, 1.0, jnp.sqrt(-jnp.expm1(2.0 * log_decay)))
        return (decay, multiplier * jax.nn.sigmoid(pre_input) * conv_vals)

    pre_input = gate_pre(gate_x_weight, gate_x_bias)
    pre_recur = gate_pre(gate_a_weight, gate_a_bias)
    (decay, drive), recur_pull = jax.vjp(
        recurrence_in, mixed_low.astype(jnp.float32), pre_input, pre_recur, decay_param
    )
    decay, drive, *pieces = lax.optimization_barrier((decay, drive, *pieces))
    up_cols, down_cols = all_rows(placed(pieces))
    states, entering = scan_stream(decay, drive, False)
    previous = jnp.concatenate([entering, states[:-1]], axis=0)
    gelu_y, gelu_pull = jax.vjp(gelu_tanh, branch_y)
    product_low = (states * gelu_y).astype(jnp.bfloat16)
    lru_part = matmul(product_low, proj_out).astype(jnp.bfloat16)
    resid, normed2_all, cot_all = middle(lru_part, tok_own, cot_own, norm2_gain)
    cot_all = cot_all.reshape(GROUP * tok_rows, -1)
    normed2_all = normed2_all.reshape(GROUP * tok_rows, -1)
    counted = lax.iota(jnp.int32, share) >= overlap_of(hidden_width) * (spot // (GROUP - 1))

    def once(values):
        return jnp.where(counted, values, 0.0).astype(jnp.bfloat16)

    gate_act = matmul(normed2_all, gate_cols)
    up_act = matmul(normed2_all, up_cols)
    hidden, act_pull = jax.vjp(gated_product, gate_act, up_act)
    hidden_low = once(hidden)
    grad_hidden = matmul(cot_all, down_cols)
    grad_gate, grad_up = act_pull(grad_hidden)
    grad_gate_low = once(grad_gate)
    grad_up_low = once(grad_up)

    back_part = product_pair(grad_gate_low, grad_up_low, gate_cols, up_cols)
    down_grad = contract_first(cot_all, hidden_low).astype(jnp.bfloat16)
    gate_grad = contract_first(normed2_all, grad_gate_low).astype(jnp.bfloat16)
    down_rows, gate_rows = own_rows(down_grad), own_rows(gate_grad)
    back_part, _, _ = lax.optimization_barrier((back_part, down_grad, gate_grad))
    grad_resid, grad_lru_low, grad_gain2 = back_pass(back_part, resid, cot_own, norm2_gain)
    grad_lru_low = grad_lru_low.reshape(tok_rows, -1)
    grad_product = contract_last(grad_lru_low, proj_out)
    grad_states = grad_product * gelu_y
    grad_y_low = gelu_pull(grad_product * states)[0].astype(jnp.bfloat16)
    total_grad, _ = scan_stream(decay, grad_states, True)
    total_grad, late_y, late_lru = lax.optimization_barrier(
        (total_grad, grad_y_low, grad_lru_low)
    )

    def token_sum(left_rows, right_rows):
        return contract_first(left_rows, right_rows).astype(jnp.bfloat16)

    def per_device(rows):
        return rows.reshape(dp_size, rows.shape[0] // dp_size, rows.shape[1])

    dims = list(range(dp_size.bit_length() - 1))[::-1]

    def by_bits(grad):
        return grad.reshape(*[2] * len(dims), grad.shape[0] // dp_size, grad.shape[1])

    keep_y, away_y = parted(by_bits(token_sum(normed_low, late_y)), dims, 0)
    keep_o, away_o = parted(by_bits(token_sum(late_lru, product_low)), dims, 1)
    total_grad, away_y, away_o, late_up, late_hidden = lax.optimization_barrier(
        (total_grad, away_y, away_o, grad_up_low, hidden_low)
    )
    came_y, came_o = flipped(away_y, "dp", 1), flipped(away_o, "dp", 2)
    up_grad = contract_first(normed2_all, late_up)
    out_part = contract_last(late_hidden, down_cols).astype(jnp.bfloat16)
    up_rows = own_rows(up_grad)
    block_out = resid + lax.psum_scatter(
        out_part,
        everyone,
        axis_index_groups=groups,
        scatter_dimension=0,
        tiled=True,
    ).astype(jnp.float32)
    back_y = contract_last(late_y, proj_y)
    conv_direct, grad_pre_input, grad_pre_recur, grad_param = recur_pull(
        (total_grad * previous, total_grad)
    )

    grad_pre_input, grad_pre_recur, *rows = lax.optimization_barrier(
        (grad_pre_input, grad_pre_recur, down_rows, gate_rows)
    )
    row_pieces = picked(*rows)
    row_pieces = exchanged(row_pieces)

    def gate_back(weight, grad_pre):
        grad_pre_low = grad_pre.astype(jnp.bfloat16)
        grad_full = lax.dynamic_slice_in_dim(grad_pre_low, full_start, 2 * block_width, 1).reshape(
            tok_rows, 2, block_width
        )
        grad_share = lax.dynamic_slice_in_dim(grad_pre_low, shared_start, half_width, 1)
        into_full = jnp.einsum(
            "nhj,ihj->nhi", grad_full, full_weight(weight), preferred_element_type=jnp.float32
        ).reshape(tok_rows, 2 * block_width)
        into_share = contract_last(grad_share, shared_weight(weight))
        weight_full = jnp.einsum(
            "nhi,nhj->ihj", full_in, grad_full, preferred_element_type=jnp.float32
        ).reshape(block_width, 2 * block_width)
        weight_share = contract_first(shared_in, grad_share)
        return (into_full, into_share, place(weight_full, weight_share))

    input_full, input_share, grad_gx_weight = gate_back(gate_x_weight, grad_pre_input)
    recur_full, recur_share, grad_ga_weight = gate_back(gate_a_weight, grad_pre_recur)
    full_sum = input_full + recur_full
    share_sum = input_share + recur_share
    own_grad = jnp.where(parity == 0, share_sum[:, :half_width], share_sum[:, half_width:])
    other_grad = jnp.where(parity == 0, share_sum[:, half_width:], share_sum[:, :half_width])
    returned = flipped(other_grad.astype(jnp.bfloat16), "tensor", 1).astype(other_grad.dtype)
    grad_conv = conv_direct + place(full_sum, own_grad + returned)
    grad_extended, grad_conv_weight, grad_conv_bias = conv_pull(grad_conv)
    rim_rows, came_y, came_o = lax.optimization_barrier(
        (grad_extended[: tap_count - 1], came_y, came_o)
    )
    side_y, side_o = added(keep_y, came_y), added(keep_o, came_o)
    rim_grad = shifted(rim_rows, "dp", -1)
    grad_branch_x = grad_extended[tap_count - 1 :] + jnp.concatenate(
        [jnp.zeros((tok_rows - tap_count + 1, chan_width), jnp.float32), rim_grad], axis=0
    )
    grad_x_low = grad_branch_x.astype(jnp.bfloat16)
    wide = jnp.concatenate([grad_gx_weight, grad_ga_weight], axis=0)
    sums = jnp.concatenate(
        [
            grad_conv_weight,
            grad_conv_bias[None],
            jnp.sum(grad_pre_input, axis=0)[None],
            jnp.sum(grad_pre_recur, axis=0)[None],
            grad_param[None],
        ],
        axis=0,
    )
    spare = dp_size * 16 - sums.shape[0]
    sums = jnp.concatenate([sums, jnp.zeros((spare, chan_width), jnp.float32)], axis=0)
    few = jnp.concatenate(
        [per_device(wide.astype(jnp.bfloat16)), per_device(sums.astype(jnp.bfloat16))], axis=1
    )
    grad_tokens, grad_gain1, grad_proj_x, reduced, grad_proj_y, grad_out, grad_mlp_up = last_pass(
        (contract_last(grad_x_low, proj_x) + back_y).astype(jnp.bfloat16),
        tok_own,
        grad_resid,
        norm1_gain,
        per_device(token_sum(normed_low, grad_x_low)),
        few,
        side_y,
        side_o,
        up_rows,
        hidden_width,
    )
    grad_proj_out = grad_out.T
    shared, gains = final_pass(reduced, grad_gain1, grad_gain2)
    gains, *row_pieces = lax.optimization_barrier((gains, *row_pieces))
    grad_mlp_down, grad_mlp_gate = joined(row_pieces, hidden_width)
    wide_rows = 2 * block_width // dp_size
    wide = shared[:, :wide_rows].reshape(2 * block_width, chan_width).astype(jnp.float32)
    small = shared[:, wide_rows:].reshape(dp_size * 16, chan_width).astype(jnp.float32)
    return (
        block_out,
        grad_tokens,
        gains[0],
        grad_proj_x,
        grad_proj_y,
        small[:tap_count],
        small[tap_count],
        wide[:block_width],
        small[tap_count + 1],
        wide[block_width:],
        small[tap_count + 2],
        small[tap_count + 3],
        grad_proj_out,
        gains[1],
        grad_mlp_gate,
        grad_mlp_up,
        grad_mlp_down,
    )


def solution(mesh):
    placed = (
        P("dp", None),
        P("dp"),
        P(),
        P(None, "tensor"),
        P(None, "tensor"),
        P(None, "tensor"),
        P("tensor"),
        P(None, "tensor"),
        P("tensor"),
        P(None, "tensor"),
        P("tensor"),
        P("tensor"),
        P("tensor", None),
        P(),
        P("dp", "tensor"),
        P("dp", "tensor"),
        P("dp", "tensor"),
        P("dp", None),
    )
    return jax.shard_map(
        inner,
        mesh=mesh,
        in_specs=placed,
        out_specs=(
            P(("dp", "tensor"), None),
            P(("dp", "tensor"), None),
            P(),
            P("dp", "tensor"),
            P("dp", "tensor"),
            P(None, "tensor"),
            P("tensor"),
            P(None, "tensor"),
            P("tensor"),
            P(None, "tensor"),
            P("tensor"),
            P("tensor"),
            P("tensor", "dp"),
            P(),
            P("dp", "tensor"),
            P("dp", "tensor"),
            P("dp", "tensor"),
        ),
        check_vma=False,
    )
```
